32 devices in a mesh: dp: 2 (over x), sp: 4 (over z), tp: 4 (over y, core).
Axes of the slice: x: 2, y: 2, z: 4, core: 2. Of those that a mesh axis runs over, the one named last changes fastest.
Arguments:
- x_in: bfloat16 [32768, 4096], P(('dp', 'sp', 'tp')), parts along dimension 0
- seg_ids: int32 [32768], P(('dp', 'sp', 'tp')), parts along dimension 0
- w_zx: bfloat16 [4096, 2, 8192], P(None, None, 'tp')
- w_bc: bfloat16 [4096, 2, 1024], P(None, None, 'tp')
- w_dt: bfloat16 [4096, 128], P(None, 'tp')
- conv_x: bfloat16 [4, 8192], P(None, 'tp')
- conv_bc: bfloat16 [4, 2, 1024], P(None, None, 'tp')
- bias_x: bfloat16 [8192], P('tp')
- bias_bc: bfloat16 [2, 1024], P(None, 'tp')
- a_log: float32 [128], P('tp')
- dt_bias: float32 [128], P('tp')
- d_skip: float32 [128], P('tp')
- norm_w: bfloat16 [8192], P('tp')
- w_out: bfloat16 [8192, 4096], P('tp')
Outputs:
- output: bfloat16 [32768, 4096], P(('dp', 'sp', 'tp')), parts along dimension 0
There are 2 independent parts. The reference program is written for one: setup_inputs(seed, part) draws one part's arguments, and reference() takes and returns one part's arrays. A program takes and returns all parts, laid end to end along the dimension named above; an argument that names none is the same for every part.
All inputs are finite; a program needn't handle non-finite values.
Results may differ from the reference program's by a relative error of at most 0.00663.
Values are sent between devices in bfloat16 or wider.
A program may use at most 1 GiB of HBM per device.

```python
import math
import jax
import jax.numpy as jnp
from jax import lax

D_MODEL = 4096
NUM_HEADS = 128
NUM_GROUPS = 8
TOK_DEV = 1024
SEQ_SHARDS = 4
HEAD_SHARDS = 4
HEAD_DIM = 64
STATE_DIM = 128
CONV_WIDTH = 4
SSD_TILE = 256
NORM_EPS = 1e-5
SEQ_LEN = TOK_DEV * SEQ_SHARDS * HEAD_SHARDS
BLOCK_LEN = TOK_DEV * HEAD_SHARDS
INNER_DIM = NUM_HEADS * HEAD_DIM
GROUP_WIDTH = NUM_GROUPS * STATE_DIM
PER_GROUP = NUM_HEADS // NUM_GROUPS


def setup_inputs(seed: int = 0, part: int = 0) -> dict:
    shared = jax.random.split(jax.random.key(seed), 12)
    part_key = jax.random.fold_in(jax.random.key(seed + 1), part)
    key_x, key_seg, key_pos = jax.random.split(part_key, 3)
    x_in = jax.random.normal(key_x, (SEQ_LEN, D_MODEL), jnp.float32)
    start_draw = jax.random.randint(key_seg, (SEQ_LEN,), 0, BLOCK_LEN)
    forced_pos = jax.random.randint(key_pos, (), 1, SEQ_LEN)
    is_start = (start_draw == 0) | (jnp.arange(SEQ_LEN) == forced_pos)
    seg_ids = jnp.cumsum(is_start.astype(jnp.int32)).astype(jnp.int32)
    in_scale = D_MODEL ** -0.5
    w_zx = jax.random.normal(shared[0], (D_MODEL, 2, INNER_DIM), jnp.float32) * in_scale
    w_bc = jax.random.normal(shared[1], (D_MODEL, 2, GROUP_WIDTH), jnp.float32) * in_scale
    w_dt = jax.random.normal(shared[2], (D_MODEL, NUM_HEADS), jnp.float32) * in_scale
    conv_x = jax.random.normal(shared[3], (CONV_WIDTH, INNER_DIM), jnp.float32) * 0.5
    conv_bc = jax.random.normal(shared[4], (CONV_WIDTH, 2, GROUP_WIDTH), jnp.float32) * 0.5
    bias_x = jax.random.normal(shared[5], (INNER_DIM,), jnp.float32) * 0.5
    bias_bc = jax.random.normal(shared[6], (2, GROUP_WIDTH), jnp.float32) * 0.5
    a_base = math.log(0.5 * math.sqrt(STATE_DIM / BLOCK_LEN))
    dt_base = math.log(1.0 / math.sqrt(BLOCK_LEN * STATE_DIM))
    a_log = a_base + jax.random.uniform(shared[7], (NUM_HEADS,), jnp.float32, -0.5, 0.5)
    dt_bias = dt_base + jax.random.uniform(shared[8], (NUM_HEADS,), jnp.float32, -0.5, 0.5)
    d_skip = jax.random.uniform(shared[9], (NUM_HEADS,), jnp.float32, 0.5, 1.5)
    norm_w = jax.random.uniform(shared[10], (INNER_DIM,), jnp.float32, 0.5, 1.5)
    w_out = jax.random.normal(shared[11], (INNER_DIM, D_MODEL), jnp.float32) * INNER_DIM ** -0.5
    return {'x_in': x_in.astype(jnp.bfloat16), 'seg_ids': seg_ids, 'w_zx': w_zx.astype(jnp.bfloat16), 'w_bc': w_bc.astype(jnp.bfloat16), 'w_dt': w_dt.astype(jnp.bfloat16), 'conv_x': conv_x.astype(jnp.bfloat16), 'conv_bc': conv_bc.astype(jnp.bfloat16), 'bias_x': bias_x.astype(jnp.bfloat16), 'bias_bc': bias_bc.astype(jnp.bfloat16), 'a_log': a_log, 'dt_bias': dt_bias, 'd_skip': d_skip, 'norm_w': norm_w.astype(jnp.bfloat16), 'w_out': w_out.astype(jnp.bfloat16)}


def reference(x_in, seg_ids, w_zx, w_bc, w_dt, conv_x, conv_bc, bias_x, bias_bc, a_log, dt_bias, d_skip, norm_w, w_out):
    halo_len = CONV_WIDTH - 1
    n_tiles = SEQ_LEN // SSD_TILE
    last_row = SSD_TILE - 1
    conv_w = jnp.concatenate([conv_x, conv_bc.reshape(CONV_WIDTH, 2 * GROUP_WIDTH)], axis=1).astype(jnp.float32)
    conv_b = jnp.concatenate([bias_x, bias_bc.reshape(2 * GROUP_WIDTH)]).astype(jnp.float32)
    decay_rate = jnp.exp(a_log).reshape(NUM_GROUPS, PER_GROUP)
    skip_gain = d_skip.reshape(NUM_GROUPS, PER_GROUP)
    w_zx_flat = w_zx.reshape(D_MODEL, 2 * INNER_DIM)
    w_bc_flat = w_bc.reshape(D_MODEL, 2 * GROUP_WIDTH)
    norm_gain = norm_w.astype(jnp.float32)
    causal = jnp.arange(SSD_TILE)[:, None] >= jnp.arange(SSD_TILE)[None, :]

    def step(carry, inputs):
        xbc_tail, seg_tail, state = carry
        x_tile, seg_tile = inputs
        zx_proj = jnp.dot(x_tile, w_zx_flat, preferred_element_type=jnp.float32).astype(jnp.bfloat16)
        bc_pre = jnp.dot(x_tile, w_bc_flat, preferred_element_type=jnp.float32).astype(jnp.bfloat16)
        dt_raw = jnp.dot(x_tile, w_dt, preferred_element_type=jnp.float32).astype(jnp.bfloat16)
        xbc = jnp.concatenate([zx_proj[:, INNER_DIM:], bc_pre], axis=1)
        padded = jnp.concatenate([xbc_tail, xbc], axis=0).astype(jnp.float32)
        seg_pad = jnp.concatenate([seg_tail, seg_tile])
        conv_acc = conv_b
        for tap_idx in range(CONV_WIDTH):
            keep_tap = (seg_pad[tap_idx:tap_idx + SSD_TILE] == seg_tile)[:, None]
            conv_acc = conv_acc + jnp.where(keep_tap, padded[tap_idx:tap_idx + SSD_TILE] * conv_w[tap_idx], 0.0)
        conv_act = jax.nn.silu(conv_acc).astype(jnp.bfloat16).astype(jnp.float32)
        x_ssm = conv_act[:, :INNER_DIM].reshape(SSD_TILE, NUM_GROUPS, PER_GROUP, HEAD_DIM)
        b_ssm = conv_act[:, INNER_DIM:INNER_DIM + GROUP_WIDTH].reshape(SSD_TILE, NUM_GROUPS, STATE_DIM)
        c_ssm = conv_act[:, INNER_DIM + GROUP_WIDTH:].reshape(SSD_TILE, NUM_GROUPS, STATE_DIM)
        dt_val = jax.nn.softplus(dt_raw.astype(jnp.float32) + dt_bias).reshape(SSD_TILE, NUM_GROUPS, PER_GROUP)
        log_a = -decay_rate * dt_val
        seg_prev = seg_tail[halo_len - 1]
        cum_log = jnp.cumsum(log_a, axis=0)
        same_doc = ((seg_tile[:, None] == seg_tile[None, :]) & causal)[:, :, None, None]
        decay = jnp.where(same_doc, jnp.exp(jnp.where(same_doc, cum_log[:, None] - cum_log[None, :], 0.0)), 0.0)
        scores = jnp.einsum('tgn,sgn->tsg', c_ssm, b_ssm)
        mix_mat = scores[..., None] * decay * dt_val[None]
        y_ssm = jnp.einsum('tsgr,sgrp->tgrp', mix_mat, x_ssm)
        keep_in = (seg_tile == seg_prev)[:, None, None]
        y_ssm = y_ssm + jnp.einsum('tgn,grpn->tgrp', c_ssm, state) * jnp.where(keep_in, jnp.exp(cum_log), 0.0)[..., None]
        y_ssm = y_ssm + skip_gain[None, :, :, None] * x_ssm
        keep_end = (seg_tile == seg_tile[last_row])[:, None, None]
        end_w = jnp.where(keep_end, jnp.exp(cum_log[last_row][None] - cum_log), 0.0) * dt_val
        carry_fac = jnp.where(seg_tile[last_row] == seg_prev, jnp.exp(cum_log[last_row]), 0.0)
        state = carry_fac[:, :, None, None] * state + jnp.einsum('sgrp,sgn->grpn', x_ssm * end_w[..., None], b_ssm)
        gate_val = jax.nn.silu(zx_proj[:, :INNER_DIM].astype(jnp.float32))
        gated = (y_ssm.reshape(SSD_TILE, INNER_DIM) * gate_val).reshape(SSD_TILE, NUM_GROUPS, INNER_DIM // NUM_GROUPS)
        normed = gated * lax.rsqrt(jnp.mean(gated * gated, axis=-1, keepdims=True) + NORM_EPS)
        y_norm = (normed.reshape(SSD_TILE, INNER_DIM) * norm_gain).astype(jnp.bfloat16)
        out_proj = jnp.dot(y_norm, w_out, preferred_element_type=jnp.float32)
        y_tile = (x_tile.astype(jnp.float32) + out_proj).astype(jnp.bfloat16)
        return (xbc[SSD_TILE - halo_len:], seg_tile[SSD_TILE - halo_len:], state), y_tile

    init_carry = (jnp.zeros((halo_len, INNER_DIM + 2 * GROUP_WIDTH), jnp.bfloat16), jnp.zeros((halo_len,), jnp.int32), jnp.zeros((NUM_GROUPS, PER_GROUP, HEAD_DIM, STATE_DIM), jnp.float32))
    tiles_in = (x_in.reshape(n_tiles, SSD_TILE, D_MODEL), seg_ids.reshape(n_tiles, SSD_TILE))
    scan_out = lax.scan(step, init_carry, tiles_in)
    return scan_out[1].reshape(SEQ_LEN, D_MODEL)
```

```python
import functools
import jax
import jax.numpy as jnp
from jax import lax
from jax.sharding import PartitionSpec as P
from jax.experimental import pallas as pl
from jax.experimental.pallas import tpu as pltpu

T = 128
XW = 2048
NB = 512
GW = 1024
D = 4096
TOK = 1024
HEADS, HEAD = 32, 64
XT = 512
MT = 256
HALO = 16
SUB = 8
MH = MT + HALO
LOG2E = 1.4426950408889634
NORM_EPS = 1e-5
MIB = 2**20
f32, bf16 = jnp.float32, jnp.bfloat16
MESH = pl.DeviceIdType.MESH
ONE = pl.Buffered(1)


def silu(v):
    h = 0.5 * v
    return h + h * jnp.tanh(h)


def lane_bcast(cols, h):
    return jnp.broadcast_to(cols[:, h:h + 1], (cols.shape[0], T))


def pair_bcast(cols, p):
    lanes = lax.broadcasted_iota(jnp.int32, (cols.shape[0], T), 1)
    return jnp.where(lanes < HEAD, lane_bcast(cols, 2 * p), lane_bcast(cols, 2 * p + 1))


def row(ref, r):
    return ref[r:r + 1, :]


def mac(a, b, ca=1, cb=0, **kw):
    return lax.dot_general(a, b, (((ca,), (cb,)), ((), ())), preferred_element_type=f32, **kw)


def rows_from(start, size):
    return pl.ds(start if isinstance(start, int) else pl.multiple_of(start, 16), size)


def front_kernel(pre, *refs, nx, per, hrows):
    xs_, hs_, auxs = refs[:nx], refs[nx:2 * nx], refs[2 * nx:3 * nx]
    (wx_ref, wb_ref, wdt_ref, cin_ref, cw_ref, cwb_ref, hp_ref,
     xa_ref, bca_ref, dc_ref, cout_ref, xbuf, pbuf, bbuf, xw, bt, cum_all, wgt, abuf, sem) = refs[3 * nx:]
    n = pl.program_id(0)
    last_n = XW // XT
    nm = nx * per
    rows = lax.broadcasted_iota(jnp.int32, (T, T), 0)
    cols = lax.broadcasted_iota(jnp.int32, (T, T), 1)
    tiles = [slice(t * T, (t + 1) * T) for t in range(MT // T)]

    def copies(m):
        i, s = divmod(m, per)
        if s:
            return [pltpu.make_async_copy(xs_[i].at[rows_from(s * MT - HALO, MH)], xbuf.at[m], sem.at[m])]
        return [pltpu.make_async_copy(hs_[i].at[rows_from(hrows[i](pre), HALO)], xbuf.at[m, pl.ds(0, HALO)], sem.at[m]),
                pltpu.make_async_copy(xs_[i].at[pl.ds(0, MT)], xbuf.at[m, pl.ds(HALO, MT)], sem.at[m])]

    def left(i):
        return slice(nm * MT + SUB * (i + 1), nm * MT + SUB * (i + 2))

    def heads_first(v):
        return pltpu.roll(v, lax.rem(T - (XT // HEAD) * (n - 1), T), 1)

    def at(m, ts):
        return pl.ds(pl.multiple_of(m * MT + ts.start, T), T)

    def conv(read, lo, w, keep):
        cs = slice(lo, lo + T)
        acc = read(0, cs) * row(w, 3)[:, cs] + row(w, 4)[:, cs]
        for k in range(3):
            acc = acc + (read(3 - k, cs) * w[k:k + 1, cs]) * keep[k]
        return silu(acc).astype(bf16)

    def taps(m, ts):
        return [lane_bcast(abuf[m, ts, :], 2 - k) for k in range(3)]

    def x_dot(m):
        pbuf[lax.rem(n, 2), m] = jnp.dot(xbuf[m], wx_ref[...], preferred_element_type=f32).astype(bf16).astype(f32)

    def setup(m, i, s):
        for ts in tiles:
            r0 = HALO + ts.start
            keep = taps(m, ts)
            for c in range(NB // T):
                act = conv(lambda d, cs: bbuf[r0 - d:r0 - d + T, cs], c * T, cwb_ref, keep)
                bca_ref[at(m, ts), c * T:(c + 1) * T] = act
                if c < 2:
                    bt[i, c, :, at(s, ts)] = act.T
            raw = bbuf[r0:r0 + T, NB:NB + T] + row(hp_ref, 0)
            dtv = jnp.maximum(raw, 0.0) + jnp.log1p(jnp.exp(-jnp.abs(raw)))
            log_a = -jnp.exp(row(hp_ref, 1)) * dtv * LOG2E
            cum = mac((rows >= cols).astype(f32), log_a, precision=lax.Precision.HIGHEST)
            dc_ref[at(m, ts), :] = jnp.where(cols < HEADS, cum, pltpu.roll(dtv, HEADS, 1))
            before = jnp.where((s == 0) & (ts.start == 0), 0.0, row(cum_all, nm * MT))
            cum = cum + before
            cum_all[at(m, ts), :] = cum
            cum_all[nm * MT:nm * MT + SUB, :] = jnp.broadcast_to(cum[T - 1:T, :], (8, T))
            wgt[at(m, ts), :] = dtv

    def weigh(i):
        lo, end = i * per * MT, (i + 1) * per * MT
        doc = abuf[end // MT - 1, MT - 1:MT, 5:6]
        last = row(cum_all, end - 1)
        keep_in = abuf[lo // MT, 0:1, 0:1] * (abuf[lo // MT, 0:1, 5:6] == doc).astype(f32)
        carry = jnp.broadcast_to(jnp.exp2(last) * keep_in, (8, T))
        for r in range(lo, end, T):
            keep = jnp.broadcast_to((abuf[r // MT, r % MT:r % MT + T, 5:6] == doc).astype(f32), (T, T))
            wgt[r:r + T, :] = jnp.exp2(last - cum_all[r:r + T, :]) * wgt[r:r + T, :] * keep
        cum_all[left(i), :] = carry

    def x_conv(m):
        slot = lax.rem(n + 1, 2)
        for ts in tiles:
            r0 = HALO + ts.start
            keep = taps(m, ts)
            wg = heads_first(wgt[at(m, ts), :])
            for p in range(XT // T):
                cs = slice(p * T, (p + 1) * T)
                xa = conv(lambda d, cs: pbuf[slot, m, r0 - d:r0 - d + T, cs], p * T, cw_ref, keep)
                xa_ref[at(m, ts), cs] = xa
                xw[at(m, ts), cs] = (xa.astype(f32) * pair_bcast(wg, p)).astype(bf16)

    def end_state():
        g = (n - 1) // (GW // XT)
        for i in range(nx):
            upd = jnp.dot(bt[i, g], xw[i * per * MT:(i + 1) * per * MT, :], preferred_element_type=f32)
            cr = heads_first(cum_all[left(i), :])
            for p in range(XT // T):
                cs = slice(p * T, (p + 1) * T)
                carry = pair_bcast(cr, p)
                cout_ref[i, 0:T, cs] = cin_ref[i, 0:T, cs] * jnp.broadcast_to(carry[0:1], (T, T)) + upd[:, cs]
                cout_ref[i, T:T + 8, cs] = cin_ref[i, T:T + 8, cs] * carry

    @pl.when(n == 0)
    def _():
        for m in range(nm):
            for c in copies(m):
                c.start()
        bbuf[:, NB:] = jnp.zeros((MH, T), f32)
        for m in range(nm):
            i, s = divmod(m, per)
            abuf[m] = auxs[i][s * MT:(s + 1) * MT, :]

        @pl.loop(0, nm)
        def _(m):
            for k in range(nm):
                @pl.when(m == k)
                def _():
                    for c in copies(k):
                        c.wait()
            bbuf[:, 0:NB] = jnp.dot(xbuf[m], wb_ref[...], preferred_element_type=f32).astype(bf16).astype(f32)
            bbuf[:, NB:NB + HEADS] = jnp.dot(xbuf[m], wdt_ref[...], preferred_element_type=f32).astype(bf16).astype(f32)
            x_dot(m)
            setup(m, m // per, lax.rem(m, per))

        for i in range(nx):
            weigh(i)

    @pl.when((n > 0) & (n < last_n))
    def _():
        @pl.loop(0, nm)
        def _(m):
            x_dot(m)
            x_conv(m)

    @pl.when(n == last_n)
    def _():
        @pl.loop(0, nm)
        def _(m):
            x_conv(m)

    @pl.when(n > 0)
    def _():
        end_state()


def front_call(pre, aux, amaps, xs, halos, hrows, weights, cin, consts, *, per):
    nx = len(xs)
    nm = nx * per
    n = nm * MT
    nt = XW // XT
    w2, wb, wdt = weights
    hbm = pl.BlockSpec(memory_space=pl.ANY)
    prev = lambda j: jnp.maximum(j - 1, 0)
    whole = lambda *shape, mode=ONE: pl.BlockSpec(shape, lambda j, b: (0,) * len(shape), pipeline_mode=mode)
    cols = lambda k: pl.BlockSpec((k, XT), lambda j, b: (0, prev(j)))
    state = pl.BlockSpec((nx, T + 8, XT), lambda j, b: (0, 0, prev(j)))
    in_specs = [hbm] * (2 * nx) + [pl.BlockSpec((per * MT, T), lambda j, b, f=f: (f(b), 0), pipeline_mode=ONE) for f in amaps] + [
        pl.BlockSpec((D, XT), lambda j, b: (0, nt + jnp.minimum(j, nt - 1))), whole(D, NB), whole(D, HEADS),
        state, cols(8), whole(8, NB), whole(8, T)]
    gs = pltpu.PrefetchScalarGridSpec(
        num_scalar_prefetch=1, grid=(nt + 1,), in_specs=in_specs,
        out_specs=[cols(n), whole(n, NB, mode=None), whole(n, T, mode=None), state],
        scratch_shapes=[pltpu.VMEM((nm, MH, D), bf16), pltpu.VMEM((2, nm, MH, XT), f32), pltpu.VMEM((MH, NB + T), f32),
                        pltpu.VMEM((n, XT), bf16), pltpu.VMEM((nx, 2, T, per * MT), bf16),
                        pltpu.VMEM((n + 8 * (nx + 1), T), f32), pltpu.VMEM((n, T), f32), pltpu.VMEM((nm, MT, T), f32),
                        pltpu.SemaphoreType.DMA((nm,))],
    )
    return pl.pallas_call(
        functools.partial(front_kernel, nx=nx, per=per, hrows=hrows), grid_spec=gs,
        out_shape=[jax.ShapeDtypeStruct((n, XW), bf16), jax.ShapeDtypeStruct((n, NB), bf16),
                   jax.ShapeDtypeStruct((n, T), f32), jax.ShapeDtypeStruct((nx, T + 8, XW), f32)],
        compiler_params=pltpu.CompilerParams(dimension_semantics=("arbitrary",), vmem_limit_bytes=62 * MIB),
        cost_estimate=pl.CostEstimate(flops=n * 25_000_000, bytes_accessed=n * 10000, transcendentals=n * 4096),
        name="front",
    )(pre, *xs, *halos, *[aux] * nx, w2, wb, wdt, cin, *consts)


def mixz_kernel(pre, *refs, nx):
    xs_, auxs = refs[:nx], refs[nx:2 * nx]
    (xa_ref, bg_ref, cg_ref, dc_ref, wz_ref, cin_ref, hp_ref, yn_ref, cout_ref, xv, av, zbuf, ybuf, xw, state) = refs[2 * nx:]
    g, i, tile = pl.program_id(0), pl.program_id(1), pl.program_id(2)
    n_tiles = pl.num_programs(2)

    @pl.when(tile == 0)
    def _():
        state[...] = cin_ref[0]

    for k in range(nx):
        @pl.when(i == k)
        def _():
            xv[...] = xs_[k][...]
            av[...] = auxs[k][...]

    zbuf[...] = jnp.dot(xv[...], wz_ref[...], preferred_element_type=f32).astype(bf16).astype(f32)
    rows = lax.broadcasted_iota(jnp.int32, (T, T), 0)
    cols = lax.broadcasted_iota(jnp.int32, (T, T), 1)
    lo_half = cols < 64
    zero = jnp.zeros((T, T), bf16)
    for t in range(MT // T):
        rs = slice(t * T, (t + 1) * T)
        aux = av[rs, :]
        auxt = aux.T
        mask = (rows >= cols) & (lane_bcast(aux, 5) == jnp.broadcast_to(auxt[5:6, :], (T, T)))
        k_in = lane_bcast(aux, 3)
        k_end = lane_bcast(aux, 4)
        dc = pltpu.roll(dc_ref[rs, :], lax.rem(T - 16 * g, T), 1)
        dct = dc.T
        rel = dct[:HEADS // 2, :] - jnp.log2(dct[HEADS:HEADS + HEADS // 2, :])
        bg, cg = bg_ref[rs, :], cg_ref[rs, :]
        sm = jnp.where(mask, mac(cg, bg, 1, 1), 0.0)
        ybuf[...] = mac(cg, state[...].astype(bf16))
        sq = jnp.zeros((T, T), f32)
        for p in range(GW // T):
            cs = slice(p * T, (p + 1) * T)
            xa = xa_ref[rs, cs]
            xaf = xa.astype(f32)
            c0, c1 = lane_bcast(dc, 2 * p), lane_bcast(dc, 2 * p + 1)
            mixes = []
            for hh, cb in ((2 * p, c0), (2 * p + 1, c1)):
                diff = jnp.minimum(cb - jnp.broadcast_to(rel[hh:hh + 1, :], (T, T)), 126.0)
                mixes.append((sm * jnp.exp2(diff)).astype(bf16))
            lhs = jnp.concatenate(mixes, axis=1)
            rhs = jnp.concatenate([jnp.where(lo_half, xa, zero), jnp.where(lo_half, zero, xa)], axis=0)
            y = mac(lhs, rhs)
            cump = jnp.where(lo_half, c0, c1)
            dtp = pair_bcast(dc, HEADS // 2 + p)
            last = cump[T - 1:T, :]
            xw[:, cs] = (xaf * (jnp.exp2(last - cump) * dtp * k_end)).astype(bf16)
            y = y + ybuf[:, cs] * (jnp.exp2(cump) * k_in) + hp_ref[0:1, cs] * xaf
            v = y * silu(zbuf[rs, cs])
            ybuf[:, cs] = v
            sq = sq + v * v
            state[:, cs] = state[:, cs] * (jnp.exp2(last) * k_in[T - 1:T, :])
        ms = jnp.sum(sq, axis=1, keepdims=True) * (1.0 / GW)
        r = jnp.broadcast_to(lax.rsqrt(ms + NORM_EPS), (T, T))
        for p in range(GW // T):
            cs = slice(p * T, (p + 1) * T)
            yn_ref[rs, cs] = (ybuf[:, cs] * r * hp_ref[1:2, cs]).astype(bf16)
        state[...] = state[...] + mac(bg, xw[...], 0, 0)

    @pl.when(tile == n_tiles - 1)
    def _():
        cout_ref[0] = state[...]


def mixz_call(pre, aux, amaps, xs, arrs, w2, cin, hp, *, per, cofs):
    nx = len(xs)
    n = nx * per * MT
    xa, bca, dc = arrs
    piece = lambda k: (lambda g, i, t: jnp.clip((i - k) * per + t, 0, per - 1))
    rows = lambda w, c: pl.BlockSpec((MT, w), lambda g, i, t, b: (i * per + t, c(g)))
    state = lambda ofs: pl.BlockSpec((1, T, GW), lambda g, i, t, b: (ofs + i, 0, g))
    cols = lambda k: pl.BlockSpec((k, GW), lambda g, i, t, b: (0, g))
    in_specs = [pl.BlockSpec((MT, D), lambda g, i, t, b, k=k: (piece(k)(g, i, t), 0)) for k in range(nx)]
    in_specs += [pl.BlockSpec((MT, T), lambda g, i, t, b, k=k: (amaps[k](b) * per + piece(k)(g, i, t), 0)) for k in range(nx)]
    same = lambda g: g
    in_specs += [rows(GW, same), rows(T, same), rows(T, lambda g: 2 + g), rows(T, lambda g: 0), cols(D), state(cofs), cols(8)]
    gs = pltpu.PrefetchScalarGridSpec(
        num_scalar_prefetch=1, grid=(2, nx, per), in_specs=in_specs, out_specs=[rows(GW, same), state(0)],
        scratch_shapes=[pltpu.VMEM((MT, D), bf16), pltpu.VMEM((MT, T), f32), pltpu.VMEM((MT, GW), f32), pltpu.VMEM((T, GW), f32),
                        pltpu.VMEM((T, GW), bf16), pltpu.VMEM((T, GW), f32)],
    )
    return pl.pallas_call(
        functools.partial(mixz_kernel, nx=nx), grid_spec=gs,
        out_shape=[jax.ShapeDtypeStruct((n, XW), bf16), jax.ShapeDtypeStruct((nx, T, XW), f32)],
        compiler_params=pltpu.CompilerParams(dimension_semantics=("arbitrary",) * 3, vmem_limit_bytes=60 * MIB),
        cost_estimate=pl.CostEstimate(flops=n * 20_000_000, bytes_accessed=n * 14000, transcendentals=n * 10000),
        name="mixz",
    )(pre, *xs, *[aux] * nx, xa, bca, bca, dc, w2, cin, hp)


def seq_slot(me, s):
    c = (me % 2 + s % 2) % 2
    y = (me // 2 + s // 2) % 2
    return 2 * y + c


def count(flag):
    return jnp.where(flag, 1, 0)


def ahead_kernel(n_blocks, seg_ref, tail_ref, segs_ref, tails_ref, send_sem, recv_sem):
    me, blk = lax.axis_index('tp'), lax.axis_index('sp')
    barrier = pltpu.get_barrier_semaphore()
    others = [{'tp': seq_slot(me, s)} for s in (1, 2, 3)]
    before = {'sp': jnp.maximum(blk - 1, 0), 'tp': 3}
    after = [{'sp': jnp.minimum(blk + 1, n_blocks - 1), 'tp': q} for q in range(4)]
    sends_on = (me == 3) & (blk < n_blocks - 1)
    for dev in others:
        pl.semaphore_signal(barrier, inc=1, device_id=dev, device_id_type=MESH)

    @pl.when(blk > 0)
    def _():
        pl.semaphore_signal(barrier, inc=1, device_id=before, device_id_type=MESH)

    @pl.when(sends_on)
    def _():
        for dev in after:
            pl.semaphore_signal(barrier, inc=1, device_id=dev, device_id_type=MESH)

    pl.semaphore_wait(barrier, 3 + count(blk > 0) + 4 * count(sends_on))

    def copies(dev, entry, k, rk):
        return [pltpu.make_async_remote_copy(src_ref=seg_ref, dst_ref=segs_ref.at[entry], send_sem=send_sem.at[k, 0],
                                             recv_sem=recv_sem.at[rk, 0], device_id=dev, device_id_type=MESH),
                pltpu.make_async_remote_copy(src_ref=tail_ref, dst_ref=tails_ref.at[entry], send_sem=send_sem.at[k, 1],
                                             recv_sem=recv_sem.at[rk, 1], device_id=dev, device_id_type=MESH)]

    inner = [copies(dev, me + 1, k, k) for k, dev in enumerate(others)]
    outer = [copies(dev, 0, 3 + q, 3) for q, dev in enumerate(after)]
    for cs in inner:
        for c in cs:
            c.start()

    @pl.when(sends_on)
    def _():
        for cs in outer:
            for c in cs:
                c.start()

    segs_ref[me + 1] = seg_ref[...]
    tails_ref[me + 1] = tail_ref[...]

    @pl.when(blk == 0)
    def _():
        segs_ref[0] = jnp.zeros_like(seg_ref)
        tails_ref[0] = jnp.zeros_like(tail_ref)

    for cs in inner:
        for c in cs:
            c.wait_send()
            c.wait_recv()

    @pl.when(sends_on)
    def _():
        for cs in outer:
            for c in cs:
                c.wait_send()

    @pl.when(blk > 0)
    def _():
        for c in outer[0]:
            c.wait_recv()


def ahead_call(seg, x, n_blocks):
    rows = x.shape[0]
    vmem = pl.BlockSpec(memory_space=pltpu.VMEM)
    return pl.pallas_call(
        functools.partial(ahead_kernel, n_blocks),
        grid=(1,),
        in_specs=[vmem, pl.BlockSpec((HALO, D), lambda i: (rows // HALO - 1, 0))],
        out_specs=[vmem, vmem],
        out_shape=[jax.ShapeDtypeStruct((5, rows // T, T), jnp.int32), jax.ShapeDtypeStruct((5, HALO, D), bf16)],
        scratch_shapes=[pltpu.SemaphoreType.DMA((7, 2)), pltpu.SemaphoreType.DMA((4, 2))],
        compiler_params=pltpu.CompilerParams(collective_id=0, has_side_effects=True, vmem_limit_bytes=16 * MIB),
        name="ahead",
    )(seg.reshape(rows // T, T), x)


CW = 256


def chain_kernel(n_blocks, e01_ref, e2_ref, e3_ref, out_ref, ebuf, sbuf, obuf, lsem, send_sem, recv_sem):
    me, blk = lax.axis_index('tp'), lax.axis_index('sp')
    srcs = [e01_ref.at[0], e01_ref.at[1], e2_ref.at[0], e3_ref.at[0]]
    loads = [pltpu.make_async_copy(src, ebuf.at[seq_slot(me, s)], lsem.at[s]) for s, src in enumerate(srcs)]
    for c in loads:
        c.start()
    barrier = pltpu.get_barrier_semaphore()
    before = {'sp': jnp.maximum(blk - 1, 0)}
    after = {'sp': jnp.minimum(blk + 1, n_blocks - 1)}

    @pl.when(blk > 0)
    def _():
        pl.semaphore_signal(barrier, inc=1, device_id=before, device_id_type=MESH)

    @pl.when(blk < n_blocks - 1)
    def _():
        pl.semaphore_signal(barrier, inc=1, device_id=after, device_id_type=MESH)

    pl.semaphore_wait(barrier, count(blk > 0) + count(blk < n_blocks - 1))

    for c in loads:
        c.wait()

    def through(q, s, cs):
        return ebuf[q, :T, cs] + ebuf[q, T:T + 1, cs] * s

    for q in (1, 2, 3):
        ebuf[q, :T, :] = through(q, ebuf[q - 1, :T, :], slice(None))
        ebuf[q, T:, :] = ebuf[q, T:, :] * ebuf[q - 1, T:, :]

    @pl.when(blk == 0)
    def _():
        sbuf[...] = jnp.zeros_like(sbuf)

    n = XW // CW

    def send(j):
        return pltpu.make_async_remote_copy(src_ref=obuf.at[j], dst_ref=sbuf.at[j], send_sem=send_sem.at[j],
                                            recv_sem=recv_sem.at[j], device_id=after, device_id_type=MESH)

    for j in range(n):
        cs = slice(j * CW, (j + 1) * CW)

        @pl.when(blk > 0)
        def _():
            send(j).wait_recv()

        @pl.when(blk < n_blocks - 1)
        def _():
            obuf[j] = through(3, sbuf[j], cs)
            send(j).start()

    for j in range(n):
        cs = slice(j * CW, (j + 1) * CW)
        for q in range(4):
            v = through(q - 1, sbuf[j], cs) if q else sbuf[j]
            out_ref[seq_slot(me, q), :, cs] = v

    @pl.when(blk < n_blocks - 1)
    def _():
        for j in range(n):
            send(j).wait_send()


def chain_call(e01, e2, e3, n_blocks):
    hbm = pl.BlockSpec(memory_space=pl.ANY)
    n = XW // CW
    return pl.pallas_call(
        functools.partial(chain_kernel, n_blocks),
        in_specs=[hbm] * 3,
        out_specs=pl.BlockSpec(memory_space=pltpu.VMEM),
        out_shape=jax.ShapeDtypeStruct((4, T, XW), f32),
        scratch_shapes=[pltpu.VMEM((4, T + SUB, XW), f32), pltpu.VMEM((n, T, CW), f32), pltpu.VMEM((n, T, CW), f32),
                        pltpu.SemaphoreType.DMA((4,)), pltpu.SemaphoreType.DMA((n,)), pltpu.SemaphoreType.DMA((n,))],
        compiler_params=pltpu.CompilerParams(collective_id=1, has_side_effects=True, vmem_limit_bytes=40 * MIB),
        name="chain",
    )(e01, e2, e3)


NT = 512


def out_kernel(y_ref, yr_ref, w_ref, wr0_ref, wr1_ref, *refs):
    h = XW // 2
    acc = (jnp.dot(y_ref[...], w_ref[...], preferred_element_type=f32)
           + jnp.dot(yr_ref[:, 0:h], wr0_ref[...], preferred_element_type=f32)
           + jnp.dot(yr_ref[:, h:], wr1_ref[...], preferred_element_type=f32))
    if len(refs) > 1:
        x_ref, other_ref = refs[:2]
        acc = x_ref[...].astype(f32) + (acc + other_ref[...])
    refs[-1][...] = acc.astype(refs[-1].dtype)


def out_call(run, part, y, yr, w, wr, x=None, other=None, into=None):
    rows = yr.shape[0]
    h = XW // 2
    at = lambda r: (lambda j: (r, j))
    cols = at(0)
    ins = [y, yr, w, *wr]
    specs = [pl.BlockSpec((rows, XW), lambda j: (run * (TOK // rows) + part, 0), pipeline_mode=ONE),
             pl.BlockSpec((rows, XW), lambda j: (0, 0), pipeline_mode=ONE),
             pl.BlockSpec((XW, NT), cols), pl.BlockSpec((h, NT), cols), pl.BlockSpec((h, NT), cols)]
    alias = {}
    if x is not None:
        ins += [x, other]
        specs += [pl.BlockSpec((rows, NT), at(part)), pl.BlockSpec((rows, NT), cols)]
    if into is not None:
        alias = {len(ins): 0}
        ins.append(into)
        specs.append(pl.BlockSpec(memory_space=pl.ANY))
    return pl.pallas_call(
        out_kernel,
        grid=(D // NT,), in_specs=specs,
        out_specs=pl.BlockSpec((rows, NT), cols if x is None else at(part)),
        out_shape=jax.ShapeDtypeStruct((rows, D), f32) if x is None else jax.ShapeDtypeStruct(x.shape, bf16),
        input_output_aliases=alias,
        compiler_params=pltpu.CompilerParams(dimension_semantics=("arbitrary",), vmem_limit_bytes=56 * MIB),
        cost_estimate=pl.CostEstimate(flops=rows * 33_000_000, bytes_accessed=rows * 100000, transcendentals=0),
        name="out_proj",
    )(*ins)


def send(v, perm):
    return lax.ppermute(v, 'tp', perm)


def after(v, *deps):
    return lax.optimization_barrier((v,) + deps)[0]


NCH = 2
CORE_SWAP = [(i, i ^ 1) for i in range(4)]
CHIP_SWAP = [(i, i ^ 2) for i in range(4)]


def token_aux(seg_ext):
    seg = seg_ext[3:]
    n = seg.shape[0]
    tile_prev = jnp.repeat(seg_ext[2:n + 2:T], T)
    tile_last = jnp.repeat(seg[T - 1::T], T)
    cols = [seg == seg_ext[3 - k:n + 3 - k] for k in (1, 2, 3)] + [seg == tile_prev, seg == tile_last, seg - seg_ext[0]]
    lane = lax.broadcasted_iota(jnp.int32, (n, T), 1)
    out = jnp.zeros((n, T), f32)
    for i, c in enumerate(cols):
        out = jnp.where(lane == i, c.astype(f32)[:, None], out)
    return out


def solution(mesh):
    n_blocks = mesh.shape['sp']
    token_spec = seg_spec = P(('dp', 'sp', 'tp'))
    weight_specs = tuple(P(*['tp' if i == dim else None for i in range(dim + 1)]) for dim in (2, 2, 1, 1, 2, 0, 1, 0, 0, 0, 0, 0))

    def body(x_loc, seg_loc, w_zx, w_bc, w_dt, conv_x, conv_bc, bias_x, bias_bc, a_log, dt_bias, d_skip, norm_w, w_out):
        rows, d = x_loc.shape
        me, blk = lax.axis_index('tp'), lax.axis_index('sp')
        ch = rows // NCH
        per, kper = rows // MT, ch // MT
        segs, tails = ahead_call(seg_loc, x_loc, n_blocks)
        x_snd, segs = lax.optimization_barrier((x_loc, segs))
        x_par = send(x_snd, CORE_SWAP)
        parts = [x_snd[:ch]]
        parts.append(after(x_snd, parts[0])[ch:])
        x_dir = [send(v, CHIP_SWAP) for v in parts]
        place = lax.axis_index('dp') * n_blocks + blk
        half = w_out.shape[0] // 2
        step = half // (mesh.shape['dp'] * n_blocks)
        w_half = [send(after(lax.dynamic_slice(w_out, (h * half + place * step, 0), (step, d)), segs), CHIP_SWAP) for h in range(2)]

        def w_gather(h, dep):
            return lax.all_gather(after(w_half[h], dep), ('dp', 'sp'), axis=0, tiled=True)

        aux = token_aux(jnp.concatenate([segs[0].reshape(-1)[-3:], segs[1:].reshape(-1)]))
        tails = tails.reshape(-1, d)
        w2, wb = w_zx.reshape(d, 2 * XW), w_bc.reshape(d, NB)
        pad = lambda v: jnp.pad(v.astype(f32), ((0, SUB - v.shape[0]), (0, 0)))
        cw = pad(jnp.concatenate([conv_x, bias_x[None]], axis=0))
        cwb = pad(jnp.concatenate([conv_bc.reshape(4, NB), bias_bc.reshape(1, NB)], axis=0))
        hp1 = jnp.pad(jnp.stack([dt_bias, a_log]), ((0, 6), (0, T - HEADS)))
        hp2 = pad(jnp.stack([jnp.repeat(d_skip, HEAD), norm_w.astype(f32)]))
        init = jnp.broadcast_to((jnp.arange(T + SUB) >= T).astype(f32)[None, :, None], (2, T + SUB, XW))
        pre = jnp.stack([seq_slot(me, s) for s in range(4)]).astype(jnp.int32)
        weights = (w2, wb, w_dt)
        consts = (cw, cwb, hp1)

        def front(slots, part, xs, halos, hrows, carry, per):
            return front_call(pre, aux, [lambda b, s=s: b[s] * (rows // (per * MT)) + part for s in slots], xs, halos, hrows,
                              weights, carry, consts, per=per)

        tail_row = lambda s: (lambda b: b[s] * HALO)
        *own, ends = front((0, 1), 0, [x_loc, x_par], [tails] * 2, [tail_row(0), tail_row(1)], init, per)
        w_rem = [w_gather(0, ends)]
        x_dir[0] = after(x_dir[0], ends)
        rem, carry, x_fwd = [[], []], [init[:1], after(init[:1], ends)], []
        for k in range(NCH):
            x_fwd.append(send(x_dir[k], CORE_SWAP))
            for r, xs in ((0, x_dir), (1, x_fwd)):
                halo = (tails, tail_row(2 + r)) if k == 0 else (xs[k - 1], lambda b: ch - HALO)
                c = after(carry[r], carry[0]) if r else after(carry[0], carry[1])
                *arrs, carry[r] = front((2 + r,), k, [xs[k]], [halo[0]], [halo[1]], c, kper)
                rem[r].append(arrs)
            if k + 1 < NCH:
                x_dir[k + 1] = after(x_dir[k + 1], carry[1])
        starts = chain_call(ends, carry[0], carry[1], n_blocks)
        w_rem.append(w_gather(1, starts))

        def mix(slots, part, xs, arrs, start, cofs, per):
            return mixz_call(pre, aux, [lambda b, s=s: b[s] * (rows // (per * MT)) + part for s in slots], xs, arrs, w2, start, hp2,
                             per=per, cofs=cofs)

        y_in = [[], []]
        last = starts
        for r, xs in ((1, x_fwd), (0, x_dir)):
            c, cofs = after(starts, last), 2 + r
            for k in range(NCH):
                yn, c = mix((2 + r,), k, [xs[k]], rem[r][k], c, cofs, kper)
                last, cofs = c, 0
                y_in[r].append(send(yn, CHIP_SWAP))
        y_own, _ = mix((0, 1), 0, [x_loc, x_par], own, after(starts, last), 0, per)
        other = []
        for k in range(NCH):
            part = out_call(1, k, y_own, y_in[1][k], w_out, w_rem)
            other.append(send(part, CORE_SWAP))
        y = None
        for k in range(NCH):
            y = out_call(0, k, y_own, y_in[0][k], w_out, w_rem, x_loc, other[k], y)
        return y

    return jax.shard_map(body, mesh=mesh, in_specs=(token_spec, seg_spec) + weight_specs, out_specs=token_spec, check_vma=False)
```

```python
import functools
import jax
import jax.numpy as jnp
from jax import lax
from jax.sharding import PartitionSpec as P
from jax.experimental import pallas as pl
from jax.experimental.pallas import tpu as pltpu

T = 128
XW = 2048
NB = 512
GW = 1024
D = 4096
TOK = 1024
HEADS, HEAD = 32, 64
XT = 512
MT = 256
HALO = 16
SUB = 8
MH = MT + HALO
LOG2E = 1.4426950408889634
NORM_EPS = 1e-5
MIB = 2**20
f32, bf16 = jnp.float32, jnp.bfloat16
MESH = pl.DeviceIdType.MESH
ONE = pl.Buffered(1)


def silu(v):
    h = 0.5 * v
    return h + h * jnp.tanh(h)


def lane_bcast(cols, h):
    return jnp.broadcast_to(cols[:, h:h + 1], (cols.shape[0], T))


def pair_bcast(cols, p):
    lanes = lax.broadcasted_iota(jnp.int32, (cols.shape[0], T), 1)
    return jnp.where(lanes < HEAD, lane_bcast(cols, 2 * p), lane_bcast(cols, 2 * p + 1))


def row(ref, r):
    return ref[r:r + 1, :]


def mac(a, b, ca=1, cb=0, **kw):
    return lax.dot_general(a, b, (((ca,), (cb,)), ((), ())), preferred_element_type=f32, **kw)


def rows_from(start, size):
    return pl.ds(start if isinstance(start, int) else pl.multiple_of(start, 16), size)


def front_kernel(pre, *refs, nx, per, hrows, more):
    xs_, hs_, auxs = refs[:nx], refs[nx:2 * nx], refs[2 * nx:3 * nx]
    wx_ref, wb_ref, wdt_ref, cw_ref, cwb_ref, hp_ref, *cins = refs[3 * nx:][:6 + more]
    (xa_ref, bca_ref, dc_ref, cout_ref, xbuf, pbuf, bbuf, xw, bt, cum_all, wgt, abuf, sem) = refs[3 * nx + 6 + more:]
    n = pl.program_id(0)
    last_n = XW // XT
    nm = nx * per
    rows = lax.broadcasted_iota(jnp.int32, (T, T), 0)
    cols = lax.broadcasted_iota(jnp.int32, (T, T), 1)
    tiles = [slice(t * T, (t + 1) * T) for t in range(MT // T)]

    def copies(m):
        i, s = divmod(m, per)
        if s:
            return [pltpu.make_async_copy(xs_[i].at[rows_from(s * MT - HALO, MH)], xbuf.at[m], sem.at[m])]
        return [pltpu.make_async_copy(hs_[i].at[rows_from(hrows[i](pre), HALO)], xbuf.at[m, pl.ds(0, HALO)], sem.at[m]),
                pltpu.make_async_copy(xs_[i].at[pl.ds(0, MT)], xbuf.at[m, pl.ds(HALO, MT)], sem.at[m])]

    def left(i):
        return slice(nm * MT + SUB * (i + 1), nm * MT + SUB * (i + 2))

    def heads_first(v):
        return pltpu.roll(v, lax.rem(T - (XT // HEAD) * (n - 1), T), 1)

    def at(m, ts):
        return pl.ds(pl.multiple_of(m * MT + ts.start, T), T)

    def conv(read, lo, w, keep):
        cs = slice(lo, lo + T)
        acc = read(0, cs) * row(w, 3)[:, cs] + row(w, 4)[:, cs]
        for k in range(3):
            acc = acc + (read(3 - k, cs) * w[k:k + 1, cs]) * keep[k]
        return silu(acc).astype(bf16)

    def taps(m, ts):
        return [lane_bcast(abuf[m, ts, :], 2 - k) for k in range(3)]

    def x_dot(m):
        pbuf[lax.rem(n, 2), m] = jnp.dot(xbuf[m], wx_ref[...], preferred_element_type=f32).astype(bf16).astype(f32)

    def setup(m, i, s):
        for ts in tiles:
            r0 = HALO + ts.start
            keep = taps(m, ts)
            for c in range(NB // T):
                act = conv(lambda d, cs: bbuf[r0 - d:r0 - d + T, cs], c * T, cwb_ref, keep)
                bca_ref[at(m, ts), c * T:(c + 1) * T] = act
                if c < 2:
                    bt[i, c, :, at(s, ts)] = act.T
            raw = bbuf[r0:r0 + T, NB:NB + T] + row(hp_ref, 0)
            dtv = jnp.maximum(raw, 0.0) + jnp.log1p(jnp.exp(-jnp.abs(raw)))
            log_a = -jnp.exp(row(hp_ref, 1)) * dtv * LOG2E
            cum = mac((rows >= cols).astype(f32), log_a, precision=lax.Precision.HIGHEST)
            dc_ref[at(m, ts), :] = jnp.where(cols < HEADS, cum, pltpu.roll(dtv, HEADS, 1))
            before = jnp.where((s == 0) & (ts.start == 0), 0.0, row(cum_all, nm * MT))
            cum = cum + before
            cum_all[at(m, ts), :] = cum
            cum_all[nm * MT:nm * MT + SUB, :] = jnp.broadcast_to(cum[T - 1:T, :], (8, T))
            wgt[at(m, ts), :] = dtv

    def weigh(i):
        lo, end = i * per * MT, (i + 1) * per * MT
        doc = abuf[end // MT - 1, MT - 1:MT, 5:6]
        last = row(cum_all, end - 1)
        keep_in = abuf[lo // MT, 0:1, 0:1] * (abuf[lo // MT, 0:1, 5:6] == doc).astype(f32)
        carry = jnp.broadcast_to(jnp.exp2(last) * keep_in, (8, T))
        for r in range(lo, end, T):
            keep = jnp.broadcast_to((abuf[r // MT, r % MT:r % MT + T, 5:6] == doc).astype(f32), (T, T))
            wgt[r:r + T, :] = jnp.exp2(last - cum_all[r:r + T, :]) * wgt[r:r + T, :] * keep
        cum_all[left(i), :] = carry

    def x_conv(m):
        slot = lax.rem(n + 1, 2)
        for ts in tiles:
            r0 = HALO + ts.start
            keep = taps(m, ts)
            wg = heads_first(wgt[at(m, ts), :])
            for p in range(XT // T):
                cs = slice(p * T, (p + 1) * T)
                xa = conv(lambda d, cs: pbuf[slot, m, r0 - d:r0 - d + T, cs], p * T, cw_ref, keep)
                xa_ref[at(m, ts), cs] = xa
                xw[at(m, ts), cs] = (xa.astype(f32) * pair_bcast(wg, p)).astype(bf16)

    def end_state():
        g = (n - 1) // (GW // XT)
        for i in range(nx):
            upd = jnp.dot(bt[i, g], xw[i * per * MT:(i + 1) * per * MT, :], preferred_element_type=f32)
            cr = heads_first(cum_all[left(i), :])
            for p in range(XT // T):
                cs = slice(p * T, (p + 1) * T)
                carry = pair_bcast(cr, p)
                if cins:
                    cout_ref[i, :T, cs] = cins[0][i, :T, cs] * jnp.broadcast_to(carry[:1], (T, T)) + upd[:, cs]
                    cout_ref[i, T:, cs] = cins[0][i, T:, cs] * carry
                else:
                    cout_ref[i, :T, cs] = upd[:, cs]
                    cout_ref[i, T:, cs] = carry

    @pl.when(n == 0)
    def _():
        for m in range(nm):
            for c in copies(m):
                c.start()
        bbuf[:, NB:] = jnp.zeros((MH, T), f32)
        for m in range(nm):
            i, s = divmod(m, per)
            abuf[m] = auxs[i][s * MT:(s + 1) * MT, :]

        @pl.loop(0, nm)
        def _(m):
            for k in range(nm):
                @pl.when(m == k)
                def _():
                    for c in copies(k):
                        c.wait()
            bbuf[:, 0:NB] = jnp.dot(xbuf[m], wb_ref[...], preferred_element_type=f32).astype(bf16).astype(f32)
            bbuf[:, NB:NB + HEADS] = jnp.dot(xbuf[m], wdt_ref[...], preferred_element_type=f32).astype(bf16).astype(f32)
            x_dot(m)
            setup(m, m // per, lax.rem(m, per))

        for i in range(nx):
            weigh(i)

    @pl.when((n > 0) & (n < last_n))
    def _():
        @pl.loop(0, nm)
        def _(m):
            x_dot(m)
            x_conv(m)

    @pl.when(n == last_n)
    def _():
        @pl.loop(0, nm)
        def _(m):
            x_conv(m)

    @pl.when(n > 0)
    def _():
        end_state()


def front_call(pre, aux, amaps, xs, halos, hrows, weights, cin, consts, *, per):
    nx = len(xs)
    nm = nx * per
    n = nm * MT
    nt = XW // XT
    w2, wb, wdt = weights
    hbm = pl.BlockSpec(memory_space=pl.ANY)
    prev = lambda j: jnp.maximum(j - 1, 0)
    whole = lambda *shape, mode=ONE: pl.BlockSpec(shape, lambda j, b: (0,) * len(shape), pipeline_mode=mode)
    cols = lambda k: pl.BlockSpec((k, XT), lambda j, b: (0, prev(j)))
    state = pl.BlockSpec((nx, T + 8, XT), lambda j, b: (0, 0, prev(j)))
    in_specs = [hbm] * (2 * nx) + [pl.BlockSpec((per * MT, T), lambda j, b, f=f: (f(b), 0), pipeline_mode=ONE) for f in amaps] + [
        pl.BlockSpec((D, XT), lambda j, b: (0, nt + jnp.minimum(j, nt - 1))), whole(D, NB), whole(D, HEADS),
        cols(SUB), whole(SUB, NB), whole(SUB, T)] + ([] if cin is None else [state])
    gs = pltpu.PrefetchScalarGridSpec(
        num_scalar_prefetch=1, grid=(nt + 1,), in_specs=in_specs,
        out_specs=[cols(n), whole(n, NB, mode=None), whole(n, T, mode=None), state],
        scratch_shapes=[pltpu.VMEM((nm, MH, D), bf16), pltpu.VMEM((2, nm, MH, XT), f32), pltpu.VMEM((MH, NB + T), f32),
                        pltpu.VMEM((n, XT), bf16), pltpu.VMEM((nx, 2, T, per * MT), bf16),
                        pltpu.VMEM((n + 8 * (nx + 1), T), f32), pltpu.VMEM((n, T), f32), pltpu.VMEM((nm, MT, T), f32),
                        pltpu.SemaphoreType.DMA((nm,))],
    )
    return pl.pallas_call(
        functools.partial(front_kernel, nx=nx, per=per, hrows=hrows, more=int(cin is not None)), grid_spec=gs,
        out_shape=[jax.ShapeDtypeStruct((n, XW), bf16), jax.ShapeDtypeStruct((n, NB), bf16),
                   jax.ShapeDtypeStruct((n, T), f32), jax.ShapeDtypeStruct((nx, T + 8, XW), f32)],
        compiler_params=pltpu.CompilerParams(dimension_semantics=("arbitrary",), vmem_limit_bytes=62 * MIB),
        cost_estimate=pl.CostEstimate(flops=n * 25_000_000, bytes_accessed=n * 10000, transcendentals=n * 4096),
        name="front",
    )(pre, *xs, *halos, *[aux] * nx, w2, wb, wdt, *consts, *([] if cin is None else [cin]))


def mixz_kernel(pre, *refs, nx):
    xs_, auxs = refs[:nx], refs[nx:2 * nx]
    (xa_ref, bg_ref, cg_ref, dc_ref, wz_ref, cin_ref, hp_ref, yn_ref, cout_ref, xv, av, zbuf, ybuf, xw, state) = refs[2 * nx:]
    g, i, tile = pl.program_id(0), pl.program_id(1), pl.program_id(2)
    n_tiles = pl.num_programs(2)

    @pl.when(tile == 0)
    def _():
        state[...] = cin_ref[0]

    for k in range(nx):
        @pl.when(i == k)
        def _():
            xv[...] = xs_[k][...]
            av[...] = auxs[k][...]

    rows = lax.broadcasted_iota(jnp.int32, (T, T), 0)
    cols = lax.broadcasted_iota(jnp.int32, (T, T), 1)
    lo_half = cols < 64
    zero = jnp.zeros((T, T), bf16)
    for t in range(MT // T):
        rs = slice(t * T, (t + 1) * T)
        aux = av[rs, :]
        auxt = aux.T
        mask = (rows >= cols) & (lane_bcast(aux, 5) == jnp.broadcast_to(auxt[5:6, :], (T, T)))
        k_in = lane_bcast(aux, 3)
        k_end = lane_bcast(aux, 4)
        dc = pltpu.roll(dc_ref[rs, :], lax.rem(T - 16 * g, T), 1)
        dct = dc.T
        rel = dct[:HEADS // 2, :] - jnp.log2(dct[HEADS:HEADS + HEADS // 2, :])
        bg, cg = bg_ref[rs, :], cg_ref[rs, :]
        sm = jnp.where(mask, mac(cg, bg, 1, 1), 0.0)
        ybuf[...] = mac(cg, state[...].astype(bf16))
        sq = jnp.zeros((T, T), f32)
        if t == 0:
            zbuf[...] = jnp.dot(xv[...], wz_ref[...], preferred_element_type=f32).astype(bf16).astype(f32)
        for p in range(GW // T):
            cs = slice(p * T, (p + 1) * T)
            xa = xa_ref[rs, cs]
            xaf = xa.astype(f32)
            c0, c1 = lane_bcast(dc, 2 * p), lane_bcast(dc, 2 * p + 1)
            mixes = []
            for hh, cb in ((2 * p, c0), (2 * p + 1, c1)):
                diff = jnp.minimum(cb - jnp.broadcast_to(rel[hh:hh + 1, :], (T, T)), 126.0)
                mixes.append((sm * jnp.exp2(diff)).astype(bf16))
            lhs = jnp.concatenate(mixes, axis=1)
            rhs = jnp.concatenate([jnp.where(lo_half, xa, zero), jnp.where(lo_half, zero, xa)], axis=0)
            y = mac(lhs, rhs)
            cump = jnp.where(lo_half, c0, c1)
            dtp = pair_bcast(dc, HEADS // 2 + p)
            last = cump[T - 1:T, :]
            xw[:, cs] = (xaf * (jnp.exp2(last - cump) * dtp * k_end)).astype(bf16)
            y = y + ybuf[:, cs] * (jnp.exp2(cump) * k_in) + hp_ref[0:1, cs] * xaf
            v = y * silu(zbuf[rs, cs])
            ybuf[:, cs] = v
            sq = sq + v * v
            state[:, cs] = state[:, cs] * (jnp.exp2(last) * k_in[T - 1:T, :])
        ms = jnp.sum(sq, axis=1, keepdims=True) * (1.0 / GW)
        r = jnp.broadcast_to(lax.rsqrt(ms + NORM_EPS), (T, T))
        for p in range(GW // T):
            cs = slice(p * T, (p + 1) * T)
            yn_ref[rs, cs] = (ybuf[:, cs] * r * hp_ref[1:2, cs]).astype(bf16)
        state[...] = state[...] + mac(bg, xw[...], 0, 0)

    @pl.when(tile == n_tiles - 1)
    def _():
        cout_ref[0] = state[...]


def mixz_call(pre, aux, amaps, xs, arrs, w2, cin, hp, *, per, cofs):
    nx = len(xs)
    n = nx * per * MT
    xa, bca, dc = arrs
    piece = lambda k: (lambda g, i, t: jnp.clip((i - k) * per + t, 0, per - 1))
    rows = lambda w, c: pl.BlockSpec((MT, w), lambda g, i, t, b: (i * per + t, c(g)))
    state = lambda ofs: pl.BlockSpec((1, T, GW), lambda g, i, t, b: (ofs + i, 0, g))
    cols = lambda k: pl.BlockSpec((k, GW), lambda g, i, t, b: (0, g))
    in_specs = [pl.BlockSpec((MT, D), lambda g, i, t, b, k=k: (piece(k)(g, i, t), 0)) for k in range(nx)]
    in_specs += [pl.BlockSpec((MT, T), lambda g, i, t, b, k=k: (amaps[k](b) * per + piece(k)(g, i, t), 0)) for k in range(nx)]
    same = lambda g: g
    in_specs += [rows(GW, same), rows(T, same), rows(T, lambda g: 2 + g), rows(T, lambda g: 0), cols(D), state(cofs), cols(8)]
    gs = pltpu.PrefetchScalarGridSpec(
        num_scalar_prefetch=1, grid=(2, nx, per), in_specs=in_specs, out_specs=[rows(GW, same), state(0)],
        scratch_shapes=[pltpu.VMEM((MT, D), bf16), pltpu.VMEM((MT, T), f32), pltpu.VMEM((MT, GW), f32), pltpu.VMEM((T, GW), f32),
                        pltpu.VMEM((T, GW), bf16), pltpu.VMEM((T, GW), f32)],
    )
    return pl.pallas_call(
        functools.partial(mixz_kernel, nx=nx), grid_spec=gs,
        out_shape=[jax.ShapeDtypeStruct((n, XW), bf16), jax.ShapeDtypeStruct((nx, T, XW), f32)],
        compiler_params=pltpu.CompilerParams(dimension_semantics=("arbitrary",) * 3, vmem_limit_bytes=60 * MIB),
        cost_estimate=pl.CostEstimate(flops=n * 20_000_000, bytes_accessed=n * 14000, transcendentals=n * 10000),
        name="mixz",
    )(pre, *xs, *[aux] * nx, xa, bca, bca, dc, w2, cin, hp)


def seq_slot(me, s):
    c = (me % 2 + s % 2) % 2
    y = (me // 2 + s // 2) % 2
    return 2 * y + c


NCH = 2


def count(flag):
    return jnp.where(flag, 1, 0)


def ahead_kernel(n_blocks, n_pl, seg_ref, tail_ref, x_hbm, w_hbm, segs_ref, tails_ref, x0_hbm, x1_hbm, w0_hbm, w1_hbm,
                 xbuf, wbuf, in_sem, out_sem, send_sem, recv_sem):
    me, blk = lax.axis_index('tp'), lax.axis_index('sp')
    step = w0_hbm.shape[0]
    place = lax.axis_index('dp') * n_blocks + blk
    moves = []
    for k, (xo, wo) in enumerate(((x0_hbm, w0_hbm), (x1_hbm, w1_hbm))):
        at = pl.multiple_of((k * n_pl + place) * step, HALO)
        for j, (src, buf, dst) in enumerate(((x_hbm.at[pl.ds(k * xo.shape[0], xo.shape[0])], xbuf.at[k], xo),
                                             (w_hbm.at[pl.ds(at, step)], wbuf.at[k], wo))):
            moves.append((pltpu.make_async_copy(src, buf, in_sem.at[k, j]), pltpu.make_async_copy(buf, dst, out_sem.at[k, j])))
    for load, _ in moves:
        load.start()
    barrier = pltpu.get_barrier_semaphore()
    others = [{'tp': seq_slot(me, s)} for s in (1, 2, 3)]
    before = {'sp': jnp.maximum(blk - 1, 0), 'tp': 3}
    after = [{'sp': jnp.minimum(blk + 1, n_blocks - 1), 'tp': q} for q in range(4)]
    sends_on = (me == 3) & (blk < n_blocks - 1)
    for dev in others:
        pl.semaphore_signal(barrier, inc=1, device_id=dev, device_id_type=MESH)

    @pl.when(blk > 0)
    def _():
        pl.semaphore_signal(barrier, inc=1, device_id=before, device_id_type=MESH)

    @pl.when(sends_on)
    def _():
        for dev in after:
            pl.semaphore_signal(barrier, inc=1, device_id=dev, device_id_type=MESH)

    pl.semaphore_wait(barrier, 3 + count(blk > 0) + 4 * count(sends_on))

    def copies(dev, entry, k, rk):
        return [pltpu.make_async_remote_copy(src_ref=seg_ref, dst_ref=segs_ref.at[entry], send_sem=send_sem.at[k, 0],
                                             recv_sem=recv_sem.at[rk, 0], device_id=dev, device_id_type=MESH),
                pltpu.make_async_remote_copy(src_ref=tail_ref, dst_ref=tails_ref.at[entry], send_sem=send_sem.at[k, 1],
                                             recv_sem=recv_sem.at[rk, 1], device_id=dev, device_id_type=MESH)]

    inner = [copies(dev, me + 1, k, k) for k, dev in enumerate(others)]
    outer = [copies(dev, 0, 3 + q, 3) for q, dev in enumerate(after)]
    for cs in inner:
        for c in cs:
            c.start()

    @pl.when(sends_on)
    def _():
        for cs in outer:
            for c in cs:
                c.start()

    for load, store in moves:
        load.wait()
        store.start()
    segs_ref[me + 1] = seg_ref[...]
    tails_ref[me + 1] = tail_ref[...]

    @pl.when(blk == 0)
    def _():
        segs_ref[0] = jnp.zeros_like(seg_ref)
        tails_ref[0] = jnp.zeros_like(tail_ref)

    for cs in inner:
        for c in cs:
            c.wait_send()
            c.wait_recv()

    @pl.when(sends_on)
    def _():
        for cs in outer:
            for c in cs:
                c.wait_send()

    @pl.when(blk > 0)
    def _():
        for c in outer[0]:
            c.wait_recv()

    for _, store in moves:
        store.wait()


def ahead_call(seg, x, w, n_blocks, n_pl):
    rows = x.shape[0]
    half, step = rows // NCH, w.shape[0] // (NCH * n_pl)
    vmem, hbm = pl.BlockSpec(memory_space=pltpu.VMEM), pl.BlockSpec(memory_space=pl.ANY)
    sds = jax.ShapeDtypeStruct
    return pl.pallas_call(
        functools.partial(ahead_kernel, n_blocks, n_pl),
        grid=(1,),
        in_specs=[vmem, pl.BlockSpec((HALO, D), lambda i: (rows // HALO - 1, 0)), hbm, hbm],
        out_specs=[vmem] * 2 + [hbm] * 4,
        out_shape=[sds((5, rows // T, T), jnp.int32), sds((5, HALO, D), bf16)] + [sds((half, D), bf16)] * 2 + [sds((step, D), bf16)] * 2,
        scratch_shapes=[pltpu.VMEM((NCH, half, D), bf16), pltpu.VMEM((NCH, step, D), bf16), pltpu.SemaphoreType.DMA((NCH, 2)),
                        pltpu.SemaphoreType.DMA((NCH, 2)), pltpu.SemaphoreType.DMA((7, 2)), pltpu.SemaphoreType.DMA((4, 2))],
        compiler_params=pltpu.CompilerParams(collective_id=0, has_side_effects=True, vmem_limit_bytes=24 * MIB),
        name="ahead",
    )(seg.reshape(rows // T, T), x, x, w)


CW = 256


def chain_kernel(n_blocks, e01_ref, e2_ref, e3_ref, out_ref, ebuf, sbuf, obuf, lsem, send_sem, recv_sem):
    me, blk = lax.axis_index('tp'), lax.axis_index('sp')
    srcs = [e01_ref.at[0], e01_ref.at[1], e2_ref.at[0], e3_ref.at[0]]
    loads = [pltpu.make_async_copy(src, ebuf.at[seq_slot(me, s)], lsem.at[s]) for s, src in enumerate(srcs)]
    for c in loads:
        c.start()
    barrier = pltpu.get_barrier_semaphore()
    before = {'sp': jnp.maximum(blk - 1, 0)}
    after = {'sp': jnp.minimum(blk + 1, n_blocks - 1)}

    @pl.when(blk > 0)
    def _():
        pl.semaphore_signal(barrier, inc=1, device_id=before, device_id_type=MESH)

    @pl.when(blk < n_blocks - 1)
    def _():
        pl.semaphore_signal(barrier, inc=1, device_id=after, device_id_type=MESH)

    pl.semaphore_wait(barrier, count(blk > 0) + count(blk < n_blocks - 1))

    for c in loads:
        c.wait()

    def through(q, s, cs):
        return ebuf[q, :T, cs] + ebuf[q, T:T + 1, cs] * s

    for q in (1, 2, 3):
        ebuf[q, :T, :] = through(q, ebuf[q - 1, :T, :], slice(None))
        ebuf[q, T:, :] = ebuf[q, T:, :] * ebuf[q - 1, T:, :]

    @pl.when(blk == 0)
    def _():
        sbuf[...] = jnp.zeros_like(sbuf)

    n = XW // CW

    def send(j):
        return pltpu.make_async_remote_copy(src_ref=obuf.at[j], dst_ref=sbuf.at[j], send_sem=send_sem.at[j],
                                            recv_sem=recv_sem.at[j], device_id=after, device_id_type=MESH)

    for j in range(n):
        cs = slice(j * CW, (j + 1) * CW)

        @pl.when(blk > 0)
        def _():
            send(j).wait_recv()

        @pl.when(blk < n_blocks - 1)
        def _():
            obuf[j] = through(3, sbuf[j], cs)
            send(j).start()

    for j in range(n):
        cs = slice(j * CW, (j + 1) * CW)
        for q in range(4):
            v = through(q - 1, sbuf[j], cs) if q else sbuf[j]
            out_ref[seq_slot(me, q), :, cs] = v

    @pl.when(blk < n_blocks - 1)
    def _():
        for j in range(n):
            send(j).wait_send()


def chain_call(e01, e2, e3, n_blocks):
    hbm = pl.BlockSpec(memory_space=pl.ANY)
    n = XW // CW
    return pl.pallas_call(
        functools.partial(chain_kernel, n_blocks),
        in_specs=[hbm] * 3,
        out_specs=pl.BlockSpec(memory_space=pltpu.VMEM),
        out_shape=jax.ShapeDtypeStruct((4, T, XW), f32),
        scratch_shapes=[pltpu.VMEM((4, T + SUB, XW), f32), pltpu.VMEM((n, T, CW), f32), pltpu.VMEM((n, T, CW), f32),
                        pltpu.SemaphoreType.DMA((4,)), pltpu.SemaphoreType.DMA((n,)), pltpu.SemaphoreType.DMA((n,))],
        compiler_params=pltpu.CompilerParams(collective_id=1, has_side_effects=True, vmem_limit_bytes=40 * MIB),
        name="chain",
    )(e01, e2, e3)


NT = 512


def out_kernel(y_ref, yr_ref, w_ref, wr0_ref, wr1_ref, *refs):
    h = XW // 2
    acc = (jnp.dot(y_ref[...], w_ref[...], preferred_element_type=f32)
           + jnp.dot(yr_ref[:, 0:h], wr0_ref[...], preferred_element_type=f32)
           + jnp.dot(yr_ref[:, h:], wr1_ref[...], preferred_element_type=f32))
    if len(refs) > 1:
        x_ref, other_ref = refs[:2]
        acc = x_ref[...].astype(f32) + (acc + other_ref[...])
    refs[-1][...] = acc.astype(refs[-1].dtype)


def out_call(run, part, y, yr, w, wr, x=None, other=None, into=None):
    rows = yr.shape[0]
    h = XW // 2
    at = lambda r: (lambda j: (r, j))
    cols = at(0)
    ins = [y, yr, w, *wr]
    specs = [pl.BlockSpec((rows, XW), lambda j: (run * (TOK // rows) + part, 0), pipeline_mode=ONE),
             pl.BlockSpec((rows, XW), lambda j: (0, 0), pipeline_mode=ONE),
             pl.BlockSpec((XW, NT), cols), pl.BlockSpec((h, NT), cols), pl.BlockSpec((h, NT), cols)]
    alias = {}
    if x is not None:
        ins += [x, other]
        specs += [pl.BlockSpec((rows, NT), at(part)), pl.BlockSpec((rows, NT), cols)]
    if into is not None:
        alias = {len(ins): 0}
        ins.append(into)
        specs.append(pl.BlockSpec(memory_space=pl.ANY))
    return pl.pallas_call(
        out_kernel,
        grid=(D // NT,), in_specs=specs,
        out_specs=pl.BlockSpec((rows, NT), cols if x is None else at(part)),
        out_shape=jax.ShapeDtypeStruct((rows, D), f32) if x is None else jax.ShapeDtypeStruct(x.shape, bf16),
        input_output_aliases=alias,
        compiler_params=pltpu.CompilerParams(dimension_semantics=("arbitrary",), vmem_limit_bytes=56 * MIB),
        cost_estimate=pl.CostEstimate(flops=rows * 33_000_000, bytes_accessed=rows * 100000, transcendentals=0),
        name="out_proj",
    )(*ins)


def send(v, perm):
    return lax.ppermute(v, 'tp', perm)


def after(v, *deps):
    return lax.optimization_barrier((v,) + deps)[0]


CORE_SWAP = [(i, i ^ 1) for i in range(4)]
CHIP_SWAP = [(i, i ^ 2) for i in range(4)]


def token_aux(seg_ext):
    seg = seg_ext[3:]
    n = seg.shape[0]
    tile_prev = jnp.repeat(seg_ext[2:n + 2:T], T)
    tile_last = jnp.repeat(seg[T - 1::T], T)
    cols = [seg == seg_ext[3 - k:n + 3 - k] for k in (1, 2, 3)] + [seg == tile_prev, seg == tile_last, seg - seg_ext[0]]
    lane = lax.broadcasted_iota(jnp.int32, (n, T), 1)
    out = jnp.zeros((n, T), f32)
    for i, c in enumerate(cols):
        out = jnp.where(lane == i, c.astype(f32)[:, None], out)
    return out


def solution(mesh):
    n_blocks = mesh.shape['sp']
    token_spec = seg_spec = P(('dp', 'sp', 'tp'))
    weight_specs = tuple(P(*['tp' if i == dim else None for i in range(dim + 1)]) for dim in (2, 2, 1, 1, 2, 0, 1, 0, 0, 0, 0, 0))

    def body(x_loc, seg_loc, w_zx, w_bc, w_dt, conv_x, conv_bc, bias_x, bias_bc, a_log, dt_bias, d_skip, norm_w, w_out):
        rows, d = x_loc.shape
        me = lax.axis_index('tp')
        ch = rows // NCH
        per, kper = rows // MT, ch // MT
        n_pl = mesh.shape['dp'] * n_blocks
        segs, tails, *parts = ahead_call(seg_loc, x_loc, w_out, n_blocks, n_pl)
        x_par = send(after(x_loc, segs), CORE_SWAP)
        x_dir = [send(v, CHIP_SWAP) for v in parts[:NCH]]
        w_half = [send(v, CHIP_SWAP) for v in parts[NCH:]]

        def w_gather(h, dep):
            return lax.all_gather(after(w_half[h], dep), ('dp', 'sp'), axis=0, tiled=True)

        aux = token_aux(jnp.concatenate([segs[0].reshape(-1)[-3:], segs[1:].reshape(-1)]))
        tails = tails.reshape(-1, d)
        w2, wb = w_zx.reshape(d, 2 * XW), w_bc.reshape(d, NB)
        pad = lambda v: jnp.pad(v.astype(f32), ((0, SUB - v.shape[0]), (0, 0)))
        cw = pad(jnp.concatenate([conv_x, bias_x[None]], axis=0))
        cwb = pad(jnp.concatenate([conv_bc.reshape(4, NB), bias_bc.reshape(1, NB)], axis=0))
        hp1 = jnp.pad(jnp.stack([dt_bias, a_log]), ((0, 6), (0, T - HEADS)))
        hp2 = pad(jnp.stack([jnp.repeat(d_skip, HEAD), norm_w.astype(f32)]))
        pre = jnp.stack([seq_slot(me, s) for s in range(4)]).astype(jnp.int32)
        weights = (w2, wb, w_dt)
        consts = (cw, cwb, hp1)

        def front(slots, part, xs, halos, hrows, carry, per):
            return front_call(pre, aux, [lambda b, s=s: b[s] * (rows // (per * MT)) + part for s in slots], xs, halos, hrows,
                              weights, carry, consts, per=per)

        tail_row = lambda s: (lambda b: b[s] * HALO)
        *own, ends = front((0, 1), 0, [x_loc, x_par], [tails] * 2, [tail_row(0), tail_row(1)], None, per)
        w_rem = [w_gather(0, ends)]
        x_dir[0] = after(x_dir[0], ends)
        rem, carry, x_fwd = [[], []], [None, None], []
        last = ends
        for k in range(NCH):
            x_fwd.append(send(x_dir[k], CORE_SWAP))
            for r, xs in ((0, x_dir), (1, x_fwd)):
                halo = (tails, tail_row(2 + r)) if k == 0 else (xs[k - 1], lambda b: ch - HALO)
                *arrs, carry[r] = front((2 + r,), k, [after(xs[k], last)], [halo[0]], [halo[1]], carry[r], kper)
                last = carry[r]
                rem[r].append(arrs)
            if k + 1 < NCH:
                x_dir[k + 1] = after(x_dir[k + 1], carry[1])
        starts = chain_call(ends, carry[0], carry[1], n_blocks)
        w_rem.append(w_gather(1, starts))

        def mix(slots, part, xs, arrs, start, cofs, per):
            return mixz_call(pre, aux, [lambda b, s=s: b[s] * (rows // (per * MT)) + part for s in slots], xs, arrs, w2, start, hp2,
                             per=per, cofs=cofs)

        y_in = [[], []]
        last = starts
        for r, xs in ((1, x_fwd), (0, x_dir)):
            c, cofs = after(starts, last), 2 + r
            for k in range(NCH):
                yn, c = mix((2 + r,), k, [xs[k]], rem[r][k], c, cofs, kper)
                last, cofs = c, 0
                y_in[r].append(send(yn, CHIP_SWAP))
        y_own, _ = mix((0, 1), 0, [x_loc, x_par], own, after(starts, last), 0, per)
        other = []
        for k in range(NCH):
            part = out_call(1, k, y_own, y_in[1][k], w_out, w_rem)
            other.append(send(part, CORE_SWAP))
        y = None
        for k in range(NCH):
            y = out_call(0, k, y_own, y_in[0][k], w_out, w_rem, x_loc, other[k], y)
        return y

    return jax.shard_map(body, mesh=mesh, in_specs=(token_spec, seg_spec) + weight_specs, out_specs=token_spec, check_vma=False)
```

```python
import functools
import jax
import jax.numpy as jnp
from jax import lax
from jax.sharding import PartitionSpec as P
from jax.experimental import pallas as pl
from jax.experimental.pallas import tpu as pltpu

T = 128
XW = 2048
NB = 512
GW = 1024
D = 4096
TOK = 1024
HEADS, HEAD = 32, 64
XT = 512
MT = 256
HALO = 16
SUB = 8
MH = MT + HALO
LOG2E = 1.4426950408889634
NORM_EPS = 1e-5
MIB = 2**20
f32, bf16 = jnp.float32, jnp.bfloat16
MESH = pl.DeviceIdType.MESH
ONE = pl.Buffered(1)


def silu(v):
    h = 0.5 * v
    return h + h * jnp.tanh(h)


def lane_bcast(cols, h):
    return jnp.broadcast_to(cols[:, h:h + 1], (cols.shape[0], T))


def pair_bcast(cols, p):
    lanes = lax.broadcasted_iota(jnp.int32, (cols.shape[0], T), 1)
    return jnp.where(lanes < HEAD, lane_bcast(cols, 2 * p), lane_bcast(cols, 2 * p + 1))


def row(ref, r):
    return ref[r:r + 1, :]


def mac(a, b, ca=1, cb=0, **kw):
    return lax.dot_general(a, b, (((ca,), (cb,)), ((), ())), preferred_element_type=f32, **kw)


def rows_from(start, size):
    return pl.ds(start if isinstance(start, int) else pl.multiple_of(start, 16), size)


def front_kernel(pre, *refs, nx, per, hrows, more, skip):
    xs_, hs_, auxs = refs[:nx], refs[nx:2 * nx], refs[2 * nx:3 * nx]
    wx_ref, wb_ref, wdt_ref, cw_ref, cwb_ref, hp_ref, *cins = refs[3 * nx:][:6 + more]
    (xa_ref, bca_ref, dc_ref, cout_ref, xbuf, pbuf, bbuf, xw, bt, cum_all, wgt, abuf, sem) = refs[3 * nx + 6 + more + skip:]
    n = pl.program_id(0)
    last_n = XW // XT
    nm = nx * per
    rows = lax.broadcasted_iota(jnp.int32, (T, T), 0)
    cols = lax.broadcasted_iota(jnp.int32, (T, T), 1)
    tiles = [slice(t * T, (t + 1) * T) for t in range(MT // T)]

    def copies(m):
        i, s = divmod(m, per)
        if s:
            return [pltpu.make_async_copy(xs_[i].at[rows_from(s * MT - HALO, MH)], xbuf.at[m], sem.at[m])]
        return [pltpu.make_async_copy(hs_[i].at[rows_from(hrows[i](pre), HALO)], xbuf.at[m, pl.ds(0, HALO)], sem.at[m]),
                pltpu.make_async_copy(xs_[i].at[pl.ds(0, MT)], xbuf.at[m, pl.ds(HALO, MT)], sem.at[m])]

    def left(i):
        return slice(nm * MT + SUB * (i + 1), nm * MT + SUB * (i + 2))

    def heads_first(v):
        return pltpu.roll(v, lax.rem(T - (XT // HEAD) * (n - 1), T), 1)

    def at(m, ts):
        return pl.ds(pl.multiple_of(m * MT + ts.start, T), T)

    def conv(read, lo, w, keep):
        cs = slice(lo, lo + T)
        acc = read(0, cs) * row(w, 3)[:, cs] + row(w, 4)[:, cs]
        for k in range(3):
            acc = acc + (read(3 - k, cs) * w[k:k + 1, cs]) * keep[k]
        return silu(acc).astype(bf16)

    def taps(m, ts):
        return [lane_bcast(abuf[m, ts, :], 2 - k) for k in range(3)]

    def x_dot(m):
        pbuf[lax.rem(n, 2), m] = jnp.dot(xbuf[m], wx_ref[...], preferred_element_type=f32).astype(bf16).astype(f32)

    def setup(m, i, s):
        for ts in tiles:
            r0 = HALO + ts.start
            keep = taps(m, ts)
            for c in range(NB // T):
                act = conv(lambda d, cs: bbuf[r0 - d:r0 - d + T, cs], c * T, cwb_ref, keep)
                bca_ref[at(m, ts), c * T:(c + 1) * T] = act
                if c < 2:
                    bt[i, c, :, at(s, ts)] = act.T
            raw = bbuf[r0:r0 + T, NB:NB + T] + row(hp_ref, 0)
            dtv = jnp.maximum(raw, 0.0) + jnp.log1p(jnp.exp(-jnp.abs(raw)))
            log_a = -jnp.exp(row(hp_ref, 1)) * dtv * LOG2E
            cum = mac((rows >= cols).astype(f32), log_a, precision=lax.Precision.HIGHEST)
            dc_ref[at(m, ts), :] = jnp.where(cols < HEADS, cum, pltpu.roll(dtv, HEADS, 1))
            before = jnp.where((s == 0) & (ts.start == 0), 0.0, row(cum_all, nm * MT))
            cum = cum + before
            cum_all[at(m, ts), :] = cum
            cum_all[nm * MT:nm * MT + SUB, :] = jnp.broadcast_to(cum[T - 1:T, :], (8, T))
            wgt[at(m, ts), :] = dtv

    def weigh(i):
        lo, end = i * per * MT, (i + 1) * per * MT
        doc = abuf[end // MT - 1, MT - 1:MT, 5:6]
        last = row(cum_all, end - 1)
        keep_in = abuf[lo // MT, 0:1, 0:1] * (abuf[lo // MT, 0:1, 5:6] == doc).astype(f32)
        carry = jnp.broadcast_to(jnp.exp2(last) * keep_in, (8, T))
        for r in range(lo, end, T):
            keep = jnp.broadcast_to((abuf[r // MT, r % MT:r % MT + T, 5:6] == doc).astype(f32), (T, T))
            wgt[r:r + T, :] = jnp.exp2(last - cum_all[r:r + T, :]) * wgt[r:r + T, :] * keep
        cum_all[left(i), :] = carry

    def x_conv(m):
        slot = lax.rem(n + 1, 2)
        for ts in tiles:
            r0 = HALO + ts.start
            keep = taps(m, ts)
            wg = heads_first(wgt[at(m, ts), :])
            for p in range(XT // T):
                cs = slice(p * T, (p + 1) * T)
                xa = conv(lambda d, cs: pbuf[slot, m, r0 - d:r0 - d + T, cs], p * T, cw_ref, keep)
                xa_ref[at(m, ts), cs] = xa
                xw[at(m, ts), cs] = (xa.astype(f32) * pair_bcast(wg, p)).astype(bf16)

    def end_state():
        g = (n - 1) // (GW // XT)
        for i in range(nx):
            upd = jnp.dot(bt[i, g], xw[i * per * MT:(i + 1) * per * MT, :], preferred_element_type=f32)
            cr = heads_first(cum_all[left(i), :])
            for p in range(XT // T):
                cs = slice(p * T, (p + 1) * T)
                carry = pair_bcast(cr, p)
                if cins:
                    cout_ref[i, :T, cs] = cins[0][i, :T, cs] * jnp.broadcast_to(carry[:1], (T, T)) + upd[:, cs]
                    cout_ref[i, T:, cs] = cins[0][i, T:, cs] * carry
                else:
                    cout_ref[i, :T, cs] = upd[:, cs]
                    cout_ref[i, T:, cs] = carry

    @pl.when(n == 0)
    def _():
        for m in range(nm):
            for c in copies(m):
                c.start()
        bbuf[:, NB:] = jnp.zeros((MH, T), f32)
        for m in range(nm):
            i, s = divmod(m, per)
            abuf[m] = auxs[i][s * MT:(s + 1) * MT, :]

        @pl.loop(0, nm)
        def _(m):
            for k in range(nm):
                @pl.when(m == k)
                def _():
                    for c in copies(k):
                        c.wait()
            bbuf[:, 0:NB] = jnp.dot(xbuf[m], wb_ref[...], preferred_element_type=f32).astype(bf16).astype(f32)
            bbuf[:, NB:NB + HEADS] = jnp.dot(xbuf[m], wdt_ref[...], preferred_element_type=f32).astype(bf16).astype(f32)
            x_dot(m)
            setup(m, m // per, lax.rem(m, per))

        for i in range(nx):
            weigh(i)

    @pl.when((n > 0) & (n < last_n))
    def _():
        @pl.loop(0, nm)
        def _(m):
            x_dot(m)
            x_conv(m)

    @pl.when(n == last_n)
    def _():
        @pl.loop(0, nm)
        def _(m):
            x_conv(m)

    @pl.when(n > 0)
    def _():
        end_state()


def front_call(pre, aux, amaps, xs, halos, hrows, weights, cin, consts, into, part, parts, *, per):
    nx = len(xs)
    nm = nx * per
    n = nm * MT
    nt = XW // XT
    w2, wb, wdt = weights
    hbm = pl.BlockSpec(memory_space=pl.ANY)
    prev = lambda j: jnp.maximum(j - 1, 0)
    whole = lambda *shape, mode=ONE, r=0: pl.BlockSpec(shape, lambda j, b: (r, 0), pipeline_mode=mode)
    cols = lambda k, r=0: pl.BlockSpec((k, XT), lambda j, b: (r, prev(j)))
    state = pl.BlockSpec((nx, T + 8, XT), lambda j, b: (0, 0, prev(j)))
    in_specs = [hbm] * (2 * nx) + [pl.BlockSpec((per * MT, T), lambda j, b, f=f: (f(b), 0), pipeline_mode=ONE) for f in amaps] + [
        pl.BlockSpec((D, XT), lambda j, b: (0, nt + jnp.minimum(j, nt - 1))), whole(D, NB), whole(D, HEADS),
        cols(SUB), whole(SUB, NB), whole(SUB, T)] + ([] if cin is None else [state]) + [hbm] * len(into)
    n_in = len(in_specs) + 1
    gs = pltpu.PrefetchScalarGridSpec(
        num_scalar_prefetch=1, grid=(nt + 1,), in_specs=in_specs,
        out_specs=[cols(n, part), whole(n, NB, mode=None, r=part), whole(n, T, mode=None, r=part), state],
        scratch_shapes=[pltpu.VMEM((nm, MH, D), bf16), pltpu.VMEM((2, nm, MH, XT), f32), pltpu.VMEM((MH, NB + T), f32),
                        pltpu.VMEM((n, XT), bf16), pltpu.VMEM((nx, 2, T, per * MT), bf16),
                        pltpu.VMEM((n + 8 * (nx + 1), T), f32), pltpu.VMEM((n, T), f32), pltpu.VMEM((nm, MT, T), f32),
                        pltpu.SemaphoreType.DMA((nm,))],
    )
    return pl.pallas_call(
        functools.partial(front_kernel, nx=nx, per=per, hrows=hrows, more=int(cin is not None), skip=len(into)), grid_spec=gs,
        out_shape=[jax.ShapeDtypeStruct((parts * n, XW), bf16), jax.ShapeDtypeStruct((parts * n, NB), bf16),
                   jax.ShapeDtypeStruct((parts * n, T), f32), jax.ShapeDtypeStruct((nx, T + SUB, XW), f32)],
        input_output_aliases={n_in - len(into) + o: o for o in range(len(into))},
        compiler_params=pltpu.CompilerParams(dimension_semantics=("arbitrary",), vmem_limit_bytes=62 * MIB),
        cost_estimate=pl.CostEstimate(flops=n * 25_000_000, bytes_accessed=n * 10000, transcendentals=n * 4096),
        name="front",
    )(pre, *xs, *halos, *[aux] * nx, w2, wb, wdt, *consts, *([] if cin is None else [cin]), *into)


def mixz_kernel(pre, *refs, ns, pers):
    xs_, auxs = refs[:ns], refs[ns:2 * ns]
    (xa_ref, bg_ref, cg_ref, dc_ref, wz_ref, cin_ref, hp_ref, yn_ref, cout_ref, xv, av, zbuf, ybuf, xw, state) = refs[2 * ns:]
    g, i, tile = pl.program_id(0), pl.program_id(1), pl.program_id(2)
    n_tiles = pl.num_programs(2)

    @pl.when(tile == 0)
    def _():
        state[...] = cin_ref[0]

    src = (i * n_tiles + tile) // pers
    for k in range(ns):
        @pl.when(src == k)
        def _():
            xv[...] = xs_[k][...]
            av[...] = auxs[k][...]

    rows = lax.broadcasted_iota(jnp.int32, (T, T), 0)
    cols = lax.broadcasted_iota(jnp.int32, (T, T), 1)
    lo_half = cols < 64
    zero = jnp.zeros((T, T), bf16)
    for t in range(MT // T):
        rs = slice(t * T, (t + 1) * T)
        aux = av[rs, :]
        auxt = aux.T
        mask = (rows >= cols) & (lane_bcast(aux, 5) == jnp.broadcast_to(auxt[5:6, :], (T, T)))
        k_in = lane_bcast(aux, 3)
        k_end = lane_bcast(aux, 4)
        dc = pltpu.roll(dc_ref[rs, :], lax.rem(T - 16 * g, T), 1)
        dct = dc.T
        rel = dct[:HEADS // 2, :] - jnp.log2(dct[HEADS:HEADS + HEADS // 2, :])
        bg, cg = bg_ref[rs, :], cg_ref[rs, :]
        sm = jnp.where(mask, mac(cg, bg, 1, 1), 0.0)
        ybuf[...] = mac(cg, state[...].astype(bf16))
        sq = jnp.zeros((T, T), f32)
        if t == 0:
            zbuf[...] = jnp.dot(xv[...], wz_ref[...], preferred_element_type=f32).astype(bf16).astype(f32)
        for p in range(GW // T):
            cs = slice(p * T, (p + 1) * T)
            xa = xa_ref[rs, cs]
            xaf = xa.astype(f32)
            c0, c1 = lane_bcast(dc, 2 * p), lane_bcast(dc, 2 * p + 1)
            mixes = []
            for hh, cb in ((2 * p, c0), (2 * p + 1, c1)):
                diff = jnp.minimum(cb - jnp.broadcast_to(rel[hh:hh + 1, :], (T, T)), 126.0)
                mixes.append((sm * jnp.exp2(diff)).astype(bf16))
            lhs = jnp.concatenate(mixes, axis=1)
            rhs = jnp.concatenate([jnp.where(lo_half, xa, zero), jnp.where(lo_half, zero, xa)], axis=0)
            y = mac(lhs, rhs)
            cump = jnp.where(lo_half, c0, c1)
            dtp = pair_bcast(dc, HEADS // 2 + p)
            last = cump[T - 1:T, :]
            xw[:, cs] = (xaf * (jnp.exp2(last - cump) * dtp * k_end)).astype(bf16)
            y = y + ybuf[:, cs] * (jnp.exp2(cump) * k_in) + hp_ref[0:1, cs] * xaf
            v = y * silu(zbuf[rs, cs])
            ybuf[:, cs] = v
            sq = sq + v * v
            state[:, cs] = state[:, cs] * (jnp.exp2(last) * k_in[T - 1:T, :])
        ms = jnp.sum(sq, axis=1, keepdims=True) * (1.0 / GW)
        r = jnp.broadcast_to(lax.rsqrt(ms + NORM_EPS), (T, T))
        for p in range(GW // T):
            cs = slice(p * T, (p + 1) * T)
            yn_ref[rs, cs] = (ybuf[:, cs] * r * hp_ref[1:2, cs]).astype(bf16)
        state[...] = state[...] + mac(bg, xw[...], 0, 0)

    @pl.when(tile == n_tiles - 1)
    def _():
        cout_ref[0] = state[...]


def mixz_call(pre, aux, amaps, xs, arrs, w2, cin, hp, *, nx, per, ofs, cofs):
    ns = len(xs)
    pers = nx * per // ns
    n = nx * per * MT
    xa, bca, dc = arrs
    piece = lambda k: (lambda i, t: jnp.clip(i * per + t - k * pers, 0, pers - 1))
    rows = lambda w, c, o=ofs: pl.BlockSpec((MT, w), lambda g, i, t, b: (o + i * per + t, c(g)))
    state = lambda ofs: pl.BlockSpec((1, T, GW), lambda g, i, t, b: (ofs + i, 0, g))
    cols = lambda k: pl.BlockSpec((k, GW), lambda g, i, t, b: (0, g))
    in_specs = [pl.BlockSpec((MT, D), lambda g, i, t, b, k=k: (piece(k)(i, t), 0)) for k in range(ns)]
    in_specs += [pl.BlockSpec((MT, T), lambda g, i, t, b, k=k: (amaps[k](b) * pers + piece(k)(i, t), 0)) for k in range(ns)]
    same = lambda g: g
    in_specs += [rows(GW, same), rows(T, same), rows(T, lambda g: 2 + g), rows(T, lambda g: 0), cols(D), state(cofs), cols(8)]
    gs = pltpu.PrefetchScalarGridSpec(
        num_scalar_prefetch=1, grid=(2, nx, per), in_specs=in_specs, out_specs=[rows(GW, same, 0), state(0)],
        scratch_shapes=[pltpu.VMEM((MT, D), bf16), pltpu.VMEM((MT, T), f32), pltpu.VMEM((MT, GW), f32), pltpu.VMEM((T, GW), f32),
                        pltpu.VMEM((T, GW), bf16), pltpu.VMEM((T, GW), f32)],
    )
    return pl.pallas_call(
        functools.partial(mixz_kernel, ns=ns, pers=pers), grid_spec=gs,
        out_shape=[jax.ShapeDtypeStruct((n, XW), bf16), jax.ShapeDtypeStruct((nx, T, XW), f32)],
        compiler_params=pltpu.CompilerParams(dimension_semantics=("arbitrary",) * 3, vmem_limit_bytes=60 * MIB),
        cost_estimate=pl.CostEstimate(flops=n * 20_000_000, bytes_accessed=n * 14000, transcendentals=n * 10000),
        name="mixz",
    )(pre, *xs, *[aux] * ns, xa, bca, bca, dc, w2, cin, hp)


def seq_slot(me, s):
    c = (me % 2 + s % 2) % 2
    y = (me // 2 + s // 2) % 2
    return 2 * y + c


NCH = 2


def count(flag):
    return jnp.where(flag, 1, 0)


def ahead_kernel(n_blocks, n_pl, seg_ref, tail_ref, x_hbm, w_hbm, segs_ref, tails_ref, x0_hbm, x1_hbm, w0_hbm, w1_hbm,
                 xbuf, wbuf, in_sem, out_sem, send_sem, recv_sem):
    me, blk = lax.axis_index('tp'), lax.axis_index('sp')
    step = w0_hbm.shape[0]
    place = lax.axis_index('dp') * n_blocks + blk
    moves = []
    for k, (xo, wo) in enumerate(((x0_hbm, w0_hbm), (x1_hbm, w1_hbm))):
        at = pl.multiple_of((k * n_pl + place) * step, HALO)
        for j, (src, buf, dst) in enumerate(((x_hbm.at[pl.ds(k * xo.shape[0], xo.shape[0])], xbuf.at[k], xo),
                                             (w_hbm.at[pl.ds(at, step)], wbuf.at[k], wo))):
            moves.append((pltpu.make_async_copy(src, buf, in_sem.at[k, j]), pltpu.make_async_copy(buf, dst, out_sem.at[k, j])))
    for load, _ in moves:
        load.start()
    barrier = pltpu.get_barrier_semaphore()
    others = [{'tp': seq_slot(me, s)} for s in (1, 2, 3)]
    before = {'sp': jnp.maximum(blk - 1, 0), 'tp': 3}
    after = [{'sp': jnp.minimum(blk + 1, n_blocks - 1), 'tp': q} for q in range(4)]
    sends_on = (me == 3) & (blk < n_blocks - 1)
    for dev in others:
        pl.semaphore_signal(barrier, inc=1, device_id=dev, device_id_type=MESH)

    @pl.when(blk > 0)
    def _():
        pl.semaphore_signal(barrier, inc=1, device_id=before, device_id_type=MESH)

    @pl.when(sends_on)
    def _():
        for dev in after:
            pl.semaphore_signal(barrier, inc=1, device_id=dev, device_id_type=MESH)

    pl.semaphore_wait(barrier, 3 + count(blk > 0) + 4 * count(sends_on))

    def copies(dev, entry, k, rk):
        return [pltpu.make_async_remote_copy(src_ref=seg_ref, dst_ref=segs_ref.at[entry], send_sem=send_sem.at[k, 0],
                                             recv_sem=recv_sem.at[rk, 0], device_id=dev, device_id_type=MESH),
                pltpu.make_async_remote_copy(src_ref=tail_ref, dst_ref=tails_ref.at[entry], send_sem=send_sem.at[k, 1],
                                             recv_sem=recv_sem.at[rk, 1], device_id=dev, device_id_type=MESH)]

    inner = [copies(dev, me + 1, k, k) for k, dev in enumerate(others)]
    outer = [copies(dev, 0, 3 + q, 3) for q, dev in enumerate(after)]
    for cs in inner:
        for c in cs:
            c.start()

    @pl.when(sends_on)
    def _():
        for cs in outer:
            for c in cs:
                c.start()

    for load, store in moves:
        load.wait()
        store.start()
    segs_ref[me + 1] = seg_ref[...]
    tails_ref[me + 1] = tail_ref[...]

    @pl.when(blk == 0)
    def _():
        segs_ref[0] = jnp.zeros_like(seg_ref)
        tails_ref[0] = jnp.zeros_like(tail_ref)

    for cs in inner:
        for c in cs:
            c.wait_send()
            c.wait_recv()

    @pl.when(sends_on)
    def _():
        for cs in outer:
            for c in cs:
                c.wait_send()

    @pl.when(blk > 0)
    def _():
        for c in outer[0]:
            c.wait_recv()

    for _, store in moves:
        store.wait()


def ahead_call(seg, x, w, n_blocks, n_pl):
    rows = x.shape[0]
    half, step = rows // NCH, w.shape[0] // (NCH * n_pl)
    vmem, hbm = pl.BlockSpec(memory_space=pltpu.VMEM), pl.BlockSpec(memory_space=pl.ANY)
    sds = jax.ShapeDtypeStruct
    return pl.pallas_call(
        functools.partial(ahead_kernel, n_blocks, n_pl),
        grid=(1,),
        in_specs=[vmem, pl.BlockSpec((HALO, D), lambda i: (rows // HALO - 1, 0)), hbm, hbm],
        out_specs=[vmem] * 2 + [hbm] * 4,
        out_shape=[sds((5, rows // T, T), jnp.int32), sds((5, HALO, D), bf16)] + [sds((half, D), bf16)] * 2 + [sds((step, D), bf16)] * 2,
        scratch_shapes=[pltpu.VMEM((NCH, half, D), bf16), pltpu.VMEM((NCH, step, D), bf16), pltpu.SemaphoreType.DMA((NCH, 2)),
                        pltpu.SemaphoreType.DMA((NCH, 2)), pltpu.SemaphoreType.DMA((7, 2)), pltpu.SemaphoreType.DMA((4, 2))],
        compiler_params=pltpu.CompilerParams(collective_id=0, has_side_effects=True, vmem_limit_bytes=24 * MIB),
        name="ahead",
    )(seg.reshape(rows // T, T), x, x, w)


CW = 256


def chain_kernel(n_blocks, e01_ref, e2_ref, e3_ref, out_hbm, ebuf, sbuf, obuf, out_ref, lsem, osem, send_sem, recv_sem):
    me, blk = lax.axis_index('tp'), lax.axis_index('sp')
    srcs = [e01_ref.at[0], e01_ref.at[1], e2_ref.at[0], e3_ref.at[0]]
    loads = [pltpu.make_async_copy(src, ebuf.at[seq_slot(me, s)], lsem.at[s]) for s, src in enumerate(srcs)]
    for c in loads:
        c.start()
    barrier = pltpu.get_barrier_semaphore()
    before = {'sp': jnp.maximum(blk - 1, 0)}
    after = {'sp': jnp.minimum(blk + 1, n_blocks - 1)}

    @pl.when(blk > 0)
    def _():
        pl.semaphore_signal(barrier, inc=1, device_id=before, device_id_type=MESH)

    @pl.when(blk < n_blocks - 1)
    def _():
        pl.semaphore_signal(barrier, inc=1, device_id=after, device_id_type=MESH)

    pl.semaphore_wait(barrier, count(blk > 0) + count(blk < n_blocks - 1))

    for c in loads:
        c.wait()

    def through(q, s, cs):
        return ebuf[q, :T, cs] + ebuf[q, T:T + 1, cs] * s

    for q in (1, 2, 3):
        ebuf[q, :T, :] = through(q, ebuf[q - 1, :T, :], slice(None))
        ebuf[q, T:, :] = ebuf[q, T:, :] * ebuf[q - 1, T:, :]

    @pl.when(blk == 0)
    def _():
        sbuf[...] = jnp.zeros_like(sbuf)

    n = XW // CW

    def store(j):
        cs = pl.ds(j * CW, CW)
        return pltpu.make_async_copy(out_ref.at[:, :, cs], out_hbm.at[:, :, cs], osem.at[j])

    def send(j):
        return pltpu.make_async_remote_copy(src_ref=obuf.at[j], dst_ref=sbuf.at[j], send_sem=send_sem.at[j],
                                            recv_sem=recv_sem.at[j], device_id=after, device_id_type=MESH)

    for j in range(n):
        cs = slice(j * CW, (j + 1) * CW)

        @pl.when(blk > 0)
        def _():
            send(j).wait_recv()

        @pl.when(blk < n_blocks - 1)
        def _():
            obuf[j] = through(3, sbuf[j], cs)
            send(j).start()

    for j in range(n):
        cs = slice(j * CW, (j + 1) * CW)
        for q in range(4):
            v = through(q - 1, sbuf[j], cs) if q else sbuf[j]
            out_ref[seq_slot(me, q), :, cs] = v
        store(j).start()

    @pl.when(blk < n_blocks - 1)
    def _():
        for j in range(n):
            send(j).wait_send()

    for j in range(n):
        store(j).wait()


def chain_call(e01, e2, e3, n_blocks):
    hbm = pl.BlockSpec(memory_space=pltpu.HBM)
    n = XW // CW
    return pl.pallas_call(
        functools.partial(chain_kernel, n_blocks),
        in_specs=[hbm] * 3,
        out_specs=hbm,
        out_shape=jax.ShapeDtypeStruct((4, T, XW), f32),
        scratch_shapes=[pltpu.VMEM((4, T + SUB, XW), f32), pltpu.VMEM((n, T, CW), f32), pltpu.VMEM((n, T, CW), f32),
                        pltpu.VMEM((4, T, XW), f32),                         pltpu.SemaphoreType.DMA((4,)), pltpu.SemaphoreType.DMA((n,)),
                        pltpu.SemaphoreType.DMA((n,)), pltpu.SemaphoreType.DMA((n,))],
        compiler_params=pltpu.CompilerParams(collective_id=1, has_side_effects=True, vmem_limit_bytes=40 * MIB),
        name="chain",
    )(e01, e2, e3)


NT = 512


def out_kernel(y_ref, yr_ref, w_ref, wr0_ref, wr1_ref, *refs):
    h = XW // 2
    acc = (jnp.dot(y_ref[...], w_ref[...], preferred_element_type=f32)
           + jnp.dot(yr_ref[:, 0:h], wr0_ref[...], preferred_element_type=f32)
           + jnp.dot(yr_ref[:, h:], wr1_ref[...], preferred_element_type=f32))
    if len(refs) > 1:
        x_ref, other_ref = refs[:2]
        acc = x_ref[...].astype(f32) + (acc + other_ref[...])
    refs[-1][...] = acc.astype(refs[-1].dtype)


def out_call(run, part, y, yr, rpart, w, wr, x=None, other=None, into=None):
    rows = TOK // NCH
    h = XW // 2
    at = lambda r: (lambda j: (r, j))
    cols = at(0)
    ins = [y, yr, w, *wr]
    specs = [pl.BlockSpec((rows, XW), lambda j: (run * (TOK // rows) + part, 0), pipeline_mode=ONE),
             pl.BlockSpec((rows, XW), lambda j: (rpart, 0), pipeline_mode=ONE),
             pl.BlockSpec((XW, NT), cols), pl.BlockSpec((h, NT), cols), pl.BlockSpec((h, NT), cols)]
    alias = {}
    if x is not None:
        ins += [x, other]
        specs += [pl.BlockSpec((rows, NT), at(part)), pl.BlockSpec((rows, NT), cols)]
    if into is not None:
        alias = {len(ins): 0}
        ins.append(into)
        specs.append(pl.BlockSpec(memory_space=pl.ANY))
    return pl.pallas_call(
        out_kernel,
        grid=(D // NT,), in_specs=specs,
        out_specs=pl.BlockSpec((rows, NT), cols if x is None else at(part)),
        out_shape=jax.ShapeDtypeStruct((rows, D), f32) if x is None else jax.ShapeDtypeStruct(x.shape, bf16),
        input_output_aliases=alias,
        compiler_params=pltpu.CompilerParams(dimension_semantics=("arbitrary",), vmem_limit_bytes=56 * MIB),
        cost_estimate=pl.CostEstimate(flops=rows * 33_000_000, bytes_accessed=rows * 100000, transcendentals=0),
        name="out_proj",
    )(*ins)


def send(v, perm):
    return lax.ppermute(v, 'tp', perm)


def after(v, *deps):
    return lax.optimization_barrier((v,) + deps)[0]


CORE_SWAP = [(i, i ^ 1) for i in range(4)]
CHIP_SWAP = [(i, i ^ 2) for i in range(4)]


def token_aux(seg_ext):
    seg = seg_ext[3:]
    n = seg.shape[0]
    tile_prev = jnp.repeat(seg_ext[2:n + 2:T], T)
    tile_last = jnp.repeat(seg[T - 1::T], T)
    cols = [seg == seg_ext[3 - k:n + 3 - k] for k in (1, 2, 3)] + [seg == tile_prev, seg == tile_last, seg - seg_ext[0]]
    lane = lax.broadcasted_iota(jnp.int32, (n, T), 1)
    out = jnp.zeros((n, T), f32)
    for i, c in enumerate(cols):
        out = jnp.where(lane == i, c.astype(f32)[:, None], out)
    return out


def solution(mesh):
    n_blocks = mesh.shape['sp']
    token_spec = seg_spec = P(('dp', 'sp', 'tp'))
    weight_specs = tuple(P(*['tp' if i == dim else None for i in range(dim + 1)]) for dim in (2, 2, 1, 1, 2, 0, 1, 0, 0, 0, 0, 0))

    def body(x_loc, seg_loc, w_zx, w_bc, w_dt, conv_x, conv_bc, bias_x, bias_bc, a_log, dt_bias, d_skip, norm_w, w_out):
        rows, d = x_loc.shape
        me = lax.axis_index('tp')
        ch = rows // NCH
        per, kper = rows // MT, ch // MT
        n_pl = mesh.shape['dp'] * n_blocks
        segs, tails, *parts = ahead_call(seg_loc, x_loc, w_out, n_blocks, n_pl)
        x_par = send(after(x_loc, segs), CORE_SWAP)
        x_dir = [send(v, CHIP_SWAP) for v in parts[:NCH]]
        w_half = [send(v, CHIP_SWAP) for v in parts[NCH:]]

        def w_gather(h, dep):
            return lax.all_gather(after(w_half[h], dep), ('dp', 'sp'), axis=0, tiled=True)

        aux = token_aux(jnp.concatenate([segs[0].reshape(-1)[-3:], segs[1:].reshape(-1)]))
        tails = tails.reshape(-1, d)
        w2, wb = w_zx.reshape(d, 2 * XW), w_bc.reshape(d, NB)
        pad = lambda v: jnp.pad(v.astype(f32), ((0, SUB - v.shape[0]), (0, 0)))
        cw = pad(jnp.concatenate([conv_x, bias_x[None]], axis=0))
        cwb = pad(jnp.concatenate([conv_bc.reshape(4, NB), bias_bc.reshape(1, NB)], axis=0))
        hp1 = jnp.pad(jnp.stack([dt_bias, a_log]), ((0, 6), (0, T - HEADS)))
        hp2 = pad(jnp.stack([jnp.repeat(d_skip, HEAD), norm_w.astype(f32)]))
        pre = jnp.stack([seq_slot(me, s) for s in range(4)]).astype(jnp.int32)
        weights = (w2, wb, w_dt)
        consts = (cw, cwb, hp1)

        def front(slots, part, parts, xs, halos, hrows, carry, into, per):
            return front_call(pre, aux, [lambda b, s=s: b[s] * parts + part for s in slots], xs, halos, hrows,
                              weights, carry, consts, into, part, parts, per=per)

        tail_row = lambda s: (lambda b: b[s] * HALO)
        *own, ends = front((0, 1), 0, 1, [x_loc, x_par], [tails] * 2, [tail_row(0), tail_row(1)], None, [], per)
        w_rem = [w_gather(0, ends)]
        x_dir[0] = after(x_dir[0], ends)
        rem, carry, x_fwd = [[], []], [None, None], []
        last = ends
        for k in range(NCH):
            x_fwd.append(send(x_dir[k], CORE_SWAP))
            for r, xs in ((0, x_dir), (1, x_fwd)):
                halo = (tails, tail_row(2 + r)) if k == 0 else (xs[k - 1], lambda b: ch - HALO)
                *rem[r], carry[r] = front((2 + r,), k, NCH, [after(xs[k], last)], [halo[0]], [halo[1]], carry[r], rem[r], kper)
                last = carry[r]
            if k + 1 < NCH:
                x_dir[k + 1] = after(x_dir[k + 1], carry[1])
        starts = chain_call(ends, carry[0], carry[1], n_blocks)
        w_rem.append(w_gather(1, starts))

        def mix(amaps, xs, arrs, start, **kw):
            return mixz_call(pre, aux, amaps, xs, arrs, w2, start, hp2, **kw)

        part_of = lambda s, k: (lambda b: b[s] * NCH + k)
        y_in = [[], []]
        c, cofs = starts, 3
        for k in range(NCH):
            yn, c = mix([part_of(3, k)], [x_fwd[k]], rem[1], c, nx=1, per=kper, ofs=k * kper, cofs=cofs)
            cofs = 0
            y_in[1].append(send(yn, CHIP_SWAP))
        yn, c = mix([part_of(2, k) for k in range(NCH)], x_dir, rem[0], after(starts, c), nx=1, per=per, ofs=0, cofs=2)
        y_in[0] = send(yn, CHIP_SWAP)
        y_own, _ = mix([lambda b: b[0], lambda b: b[1]], [x_loc, x_par], own, after(starts, c), nx=2, per=per, ofs=0, cofs=0)
        other = []
        for k in range(NCH):
            part = out_call(1, k, y_own, y_in[1][k], 0, w_out, w_rem)
            other.append(send(part, CORE_SWAP))
        y = None
        for k in range(NCH):
            y = out_call(0, k, y_own, y_in[0], k, w_out, w_rem, x_loc, other[k], y)
        return y

    return jax.shard_map(body, mesh=mesh, in_specs=(token_spec, seg_spec) + weight_specs, out_specs=token_spec, check_vma=False)
```

```python
import functools
import jax
import jax.numpy as jnp
from jax import lax
from jax.sharding import PartitionSpec as P
from jax.experimental import pallas as pl
from jax.experimental.pallas import tpu as pltpu

T = 128
XW = 2048
NB = 512
GW = 1024
D = 4096
TOK = 1024
HEADS, HEAD = 32, 64
XT = 512
MT = 256
HALO = 16
SUB = 8
MH = MT + HALO
LOG2E = 1.4426950408889634
NORM_EPS = 1e-5
MIB = 2**20
f32, bf16 = jnp.float32, jnp.bfloat16
MESH = pl.DeviceIdType.MESH
ONE = pl.Buffered(1)


def silu(v):
    h = 0.5 * v
    return h + h * jnp.tanh(h)


def lane_bcast(cols, h):
    return jnp.broadcast_to(cols[:, h:h + 1], (cols.shape[0], T))


def pair_bcast(cols, p):
    lanes = lax.broadcasted_iota(jnp.int32, (cols.shape[0], T), 1)
    return jnp.where(lanes < HEAD, lane_bcast(cols, 2 * p), lane_bcast(cols, 2 * p + 1))


def row(ref, r):
    return ref[r:r + 1, :]


def mac(a, b, ca=1, cb=0, **kw):
    return lax.dot_general(a, b, (((ca,), (cb,)), ((), ())), preferred_element_type=f32, **kw)


def rows_from(start, size):
    return pl.ds(start if isinstance(start, int) else pl.multiple_of(start, 16), size)


def front_kernel(pre, *refs, nx, per, where, ns, more, skip):
    srcs, auxs = refs[:ns], refs[ns:ns + nx]
    wx_ref, wb_ref, wdt_ref, cw_ref, cwb_ref, hp_ref, *cins = refs[ns + nx:][:6 + more]
    (xa_ref, bca_ref, dc_ref, cout_ref, xbuf, pbuf, bbuf, xw, bt, cum_all, wgt, abuf, sem) = refs[ns + nx + 6 + more + skip:]
    n = pl.program_id(0)
    last_n = XW // XT
    nm = nx * per
    rows = lax.broadcasted_iota(jnp.int32, (T, T), 0)
    cols = lax.broadcasted_iota(jnp.int32, (T, T), 1)
    tiles = [slice(t * T, (t + 1) * T) for t in range(MT // T)]

    def copies(m):
        src, row, halo, h = where[m]
        h = h(pre) if callable(h) else h
        if halo == src:
            return [pltpu.make_async_copy(srcs[src].at[rows_from(row - HALO, MH)], xbuf.at[m], sem.at[m])]
        return [pltpu.make_async_copy(srcs[halo].at[rows_from(h, HALO)], xbuf.at[m, pl.ds(0, HALO)], sem.at[m]),
                pltpu.make_async_copy(srcs[src].at[pl.ds(row, MT)], xbuf.at[m, pl.ds(HALO, MT)], sem.at[m])]

    def left(i):
        return slice(nm * MT + SUB * (i + 1), nm * MT + SUB * (i + 2))

    def heads_first(v):
        return pltpu.roll(v, lax.rem(T - (XT // HEAD) * (n - 1), T), 1)

    def at(m, ts):
        return pl.ds(pl.multiple_of(m * MT + ts.start, T), T)

    def conv(read, lo, w, keep):
        cs = slice(lo, lo + T)
        acc = read(0, cs) * row(w, 3)[:, cs] + row(w, 4)[:, cs]
        for k in range(3):
            acc = acc + (read(3 - k, cs) * w[k:k + 1, cs]) * keep[k]
        return silu(acc).astype(bf16)

    def taps(m, ts):
        return [lane_bcast(abuf[m, ts, :], 2 - k) for k in range(3)]

    def x_dot(m):
        pbuf[lax.rem(n, 2), m] = jnp.dot(xbuf[m], wx_ref[...], preferred_element_type=f32).astype(bf16).astype(f32)

    def setup(m, i, s):
        for ts in tiles:
            r0 = HALO + ts.start
            keep = taps(m, ts)
            for c in range(NB // T):
                act = conv(lambda d, cs: bbuf[r0 - d:r0 - d + T, cs], c * T, cwb_ref, keep)
                bca_ref[at(m, ts), c * T:(c + 1) * T] = act
                if c < 2:
                    bt[i, c, :, at(s, ts)] = act.T
            raw = bbuf[r0:r0 + T, NB:NB + T] + row(hp_ref, 0)
            dtv = jnp.maximum(raw, 0.0) + jnp.log1p(jnp.exp(-jnp.abs(raw)))
            log_a = -jnp.exp(row(hp_ref, 1)) * dtv * LOG2E
            cum = mac((rows >= cols).astype(f32), log_a, precision=lax.Precision.HIGHEST)
            dc_ref[at(m, ts), :] = jnp.where(cols < HEADS, cum, pltpu.roll(dtv, HEADS, 1))
            before = jnp.where((s == 0) & (ts.start == 0), 0.0, row(cum_all, nm * MT))
            cum = cum + before
            cum_all[at(m, ts), :] = cum
            cum_all[nm * MT:nm * MT + SUB, :] = jnp.broadcast_to(cum[T - 1:T, :], (8, T))
            wgt[at(m, ts), :] = dtv

    def weigh(i):
        lo, end = i * per * MT, (i + 1) * per * MT
        doc = abuf[end // MT - 1, MT - 1:MT, 5:6]
        last = row(cum_all, end - 1)
        keep_in = abuf[lo // MT, 0:1, 0:1] * (abuf[lo // MT, 0:1, 5:6] == doc).astype(f32)
        carry = jnp.broadcast_to(jnp.exp2(last) * keep_in, (8, T))
        for r in range(lo, end, T):
            keep = jnp.broadcast_to((abuf[r // MT, r % MT:r % MT + T, 5:6] == doc).astype(f32), (T, T))
            wgt[r:r + T, :] = jnp.exp2(last - cum_all[r:r + T, :]) * wgt[r:r + T, :] * keep
        cum_all[left(i), :] = carry

    def x_conv(m):
        slot = lax.rem(n + 1, 2)
        for ts in tiles:
            r0 = HALO + ts.start
            keep = taps(m, ts)
            wg = heads_first(wgt[at(m, ts), :])
            for p in range(XT // T):
                cs = slice(p * T, (p + 1) * T)
                xa = conv(lambda d, cs: pbuf[slot, m, r0 - d:r0 - d + T, cs], p * T, cw_ref, keep)
                xa_ref[at(m, ts), cs] = xa
                xw[at(m, ts), cs] = (xa.astype(f32) * pair_bcast(wg, p)).astype(bf16)

    def end_state():
        g = (n - 1) // (GW // XT)
        for i in range(nx):
            upd = jnp.dot(bt[i, g], xw[i * per * MT:(i + 1) * per * MT, :], preferred_element_type=f32)
            cr = heads_first(cum_all[left(i), :])
            for p in range(XT // T):
                cs = slice(p * T, (p + 1) * T)
                carry = pair_bcast(cr, p)
                if cins:
                    cout_ref[i, :T, cs] = cins[0][i, :T, cs] * jnp.broadcast_to(carry[:1], (T, T)) + upd[:, cs]
                    cout_ref[i, T:, cs] = cins[0][i, T:, cs] * carry
                else:
                    cout_ref[i, :T, cs] = upd[:, cs]
                    cout_ref[i, T:, cs] = carry

    @pl.when(n == 0)
    def _():
        for m in range(nm):
            for c in copies(m):
                c.start()
        bbuf[:, NB:] = jnp.zeros((MH, T), f32)
        for m in range(nm):
            i, s = divmod(m, per)
            abuf[m] = auxs[i][s * MT:(s + 1) * MT, :]

        @pl.loop(0, nm)
        def _(m):
            for k in range(nm):
                @pl.when(m == k)
                def _():
                    for c in copies(k):
                        c.wait()
            bbuf[:, 0:NB] = jnp.dot(xbuf[m], wb_ref[...], preferred_element_type=f32).astype(bf16).astype(f32)
            bbuf[:, NB:NB + HEADS] = jnp.dot(xbuf[m], wdt_ref[...], preferred_element_type=f32).astype(bf16).astype(f32)
            x_dot(m)
            setup(m, m // per, lax.rem(m, per))

        for i in range(nx):
            weigh(i)

    @pl.when((n > 0) & (n < last_n))
    def _():
        @pl.loop(0, nm)
        def _(m):
            x_dot(m)
            x_conv(m)

    @pl.when(n == last_n)
    def _():
        @pl.loop(0, nm)
        def _(m):
            x_conv(m)

    @pl.when(n > 0)
    def _():
        end_state()


def front_call(pre, aux, amaps, runs, weights, cin, consts, into, part, parts, *, per):
    nx = len(runs)
    srcs, where = [], []
    for ahead, row, arrays in runs:
        srcs.append(ahead)
        halo = len(srcs) - 1
        for arr in arrays:
            srcs.append(arr)
            for r in range(0, min(arr.shape[0], per * MT), MT):
                where.append((len(srcs) - 1, r, halo, row))
                halo, row = len(srcs) - 1, r + MT - HALO
    ns = len(srcs)
    nm = nx * per
    n = nm * MT
    nt = XW // XT
    w2, wb, wdt = weights
    hbm = pl.BlockSpec(memory_space=pl.ANY)
    prev = lambda j: jnp.maximum(j - 1, 0)
    whole = lambda *shape, mode=ONE, r=0: pl.BlockSpec(shape, lambda j, b: (r, 0), pipeline_mode=mode)
    cols = lambda k, r=0: pl.BlockSpec((k, XT), lambda j, b: (r, prev(j)))
    state = pl.BlockSpec((nx, T + 8, XT), lambda j, b: (0, 0, prev(j)))
    in_specs = [hbm] * ns + [pl.BlockSpec((per * MT, T), lambda j, b, f=f: (f(b), 0), pipeline_mode=ONE) for f in amaps] + [
        pl.BlockSpec((D, XT), lambda j, b: (0, nt + jnp.minimum(j, nt - 1))), whole(D, NB), whole(D, HEADS),
        cols(SUB), whole(SUB, NB), whole(SUB, T)] + ([] if cin is None else [state]) + [hbm] * len(into)
    n_in = len(in_specs) + 1
    gs = pltpu.PrefetchScalarGridSpec(
        num_scalar_prefetch=1, grid=(nt + 1,), in_specs=in_specs,
        out_specs=[cols(n, part), whole(n, NB, mode=None, r=part), whole(n, T, mode=None, r=part), state],
        scratch_shapes=[pltpu.VMEM((nm, MH, D), bf16), pltpu.VMEM((2, nm, MH, XT), f32), pltpu.VMEM((MH, NB + T), f32),
                        pltpu.VMEM((n, XT), bf16), pltpu.VMEM((nx, 2, T, per * MT), bf16),
                        pltpu.VMEM((n + 8 * (nx + 1), T), f32), pltpu.VMEM((n, T), f32), pltpu.VMEM((nm, MT, T), f32),
                        pltpu.SemaphoreType.DMA((nm,))],
    )
    return pl.pallas_call(
        functools.partial(front_kernel, nx=nx, per=per, where=where, ns=ns, more=int(cin is not None), skip=len(into)), grid_spec=gs,
        out_shape=[jax.ShapeDtypeStruct((parts * n, XW), bf16), jax.ShapeDtypeStruct((parts * n, NB), bf16),
                   jax.ShapeDtypeStruct((parts * n, T), f32), jax.ShapeDtypeStruct((nx, T + SUB, XW), f32)],
        input_output_aliases={n_in - len(into) + o: o for o in range(len(into))},
        compiler_params=pltpu.CompilerParams(dimension_semantics=("arbitrary",), vmem_limit_bytes=62 * MIB),
        cost_estimate=pl.CostEstimate(flops=n * 25_000_000, bytes_accessed=n * 10000, transcendentals=n * 4096),
        name="front",
    )(pre, *srcs, *[aux] * nx, w2, wb, wdt, *consts, *([] if cin is None else [cin]), *into)


def mixz_kernel(pre, *refs, ns, first):
    xs_, auxs = refs[:ns], refs[ns:2 * ns]
    (xa_ref, bg_ref, cg_ref, dc_ref, wz_ref, cin_ref, hp_ref, yn_ref, cout_ref, xv, av, zbuf, ybuf, xw, state) = refs[2 * ns:]
    g, i, tile = pl.program_id(0), pl.program_id(1), pl.program_id(2)
    n_tiles = pl.num_programs(2)

    @pl.when(tile == 0)
    def _():
        state[...] = cin_ref[0]

    at = i * n_tiles + tile
    for k in range(ns):
        @pl.when((at >= first[k]) & (at < first[k + 1]))
        def _():
            xv[...] = xs_[k][...]
            av[...] = auxs[k][...]

    rows = lax.broadcasted_iota(jnp.int32, (T, T), 0)
    cols = lax.broadcasted_iota(jnp.int32, (T, T), 1)
    lo_half = cols < 64
    zero = jnp.zeros((T, T), bf16)
    for t in range(MT // T):
        rs = slice(t * T, (t + 1) * T)
        aux = av[rs, :]
        auxt = aux.T
        mask = (rows >= cols) & (lane_bcast(aux, 5) == jnp.broadcast_to(auxt[5:6, :], (T, T)))
        k_in = lane_bcast(aux, 3)
        k_end = lane_bcast(aux, 4)
        dc = pltpu.roll(dc_ref[rs, :], lax.rem(T - 16 * g, T), 1)
        dct = dc.T
        rel = dct[:HEADS // 2, :] - jnp.log2(dct[HEADS:HEADS + HEADS // 2, :])
        bg, cg = bg_ref[rs, :], cg_ref[rs, :]
        sm = jnp.where(mask, mac(cg, bg, 1, 1), 0.0)
        ybuf[...] = mac(cg, state[...].astype(bf16))
        sq = jnp.zeros((T, T), f32)
        if t == 0:
            zbuf[...] = jnp.dot(xv[...], wz_ref[...], preferred_element_type=f32).astype(bf16).astype(f32)
        for p in range(GW // T):
            cs = slice(p * T, (p + 1) * T)
            xa = xa_ref[rs, cs]
            xaf = xa.astype(f32)
            c0, c1 = lane_bcast(dc, 2 * p), lane_bcast(dc, 2 * p + 1)
            mixes = []
            for hh, cb in ((2 * p, c0), (2 * p + 1, c1)):
                diff = jnp.minimum(cb - jnp.broadcast_to(rel[hh:hh + 1, :], (T, T)), 126.0)
                mixes.append((sm * jnp.exp2(diff)).astype(bf16))
            lhs = jnp.concatenate(mixes, axis=1)
            rhs = jnp.concatenate([jnp.where(lo_half, xa, zero), jnp.where(lo_half, zero, xa)], axis=0)
            y = mac(lhs, rhs)
            cump = jnp.where(lo_half, c0, c1)
            dtp = pair_bcast(dc, HEADS // 2 + p)
            last = cump[T - 1:T, :]
            xw[:, cs] = (xaf * (jnp.exp2(last - cump) * dtp * k_end)).astype(bf16)
            y = y + ybuf[:, cs] * (jnp.exp2(cump) * k_in) + hp_ref[0:1, cs] * xaf
            v = y * silu(zbuf[rs, cs])
            ybuf[:, cs] = v
            sq = sq + v * v
            state[:, cs] = state[:, cs] * (jnp.exp2(last) * k_in[T - 1:T, :])
        ms = jnp.sum(sq, axis=1, keepdims=True) * (1.0 / GW)
        r = jnp.broadcast_to(lax.rsqrt(ms + NORM_EPS), (T, T))
        for p in range(GW // T):
            cs = slice(p * T, (p + 1) * T)
            yn_ref[rs, cs] = (ybuf[:, cs] * r * hp_ref[1:2, cs]).astype(bf16)
        state[...] = state[...] + mac(bg, xw[...], 0, 0)

    @pl.when(tile == n_tiles - 1)
    def _():
        cout_ref[0] = state[...]


def mixz_call(pre, aux, amaps, xs, arrs, w2, cin, hp, *, nx, per, ofs, cofs):
    ns = len(xs)
    first = [0]
    for v in xs:
        first.append(min(first[-1] + v.shape[0] // MT, nx * per))
    n = nx * per * MT
    xa, bca, dc = arrs
    piece = lambda k: (lambda i, t: jnp.clip(i * per + t - first[k], 0, first[k + 1] - first[k] - 1))
    rows = lambda w, c, o=ofs: pl.BlockSpec((MT, w), lambda g, i, t, b: (o + i * per + t, c(g)))
    state = lambda ofs: pl.BlockSpec((1, T, GW), lambda g, i, t, b: (ofs + i, 0, g))
    cols = lambda k: pl.BlockSpec((k, GW), lambda g, i, t, b: (0, g))
    in_specs = [pl.BlockSpec((MT, D), lambda g, i, t, b, k=k: (piece(k)(i, t), 0)) for k in range(ns)]
    in_specs += [pl.BlockSpec((MT, T), lambda g, i, t, b, k=k: (amaps[k](b) + piece(k)(i, t), 0)) for k in range(ns)]
    same = lambda g: g
    in_specs += [rows(GW, same), rows(T, same), rows(T, lambda g: 2 + g), rows(T, lambda g: 0), cols(D), state(cofs), cols(8)]
    gs = pltpu.PrefetchScalarGridSpec(
        num_scalar_prefetch=1, grid=(2, nx, per), in_specs=in_specs, out_specs=[rows(GW, same, 0), state(0)],
        scratch_shapes=[pltpu.VMEM((MT, D), bf16), pltpu.VMEM((MT, T), f32), pltpu.VMEM((MT, GW), f32), pltpu.VMEM((T, GW), f32),
                        pltpu.VMEM((T, GW), bf16), pltpu.VMEM((T, GW), f32)],
    )
    return pl.pallas_call(
        functools.partial(mixz_kernel, ns=ns, first=first), grid_spec=gs,
        out_shape=[jax.ShapeDtypeStruct((n, XW), bf16), jax.ShapeDtypeStruct((nx, T, XW), f32)],
        compiler_params=pltpu.CompilerParams(dimension_semantics=("arbitrary",) * 3, vmem_limit_bytes=60 * MIB),
        cost_estimate=pl.CostEstimate(flops=n * 20_000_000, bytes_accessed=n * 14000, transcendentals=n * 10000),
        name="mixz",
    )(pre, *xs, *[aux] * ns, xa, bca, bca, dc, w2, cin, hp)


def seq_slot(me, s):
    c = (me % 2 + s % 2) % 2
    y = (me // 2 + s // 2) % 2
    return 2 * y + c


PARTS = (2, 1, 1)
NCH = 2


def count(flag):
    return jnp.where(flag, 1, 0)


def ahead_kernel(n_blocks, n_pl, seg_ref, tail_ref, x_hbm, w_hbm, segs_ref, tails_ref, *refs):
    me, blk = lax.axis_index('tp'), lax.axis_index('sp')
    *outs, xbuf, wbuf, in_sem, out_sem, send_sem, recv_sem = refs
    xs, ws = outs[:len(PARTS)], outs[len(PARTS):]
    step = ws[0].shape[0]
    place = lax.axis_index('dp') * n_blocks + blk
    pieces, row = [], 0
    for dst in xs:
        size = dst.shape[0]
        pieces.append((x_hbm.at[pl.ds(row, size)], xbuf.at[pl.ds(row, size)], dst))
        row += size
    for k, dst in enumerate(ws):
        pieces.append((w_hbm.at[pl.ds(pl.multiple_of((k * n_pl + place) * step, HALO), step)], wbuf.at[k], dst))
    moves = [(pltpu.make_async_copy(src, buf, in_sem.at[k]), pltpu.make_async_copy(buf, dst, out_sem.at[k]))
             for k, (src, buf, dst) in enumerate(pieces)]
    for load, _ in moves:
        load.start()
    barrier = pltpu.get_barrier_semaphore()
    others = [{'tp': seq_slot(me, s)} for s in (1, 2, 3)]
    before = {'sp': jnp.maximum(blk - 1, 0), 'tp': 3}
    after = [{'sp': jnp.minimum(blk + 1, n_blocks - 1), 'tp': q} for q in range(4)]
    sends_on = (me == 3) & (blk < n_blocks - 1)
    for dev in others:
        pl.semaphore_signal(barrier, inc=1, device_id=dev, device_id_type=MESH)

    @pl.when(blk > 0)
    def _():
        pl.semaphore_signal(barrier, inc=1, device_id=before, device_id_type=MESH)

    @pl.when(sends_on)
    def _():
        for dev in after:
            pl.semaphore_signal(barrier, inc=1, device_id=dev, device_id_type=MESH)

    pl.semaphore_wait(barrier, 3 + count(blk > 0) + 4 * count(sends_on))

    def copies(dev, entry, k, rk):
        return [pltpu.make_async_remote_copy(src_ref=seg_ref, dst_ref=segs_ref.at[entry], send_sem=send_sem.at[k, 0],
                                             recv_sem=recv_sem.at[rk, 0], device_id=dev, device_id_type=MESH),
                pltpu.make_async_remote_copy(src_ref=tail_ref, dst_ref=tails_ref.at[entry], send_sem=send_sem.at[k, 1],
                                             recv_sem=recv_sem.at[rk, 1], device_id=dev, device_id_type=MESH)]

    inner = [copies(dev, me + 1, k, k) for k, dev in enumerate(others)]
    outer = [copies(dev, 0, 3 + q, 3) for q, dev in enumerate(after)]
    for cs in inner:
        for c in cs:
            c.start()

    @pl.when(sends_on)
    def _():
        for cs in outer:
            for c in cs:
                c.start()

    for load, store in moves:
        load.wait()
        store.start()
    segs_ref[me + 1] = seg_ref[...]
    tails_ref[me + 1] = tail_ref[...]

    @pl.when(blk == 0)
    def _():
        segs_ref[0] = jnp.zeros_like(seg_ref)
        tails_ref[0] = jnp.zeros_like(tail_ref)

    for cs in inner:
        for c in cs:
            c.wait_send()
            c.wait_recv()

    @pl.when(sends_on)
    def _():
        for cs in outer:
            for c in cs:
                c.wait_send()

    @pl.when(blk > 0)
    def _():
        for c in outer[0]:
            c.wait_recv()

    for _, store in moves:
        store.wait()


def ahead_call(seg, x, w, n_blocks, n_pl):
    rows = x.shape[0]
    step = w.shape[0] // (NCH * n_pl)
    n_out = len(PARTS) + NCH
    vmem, hbm = pl.BlockSpec(memory_space=pltpu.VMEM), pl.BlockSpec(memory_space=pl.ANY)
    sds = jax.ShapeDtypeStruct
    return pl.pallas_call(
        functools.partial(ahead_kernel, n_blocks, n_pl),
        grid=(1,),
        in_specs=[vmem, pl.BlockSpec((HALO, D), lambda i: (rows // HALO - 1, 0)), hbm, hbm],
        out_specs=[vmem] * 2 + [hbm] * n_out,
        out_shape=[sds((5, rows // T, T), jnp.int32), sds((5, HALO, D), bf16)] + [sds((p * MT, D), bf16) for p in PARTS] + [sds((step, D), bf16)] * NCH,
        scratch_shapes=[pltpu.VMEM((rows, D), bf16), pltpu.VMEM((NCH, step, D), bf16), pltpu.SemaphoreType.DMA((n_out,)),
                        pltpu.SemaphoreType.DMA((n_out,)), pltpu.SemaphoreType.DMA((7, 2)), pltpu.SemaphoreType.DMA((4, 2))],
        compiler_params=pltpu.CompilerParams(collective_id=0, has_side_effects=True, vmem_limit_bytes=24 * MIB),
        name="ahead",
    )(seg.reshape(rows // T, T), x, x, w)


CW = 256


def chain_kernel(n_blocks, e01_ref, e2_ref, e3_ref, out_hbm, ebuf, sbuf, obuf, out_ref, lsem, osem, send_sem, recv_sem):
    me, blk = lax.axis_index('tp'), lax.axis_index('sp')
    srcs = [e01_ref.at[0], e01_ref.at[1], e2_ref.at[0], e3_ref.at[0]]
    loads = [pltpu.make_async_copy(src, ebuf.at[seq_slot(me, s)], lsem.at[s]) for s, src in enumerate(srcs)]
    for c in loads:
        c.start()
    barrier = pltpu.get_barrier_semaphore()
    before = {'sp': jnp.maximum(blk - 1, 0)}
    after = {'sp': jnp.minimum(blk + 1, n_blocks - 1)}

    @pl.when(blk > 0)
    def _():
        pl.semaphore_signal(barrier, inc=1, device_id=before, device_id_type=MESH)

    @pl.when(blk < n_blocks - 1)
    def _():
        pl.semaphore_signal(barrier, inc=1, device_id=after, device_id_type=MESH)

    pl.semaphore_wait(barrier, count(blk > 0) + count(blk < n_blocks - 1))

    for c in loads:
        c.wait()

    def through(q, s, cs):
        return ebuf[q, :T, cs] + ebuf[q, T:T + 1, cs] * s

    for q in (1, 2, 3):
        ebuf[q, :T, :] = through(q, ebuf[q - 1, :T, :], slice(None))
        ebuf[q, T:, :] = ebuf[q, T:, :] * ebuf[q - 1, T:, :]

    @pl.when(blk == 0)
    def _():
        sbuf[...] = jnp.zeros_like(sbuf)

    n = XW // CW

    def store(j):
        cs = pl.ds(j * CW, CW)
        return pltpu.make_async_copy(out_ref.at[:, :, cs], out_hbm.at[:, :, cs], osem.at[j])

    def send(j):
        return pltpu.make_async_remote_copy(src_ref=obuf.at[j], dst_ref=sbuf.at[j], send_sem=send_sem.at[j],
                                            recv_sem=recv_sem.at[j], device_id=after, device_id_type=MESH)

    for j in range(n):
        cs = slice(j * CW, (j + 1) * CW)

        @pl.when(blk > 0)
        def _():
            send(j).wait_recv()

        @pl.when(blk < n_blocks - 1)
        def _():
            obuf[j] = through(3, sbuf[j], cs)
            send(j).start()

    for j in range(n):
        cs = slice(j * CW, (j + 1) * CW)
        for q in range(4):
            v = through(q - 1, sbuf[j], cs) if q else sbuf[j]
            out_ref[seq_slot(me, q), :, cs] = v
        store(j).start()

    @pl.when(blk < n_blocks - 1)
    def _():
        for j in range(n):
            send(j).wait_send()

    for j in range(n):
        store(j).wait()


def chain_call(e01, e2, e3, n_blocks):
    hbm = pl.BlockSpec(memory_space=pltpu.HBM)
    n = XW // CW
    return pl.pallas_call(
        functools.partial(chain_kernel, n_blocks),
        in_specs=[hbm] * 3,
        out_specs=hbm,
        out_shape=jax.ShapeDtypeStruct((4, T, XW), f32),
        scratch_shapes=[pltpu.VMEM((4, T + SUB, XW), f32), pltpu.VMEM((n, T, CW), f32), pltpu.VMEM((n, T, CW), f32),
                        pltpu.VMEM((4, T, XW), f32),                         pltpu.SemaphoreType.DMA((4,)), pltpu.SemaphoreType.DMA((n,)),
                        pltpu.SemaphoreType.DMA((n,)), pltpu.SemaphoreType.DMA((n,))],
        compiler_params=pltpu.CompilerParams(collective_id=1, has_side_effects=True, vmem_limit_bytes=63 * MIB),
        name="chain",
    )(e01, e2, e3)


NT = 512


def out_kernel(y_ref, yr_ref, w_ref, wr0_ref, wr1_ref, *refs):
    h = XW // 2
    acc = (jnp.dot(y_ref[...], w_ref[...], preferred_element_type=f32)
           + jnp.dot(yr_ref[:, 0:h], wr0_ref[...], preferred_element_type=f32)
           + jnp.dot(yr_ref[:, h:], wr1_ref[...], preferred_element_type=f32))
    if len(refs) > 1:
        x_ref, other_ref = refs[:2]
        acc = x_ref[...].astype(f32) + (acc + other_ref[...])
    refs[-1][...] = acc.astype(refs[-1].dtype)


def out_call(run, part, y, yr, rpart, w, wr, x=None, other=None, into=None):
    rows = TOK // NCH
    h = XW // 2
    at = lambda r: (lambda j: (r, j))
    cols = at(0)
    ins = [y, yr, w, *wr]
    specs = [pl.BlockSpec((rows, XW), lambda j: (run * (TOK // rows) + part, 0), pipeline_mode=ONE),
             pl.BlockSpec((rows, XW), lambda j: (rpart, 0), pipeline_mode=ONE),
             pl.BlockSpec((XW, NT), cols), pl.BlockSpec((h, NT), cols), pl.BlockSpec((h, NT), cols)]
    alias = {}
    if x is not None:
        ins += [x, other]
        specs += [pl.BlockSpec((rows, NT), at(part)), pl.BlockSpec((rows, NT), cols)]
    if into is not None:
        alias = {len(ins): 0}
        ins.append(into)
        specs.append(pl.BlockSpec(memory_space=pl.ANY))
    return pl.pallas_call(
        out_kernel,
        grid=(D // NT,), in_specs=specs,
        out_specs=pl.BlockSpec((rows, NT), cols if x is None else at(part)),
        out_shape=jax.ShapeDtypeStruct((rows, D), f32) if x is None else jax.ShapeDtypeStruct(x.shape, bf16),
        input_output_aliases=alias,
        compiler_params=pltpu.CompilerParams(dimension_semantics=("arbitrary",), vmem_limit_bytes=56 * MIB),
        cost_estimate=pl.CostEstimate(flops=rows * 33_000_000, bytes_accessed=rows * 100000, transcendentals=0),
        name="out_proj",
    )(*ins)


def send(v, perm):
    return lax.ppermute(v, 'tp', perm)


def after(v, *deps):
    return lax.optimization_barrier((v,) + deps)[0]


CORE_SWAP = [(i, i ^ 1) for i in range(4)]
CHIP_SWAP = [(i, i ^ 2) for i in range(4)]


def token_aux(seg_ext):
    seg = seg_ext[3:]
    n = seg.shape[0]
    tile_prev = jnp.repeat(seg_ext[2:n + 2:T], T)
    tile_last = jnp.repeat(seg[T - 1::T], T)
    cols = [seg == seg_ext[3 - k:n + 3 - k] for k in (1, 2, 3)] + [seg == tile_prev, seg == tile_last, seg - seg_ext[0]]
    lane = lax.broadcasted_iota(jnp.int32, (n, T), 1)
    out = jnp.zeros((n, T), f32)
    for i, c in enumerate(cols):
        out = jnp.where(lane == i, c.astype(f32)[:, None], out)
    return out


def solution(mesh):
    n_blocks = mesh.shape['sp']
    token_spec = seg_spec = P(('dp', 'sp', 'tp'))
    weight_specs = tuple(P(*['tp' if i == dim else None for i in range(dim + 1)]) for dim in (2, 2, 1, 1, 2, 0, 1, 0, 0, 0, 0, 0))

    def body(x_loc, seg_loc, w_zx, w_bc, w_dt, conv_x, conv_bc, bias_x, bias_bc, a_log, dt_bias, d_skip, norm_w, w_out):
        rows, d = x_loc.shape
        me = lax.axis_index('tp')
        per, kper = rows // MT, rows // (NCH * MT)
        n_pl = mesh.shape['dp'] * n_blocks
        segs, tails, *parts = ahead_call(seg_loc, x_loc, w_out, n_blocks, n_pl)
        x_par = send(after(x_loc, segs), CORE_SWAP)
        x_dir = [send(v, CHIP_SWAP) for v in parts[:len(PARTS)]]
        w_half = [send(v, CHIP_SWAP) for v in parts[len(PARTS):]]

        def w_gather(h, dep):
            return lax.all_gather(after(w_half[h], dep), ('dp', 'sp'), axis=0, tiled=True)

        aux = token_aux(jnp.concatenate([segs[0].reshape(-1)[-3:], segs[1:].reshape(-1)]))
        tails = tails.reshape(-1, d)
        w2, wb = w_zx.reshape(d, 2 * XW), w_bc.reshape(d, NB)
        pad = lambda v: jnp.pad(v.astype(f32), ((0, SUB - v.shape[0]), (0, 0)))
        cw = pad(jnp.concatenate([conv_x, bias_x[None]], axis=0))
        cwb = pad(jnp.concatenate([conv_bc.reshape(4, NB), bias_bc.reshape(1, NB)], axis=0))
        hp1 = jnp.pad(jnp.stack([dt_bias, a_log]), ((0, 6), (0, T - HEADS)))
        hp2 = pad(jnp.stack([jnp.repeat(d_skip, HEAD), norm_w.astype(f32)]))
        pre = jnp.stack([seq_slot(me, s) for s in range(4)]).astype(jnp.int32)
        weights = (w2, wb, w_dt)
        consts = (cw, cwb, hp1)

        def front(slots, part, parts, runs, carry, into, per):
            return front_call(pre, aux, [lambda b, s=s: b[s] * parts + part for s in slots], runs, weights, carry, consts,
                              into, part, parts, per=per)

        tail_row = lambda s: (lambda b: b[s] * HALO)
        *own, ends = front((0, 1), 0, 1, [(tails, tail_row(0), [x_loc]), (tails, tail_row(1), [x_par])], None, [], per)
        w_rem = [w_gather(0, ends)]
        x_dir[0] = after(x_dir[0], ends)
        x_fwd = [send(x_dir[0], CORE_SWAP)]
        *rem2, c2 = front((2,), 0, NCH, [(tails, tail_row(2), x_dir[:1])], None, [], kper)
        *rem3, c3 = front((3,), 0, NCH, [(tails, tail_row(3), [after(x_fwd[0], c2)])], None, [], kper)
        x_dir[1] = after(x_dir[1], c2)
        x_fwd.append(send(x_dir[1], CORE_SWAP))
        end = lambda k: PARTS[k] * MT - HALO
        *rem2, c2 = front((2,), 2, 4, [(x_dir[0], end(0), [after(x_dir[1], c3)])], c2, rem2, 1)
        x_dir[2] = after(x_dir[2], c2)
        x_fwd.append(send(x_dir[2], CORE_SWAP))
        *rem2, c2 = front((2,), 3, 4, [(x_dir[1], end(1), [x_dir[2]])], c2, rem2, 1)
        *rem3, c3 = front((3,), 1, NCH, [(x_fwd[0], end(0), [after(x_fwd[1], c2), x_fwd[2]])], c3, rem3, kper)
        starts = chain_call(ends, c2, c3, n_blocks)
        w_rem.append(w_gather(1, starts))

        def mix(amaps, xs, arrs, start, **kw):
            return mixz_call(pre, aux, amaps, xs, arrs, w2, start, hp2, **kw)

        at = lambda s, k=0: (lambda b: b[s] * per + k)
        yn, c = mix([at(3)], x_fwd[:1], rem3, starts, nx=1, per=kper, ofs=0, cofs=3)
        y_in = [send(yn, CHIP_SWAP)]
        yn, c = mix([at(3, 2), at(3, 3)], x_fwd[1:], rem3, c, nx=1, per=kper, ofs=kper, cofs=0)
        y_in.append(send(yn, CHIP_SWAP))
        yn, c = mix([at(2), at(2, 2), at(2, 3)], x_dir, rem2, after(starts, c), nx=1, per=per, ofs=0, cofs=2)
        y_in.append(send(yn, CHIP_SWAP))
        y_own, _ = mix([at(0), at(1)], [x_loc, x_par], own, after(starts, c), nx=2, per=per, ofs=0, cofs=0)
        other = []
        for k in range(NCH):
            part = out_call(1, k, y_own, y_in[k], 0, w_out, w_rem)
            other.append(send(part, CORE_SWAP))
        y = None
        for k in range(NCH):
            y = out_call(0, k, y_own, y_in[2], k, w_out, w_rem, x_loc, other[k], y)
        return y

    return jax.shard_map(body, mesh=mesh, in_specs=(token_spec, seg_spec) + weight_specs, out_specs=token_spec, check_vma=False)
```

```python
import functools
import jax
import jax.numpy as jnp
from jax import lax
from jax.sharding import PartitionSpec as P
from jax.experimental import pallas as pl
from jax.experimental.pallas import tpu as pltpu

T = 128
XW = 2048
NB = 512
GW = 1024
D = 4096
TOK = 1024
HEADS, HEAD = 32, 64
XT = 512
MT = 256
HALO = 16
SUB = 8
MH = MT + HALO
LOG2E = 1.4426950408889634
NORM_EPS = 1e-5
MIB = 2**20
f32, bf16 = jnp.float32, jnp.bfloat16
MESH = pl.DeviceIdType.MESH
ONE = pl.Buffered(1)


def silu(v):
    h = 0.5 * v
    return h + h * jnp.tanh(h)


def lane_bcast(cols, h):
    return jnp.broadcast_to(cols[:, h:h + 1], (cols.shape[0], T))


def pair_bcast(cols, p):
    lanes = lax.broadcasted_iota(jnp.int32, (cols.shape[0], T), 1)
    return jnp.where(lanes < HEAD, lane_bcast(cols, 2 * p), lane_bcast(cols, 2 * p + 1))


def columns(flags):
    return jnp.concatenate([flags, jnp.zeros((T - SUB, T), f32)], axis=0).T


def row(ref, r):
    return ref[r:r + 1, :]


def mac(a, b, ca=1, cb=0, **kw):
    return lax.dot_general(a, b, (((ca,), (cb,)), ((), ())), preferred_element_type=f32, **kw)


def rows_from(start, size):
    return pl.ds(start if isinstance(start, int) else pl.multiple_of(start, 16), size)


def front_kernel(pre, *refs, nx, per, where, ns, more, skip):
    srcs, auxs = refs[:ns], refs[ns:ns + nx]
    wx_ref, wb_ref, wdt_ref, cw_ref, cwb_ref, hp_ref, *cins = refs[ns + nx:][:6 + more]
    (xa_ref, bca_ref, dc_ref, cout_ref, xbuf, pbuf, bbuf, xw, bt, cum_all, wgt, abuf, sem) = refs[ns + nx + 6 + more + skip:]
    n = pl.program_id(0)
    last_n = XW // XT
    nm = nx * per
    rows = lax.broadcasted_iota(jnp.int32, (T, T), 0)
    cols = lax.broadcasted_iota(jnp.int32, (T, T), 1)
    lo_half = cols < HEAD
    tiles = [slice(t * T, (t + 1) * T) for t in range(MT // T)]

    def copies(m):
        src, row, halo, h = where[m]
        h = h(pre) if callable(h) else h
        if halo == src:
            return [pltpu.make_async_copy(srcs[src].at[rows_from(row - HALO, MH)], xbuf.at[m], sem.at[m])]
        return [pltpu.make_async_copy(srcs[halo].at[rows_from(h, HALO)], xbuf.at[m, pl.ds(0, HALO)], sem.at[m]),
                pltpu.make_async_copy(srcs[src].at[pl.ds(row, MT)], xbuf.at[m, pl.ds(HALO, MT)], sem.at[m])]

    def left(i):
        return slice(nm * MT + SUB * (i + 1), nm * MT + SUB * (i + 2))

    def heads_first(v):
        return pltpu.roll(v, lax.rem(T - (XT // HEAD) * (n - 1), T), 1)

    def at(m, ts):
        return pl.ds(pl.multiple_of(m * MT + ts.start, T), T)

    def conv(read, lo, w, keep):
        cs = slice(lo, lo + T)
        acc = read(0, cs) * row(w, 3)[:, cs] + row(w, 4)[:, cs]
        for k in range(3):
            acc = acc + (read(3 - k, cs) * w[k:k + 1, cs]) * keep[k]
        return silu(acc).astype(bf16)

    def taps(m, ts):
        return [lane_bcast(abuf[m, ts, :], 2 - k) for k in range(3)]

    def x_dot(m):
        pbuf[lax.rem(n, 2), m] = jnp.dot(xbuf[m], wx_ref[...], preferred_element_type=f32).astype(bf16).astype(f32)

    def setup(m, i, s):
        for ts in tiles:
            r0 = HALO + ts.start
            keep = taps(m, ts)
            for c in range(NB // T):
                act = conv(lambda d, cs: bbuf[r0 - d:r0 - d + T, cs], c * T, cwb_ref, keep)
                bca_ref[at(m, ts), c * T:(c + 1) * T] = act
                if c < 2:
                    bt[i, c, :, at(s, ts)] = act.T
            raw = bbuf[r0:r0 + T, NB:NB + T] + row(hp_ref, 0)
            dtv = jnp.maximum(raw, 0.0) + jnp.log1p(jnp.exp(-jnp.abs(raw)))
            log_a = -jnp.exp(row(hp_ref, 1)) * dtv * LOG2E
            cum = mac((rows >= cols).astype(f32), log_a, precision=lax.Precision.HIGHEST)
            dc_ref[at(m, ts), :] = jnp.where(cols < HEADS, cum, pltpu.roll(dtv, HEADS, 1))
            before = jnp.where((s == 0) & (ts.start == 0), 0.0, row(cum_all, nm * MT))
            cum = cum + before
            cum_all[at(m, ts), :] = cum
            cum_all[nm * MT:nm * MT + SUB, :] = jnp.broadcast_to(cum[T - 1:T, :], (8, T))
            wgt[at(m, ts), :] = dtv

    def weigh(i):
        lo, end = i * per * MT, (i + 1) * per * MT
        doc = abuf[end // MT - 1, MT - 1:MT, 5:6]
        last = row(cum_all, end - 1)
        keep_in = abuf[lo // MT, 0:1, 0:1] * (abuf[lo // MT, 0:1, 5:6] == doc).astype(f32)
        carry = jnp.broadcast_to(jnp.exp2(last) * keep_in, (8, T))
        for r in range(lo, end, T):
            keep = jnp.broadcast_to((abuf[r // MT, r % MT:r % MT + T, 5:6] == doc).astype(f32), (T, T))
            wgt[r:r + T, :] = jnp.exp2(last - cum_all[r:r + T, :]) * wgt[r:r + T, :] * keep
        cum_all[left(i), :] = carry

    def x_conv(m):
        slot = lax.rem(n + 1, 2)
        for ts in tiles:
            r0 = HALO + ts.start
            keep = taps(m, ts)
            wg = heads_first(wgt[at(m, ts), :])
            for p in range(XT // T):
                cs = slice(p * T, (p + 1) * T)
                xa = conv(lambda d, cs: pbuf[slot, m, r0 - d:r0 - d + T, cs], p * T, cw_ref, keep)
                xa_ref[at(m, ts), cs] = xa
                xw[at(m, ts), cs] = (xa.astype(f32) * pair_bcast(wg, p)).astype(bf16)

    def end_state():
        g = (n - 1) // (GW // XT)
        for i in range(nx):
            upd = jnp.dot(bt[i, g], xw[i * per * MT:(i + 1) * per * MT, :], preferred_element_type=f32)
            cr = heads_first(cum_all[left(i), :])
            for p in range(XT // T):
                cs = slice(p * T, (p + 1) * T)
                carry = pair_bcast(cr, p)
                if cins:
                    cout_ref[i, :T, cs] = cins[0][i, :T, cs] * jnp.broadcast_to(carry[:1], (T, T)) + upd[:, cs]
                    cout_ref[i, T:, cs] = cins[0][i, T:, cs] * carry
                else:
                    cout_ref[i, :T, cs] = upd[:, cs]
                    cout_ref[i, T:, cs] = carry

    @pl.when(n == 0)
    def _():
        for m in range(nm):
            for c in copies(m):
                c.start()
        bbuf[:, NB:] = jnp.zeros((MH, T), f32)
        for m in range(nm):
            i, s = divmod(m, per)
            for ts in tiles:
                abuf[m, ts, :] = columns(auxs[i][(s * MT + ts.start) // T])

        @pl.loop(0, nm)
        def _(m):
            for k in range(nm):
                @pl.when(m == k)
                def _():
                    for c in copies(k):
                        c.wait()
            bbuf[:, 0:NB] = jnp.dot(xbuf[m], wb_ref[...], preferred_element_type=f32).astype(bf16).astype(f32)
            bbuf[:, NB:NB + HEADS] = mac(xbuf[m], wdt_ref[...], 1, 1).astype(bf16).astype(f32)
            x_dot(m)
            setup(m, m // per, lax.rem(m, per))

        for i in range(nx):
            weigh(i)

    @pl.when((n > 0) & (n < last_n))
    def _():
        @pl.loop(0, nm)
        def _(m):
            x_dot(m)
            x_conv(m)

    @pl.when(n == last_n)
    def _():
        @pl.loop(0, nm)
        def _(m):
            x_conv(m)

    @pl.when(n > 0)
    def _():
        end_state()


def front_call(pre, aux, amaps, runs, weights, cin, consts, into, part, parts, *, per):
    nx = len(runs)
    srcs, where = [], []
    for ahead, row, arrays in runs:
        srcs.append(ahead)
        halo = len(srcs) - 1
        for arr in arrays:
            srcs.append(arr)
            for r in range(0, min(arr.shape[0], per * MT), MT):
                where.append((len(srcs) - 1, r, halo, row))
                halo, row = len(srcs) - 1, r + MT - HALO
    ns = len(srcs)
    nm = nx * per
    n = nm * MT
    nt = XW // XT
    w2, wb, wdt = weights
    hbm = pl.BlockSpec(memory_space=pl.ANY)
    prev = lambda j: jnp.maximum(j - 1, 0)
    whole = lambda *shape, mode=ONE, r=0: pl.BlockSpec(shape, lambda j, b: (r, 0), pipeline_mode=mode)
    cols = lambda k, r=0: pl.BlockSpec((k, XT), lambda j, b: (r, prev(j)))
    state = pl.BlockSpec((nx, T + 8, XT), lambda j, b: (0, 0, prev(j)))
    in_specs = [hbm] * ns + [pl.BlockSpec((per * MT // T, SUB, T), lambda j, b, f=f: (f(b), 0, 0), pipeline_mode=ONE) for f in amaps] + [
        pl.BlockSpec((D, XT), lambda j, b: (0, nt + jnp.minimum(j, nt - 1))), whole(D, NB), whole(HEADS, D),
        cols(SUB), whole(SUB, NB), whole(SUB, T)] + ([] if cin is None else [state]) + [hbm] * len(into)
    n_in = len(in_specs) + 1
    gs = pltpu.PrefetchScalarGridSpec(
        num_scalar_prefetch=1, grid=(nt + 1,), in_specs=in_specs,
        out_specs=[cols(n, part), whole(n, NB, mode=None, r=part), whole(n, T, mode=None, r=part), state],
        scratch_shapes=[pltpu.VMEM((nm, MH, D), bf16), pltpu.VMEM((2, nm, MH, XT), f32), pltpu.VMEM((MH, NB + T), f32),
                        pltpu.VMEM((n, XT), bf16), pltpu.VMEM((nx, 2, T, per * MT), bf16),
                        pltpu.VMEM((n + 8 * (nx + 1), T), f32), pltpu.VMEM((n, T), f32), pltpu.VMEM((nm, MT, T), f32),
                        pltpu.SemaphoreType.DMA((nm,))],
    )
    return pl.pallas_call(
        functools.partial(front_kernel, nx=nx, per=per, where=where, ns=ns, more=int(cin is not None), skip=len(into)), grid_spec=gs,
        out_shape=[jax.ShapeDtypeStruct((parts * n, XW), bf16), jax.ShapeDtypeStruct((parts * n, NB), bf16),
                   jax.ShapeDtypeStruct((parts * n, T), f32), jax.ShapeDtypeStruct((nx, T + SUB, XW), f32)],
        input_output_aliases={n_in - len(into) + o: o for o in range(len(into))},
        compiler_params=pltpu.CompilerParams(dimension_semantics=("arbitrary",), vmem_limit_bytes=62 * MIB),
        cost_estimate=pl.CostEstimate(flops=n * 25_000_000, bytes_accessed=n * 10000, transcendentals=n * 4096),
        name="front",
    )(pre, *srcs, *[aux] * nx, w2, wb, wdt, *consts, *([] if cin is None else [cin]), *into)


def mixz_kernel(pre, *refs, ns, first):
    xs_, auxs = refs[:ns], refs[ns:2 * ns]
    (xa_ref, bg_ref, cg_ref, dc_ref, wz_ref, cin_ref, hp_ref, yn_ref, cout_ref, xv, av, zbuf, ybuf, xw, state) = refs[2 * ns:]
    g, i, tile = pl.program_id(0), pl.program_id(1), pl.program_id(2)
    n_tiles = pl.num_programs(2)

    @pl.when(tile == 0)
    def _():
        state[...] = cin_ref[0]

    at = i * n_tiles + tile
    for k in range(ns):
        @pl.when((at >= first[k]) & (at < first[k + 1]))
        def _():
            xv[...] = xs_[k][...]
            av[...] = auxs[k][...]

    rows = lax.broadcasted_iota(jnp.int32, (T, T), 0)
    cols = lax.broadcasted_iota(jnp.int32, (T, T), 1)
    lo_half = cols < 64
    zero = jnp.zeros((T, T), bf16)
    for t in range(MT // T):
        rs = slice(t * T, (t + 1) * T)
        aux = columns(av[t])
        mask = (rows >= cols) & (lane_bcast(aux, 5) == jnp.broadcast_to(av[t, 5:6, :], (T, T)))
        k_in = lane_bcast(aux, 3)
        k_end = lane_bcast(aux, 4)
        dc = pltpu.roll(dc_ref[rs, :], lax.rem(T - 16 * g, T), 1)
        dct = dc.T
        rel = dct[:HEADS // 2, :] - jnp.log2(dct[HEADS:HEADS + HEADS // 2, :])
        bg, cg = bg_ref[rs, :], cg_ref[rs, :]
        sm = jnp.where(mask, mac(cg, bg, 1, 1), 0.0)
        ybuf[...] = mac(cg, state[...].astype(bf16))
        sq = jnp.zeros((T, T), f32)
        if t == 0:
            zbuf[...] = jnp.dot(xv[...], wz_ref[...], preferred_element_type=f32).astype(bf16).astype(f32)
        for p in range(GW // T):
            cs = slice(p * T, (p + 1) * T)
            xa = xa_ref[rs, cs]
            xaf = xa.astype(f32)
            c0, c1 = lane_bcast(dc, 2 * p), lane_bcast(dc, 2 * p + 1)
            mixes = []
            for hh, cb in ((2 * p, c0), (2 * p + 1, c1)):
                diff = jnp.minimum(cb - jnp.broadcast_to(rel[hh:hh + 1, :], (T, T)), 126.0)
                mixes.append((sm * jnp.exp2(diff)).astype(bf16))
            lhs = jnp.concatenate(mixes, axis=1)
            rhs = jnp.concatenate([jnp.where(lo_half, xa, zero), jnp.where(lo_half, zero, xa)], axis=0)
            y = mac(lhs, rhs)
            cump = jnp.where(lo_half, c0, c1)
            dtp = pair_bcast(dc, HEADS // 2 + p)
            last = cump[T - 1:T, :]
            xw[:, cs] = (xaf * (jnp.exp2(last - cump) * dtp * k_end)).astype(bf16)
            y = y + ybuf[:, cs] * (jnp.exp2(cump) * k_in) + hp_ref[0:1, cs] * xaf
            v = y * silu(zbuf[rs, cs])
            ybuf[:, cs] = v
            sq = sq + v * v
            state[:, cs] = state[:, cs] * (jnp.exp2(last) * k_in[T - 1:T, :])
        ms = jnp.sum(sq, axis=1, keepdims=True) * (1.0 / GW)
        r = jnp.broadcast_to(lax.rsqrt(ms + NORM_EPS), (T, T))
        for p in range(GW // T):
            cs = slice(p * T, (p + 1) * T)
            yn_ref[rs, cs] = (ybuf[:, cs] * r * hp_ref[1:2, cs]).astype(bf16)
        state[...] = state[...] + mac(bg, xw[...], 0, 0)

    @pl.when(tile == n_tiles - 1)
    def _():
        cout_ref[0] = state[...]


def mixz_call(pre, aux, amaps, xs, arrs, w2, cin, hp, *, nx, per, ofs, cofs):
    ns = len(xs)
    first = [0]
    for v in xs:
        first.append(min(first[-1] + v.shape[0] // MT, nx * per))
    n = nx * per * MT
    xa, bca, dc = arrs
    piece = lambda k: (lambda i, t: jnp.clip(i * per + t - first[k], 0, first[k + 1] - first[k] - 1))
    rows = lambda w, c, o=ofs: pl.BlockSpec((MT, w), lambda g, i, t, b: (o + i * per + t, c(g)))
    state = lambda ofs: pl.BlockSpec((1, T, GW), lambda g, i, t, b: (ofs + i, 0, g))
    cols = lambda k: pl.BlockSpec((k, GW), lambda g, i, t, b: (0, g))
    in_specs = [pl.BlockSpec((MT, D), lambda g, i, t, b, k=k: (piece(k)(i, t), 0)) for k in range(ns)]
    in_specs += [pl.BlockSpec((MT // T, SUB, T), lambda g, i, t, b, k=k: (amaps[k](b) + piece(k)(i, t), 0, 0)) for k in range(ns)]
    same = lambda g: g
    in_specs += [rows(GW, same), rows(T, same), rows(T, lambda g: 2 + g), rows(T, lambda g: 0), cols(D), state(cofs), cols(8)]
    gs = pltpu.PrefetchScalarGridSpec(
        num_scalar_prefetch=1, grid=(2, nx, per), in_specs=in_specs, out_specs=[rows(GW, same, 0), state(0)],
        scratch_shapes=[pltpu.VMEM((MT, D), bf16), pltpu.VMEM((MT // T, SUB, T), f32), pltpu.VMEM((MT, GW), f32), pltpu.VMEM((T, GW), f32),
                        pltpu.VMEM((T, GW), bf16), pltpu.VMEM((T, GW), f32)],
    )
    return pl.pallas_call(
        functools.partial(mixz_kernel, ns=ns, first=first), grid_spec=gs,
        out_shape=[jax.ShapeDtypeStruct((n, XW), bf16), jax.ShapeDtypeStruct((nx, T, XW), f32)],
        compiler_params=pltpu.CompilerParams(dimension_semantics=("arbitrary",) * 3, vmem_limit_bytes=60 * MIB),
        cost_estimate=pl.CostEstimate(flops=n * 20_000_000, bytes_accessed=n * 14000, transcendentals=n * 10000),
        name="mixz",
    )(pre, *xs, *[aux] * ns, xa, bca, bca, dc, w2, cin, hp)


def seq_slot(me, s):
    c = (me % 2 + s % 2) % 2
    y = (me // 2 + s // 2) % 2
    return 2 * y + c


PARTS = (2, 1, 1)
NCH = 2


def count(flag):
    return jnp.where(flag, 1, 0)


def token_flags(segs_ref, q, flags_ref):
    seg = segs_ref[q + 1]
    shape = seg.shape
    tiles, lanes = (lax.broadcasted_iota(jnp.int32, shape, d) for d in range(2))
    before = jnp.where(tiles == 0, jnp.broadcast_to(segs_ref[q][shape[0] - 1:, :], shape), pltpu.roll(seg, 1, 0))
    back = [jnp.where(lanes < d, pltpu.roll(before, d, 1), pltpu.roll(seg, d, 1)) for d in (1, 2, 3)]
    back += [jnp.broadcast_to(back[0][:, :1], shape), jnp.broadcast_to(seg[:, T - 1:], shape)]
    flags = [jnp.where(seg == v, 1.0, 0.0) for v in back] + [(seg - jnp.broadcast_to(segs_ref[1][:1, :1], shape)).astype(f32)]
    for t in range(shape[0]):
        for f, v in enumerate(flags):
            flags_ref[q * shape[0] + t, f:f + 1, :] = v[t:t + 1, :]
        flags_ref[q * shape[0] + t, len(flags):, :] = jnp.zeros((SUB - len(flags), T), f32)


def ahead_kernel(n_blocks, n_pl, seg_ref, tail_ref, x_hbm, w_hbm, flags_ref, tails_ref, *refs):
    me, blk = lax.axis_index('tp'), lax.axis_index('sp')
    *outs, segs_ref, xbuf, wbuf, in_sem, out_sem, send_sem, recv_sem = refs
    xs, ws = outs[:len(PARTS)], outs[len(PARTS):]
    step = ws[0].shape[0]
    place = lax.axis_index('dp') * n_blocks + blk
    pieces, row = [], 0
    for dst in xs:
        size = dst.shape[0]
        pieces.append((x_hbm.at[pl.ds(row, size)], xbuf.at[pl.ds(row, size)], dst))
        row += size
    for k, dst in enumerate(ws):
        pieces.append((w_hbm.at[pl.ds(pl.multiple_of((k * n_pl + place) * step, HALO), step)], wbuf.at[k], dst))
    moves = [(pltpu.make_async_copy(src, buf, in_sem.at[k]), pltpu.make_async_copy(buf, dst, out_sem.at[k]))
             for k, (src, buf, dst) in enumerate(pieces)]
    for load, _ in moves:
        load.start()
    barrier = pltpu.get_barrier_semaphore()
    others = [{'tp': seq_slot(me, s)} for s in (1, 2, 3)]
    before = {'sp': jnp.maximum(blk - 1, 0), 'tp': 3}
    after = [{'sp': jnp.minimum(blk + 1, n_blocks - 1), 'tp': q} for q in range(4)]
    sends_on = (me == 3) & (blk < n_blocks - 1)
    for dev in others:
        pl.semaphore_signal(barrier, inc=1, device_id=dev, device_id_type=MESH)

    @pl.when(blk > 0)
    def _():
        pl.semaphore_signal(barrier, inc=1, device_id=before, device_id_type=MESH)

    @pl.when(sends_on)
    def _():
        for dev in after:
            pl.semaphore_signal(barrier, inc=1, device_id=dev, device_id_type=MESH)

    pl.semaphore_wait(barrier, 3 + count(blk > 0) + 4 * count(sends_on))

    def copies(dev, entry, k, rk):
        return [pltpu.make_async_remote_copy(src_ref=seg_ref, dst_ref=segs_ref.at[entry], send_sem=send_sem.at[k, 0],
                                             recv_sem=recv_sem.at[rk, 0], device_id=dev, device_id_type=MESH),
                pltpu.make_async_remote_copy(src_ref=tail_ref, dst_ref=tails_ref.at[entry], send_sem=send_sem.at[k, 1],
                                             recv_sem=recv_sem.at[rk, 1], device_id=dev, device_id_type=MESH)]

    inner = [copies(dev, me + 1, k, k) for k, dev in enumerate(others)]
    outer = [copies(dev, 0, 3 + q, 3) for q, dev in enumerate(after)]
    for cs in inner:
        for c in cs:
            c.start()

    @pl.when(sends_on)
    def _():
        for cs in outer:
            for c in cs:
                c.start()

    for load, store in moves:
        load.wait()
        store.start()
    segs_ref[me + 1] = seg_ref[...]
    tails_ref[me + 1] = tail_ref[...]

    @pl.when(blk == 0)
    def _():
        segs_ref[0] = jnp.zeros_like(seg_ref)
        tails_ref[0] = jnp.zeros_like(tail_ref)

    for cs in inner:
        for c in cs:
            c.wait_send()
            c.wait_recv()

    @pl.when(sends_on)
    def _():
        for cs in outer:
            for c in cs:
                c.wait_send()

    @pl.when(blk > 0)
    def _():
        for c in outer[0]:
            c.wait_recv()

    for q in range(4):
        token_flags(segs_ref, q, flags_ref)
    for _, store in moves:
        store.wait()


def ahead_call(seg, x, w, n_blocks, n_pl):
    rows = x.shape[0]
    step = w.shape[0] // (NCH * n_pl)
    n_out = len(PARTS) + NCH
    vmem, hbm = pl.BlockSpec(memory_space=pltpu.VMEM), pl.BlockSpec(memory_space=pl.ANY)
    sds = jax.ShapeDtypeStruct
    return pl.pallas_call(
        functools.partial(ahead_kernel, n_blocks, n_pl),
        grid=(1,),
        in_specs=[vmem, pl.BlockSpec((HALO, D), lambda i: (rows // HALO - 1, 0)), hbm, hbm],
        out_specs=[vmem] * 2 + [hbm] * n_out,
        out_shape=[sds((4 * rows // T, SUB, T), f32), sds((5, HALO, D), bf16)] + [sds((p * MT, D), bf16) for p in PARTS] + [sds((step, D), bf16)] * NCH,
        scratch_shapes=[pltpu.VMEM((5, rows // T, T), jnp.int32), pltpu.VMEM((rows, D), bf16), pltpu.VMEM((NCH, step, D), bf16), pltpu.SemaphoreType.DMA((n_out,)),
                        pltpu.SemaphoreType.DMA((n_out,)), pltpu.SemaphoreType.DMA((7, 2)), pltpu.SemaphoreType.DMA((4, 2))],
        compiler_params=pltpu.CompilerParams(collective_id=0, has_side_effects=True, vmem_limit_bytes=24 * MIB),
        name="ahead",
    )(seg.reshape(rows // T, T), x, x, w)


CW = 256


def chain_kernel(n_blocks, e01_ref, e2_ref, e3_ref, out_hbm, ebuf, sbuf, obuf, out_ref, lsem, osem, send_sem, recv_sem):
    me, blk = lax.axis_index('tp'), lax.axis_index('sp')
    srcs = [e01_ref.at[0], e01_ref.at[1], e2_ref.at[0], e3_ref.at[0]]
    loads = [pltpu.make_async_copy(src, ebuf.at[seq_slot(me, s)], lsem.at[s]) for s, src in enumerate(srcs)]
    for c in loads:
        c.start()
    barrier = pltpu.get_barrier_semaphore()
    before = {'sp': jnp.maximum(blk - 1, 0)}
    after = {'sp': jnp.minimum(blk + 1, n_blocks - 1)}

    @pl.when(blk > 0)
    def _():
        pl.semaphore_signal(barrier, inc=1, device_id=before, device_id_type=MESH)

    @pl.when(blk < n_blocks - 1)
    def _():
        pl.semaphore_signal(barrier, inc=1, device_id=after, device_id_type=MESH)

    pl.semaphore_wait(barrier, count(blk > 0) + count(blk < n_blocks - 1))

    for c in loads:
        c.wait()

    def through(q, s, cs):
        return ebuf[q, :T, cs] + ebuf[q, T:T + 1, cs] * s

    for q in (1, 2, 3):
        ebuf[q, :T, :] = through(q, ebuf[q - 1, :T, :], slice(None))
        ebuf[q, T:, :] = ebuf[q, T:, :] * ebuf[q - 1, T:, :]

    @pl.when(blk == 0)
    def _():
        sbuf[...] = jnp.zeros_like(sbuf)

    n = XW // CW

    def store(j):
        cs = pl.ds(j * CW, CW)
        return pltpu.make_async_copy(out_ref.at[:, :, cs], out_hbm.at[:, :, cs], osem.at[j])

    def send(j):
        return pltpu.make_async_remote_copy(src_ref=obuf.at[j], dst_ref=sbuf.at[j], send_sem=send_sem.at[j],
                                            recv_sem=recv_sem.at[j], device_id=after, device_id_type=MESH)

    for j in range(n):
        cs = slice(j * CW, (j + 1) * CW)

        @pl.when(blk > 0)
        def _():
            send(j).wait_recv()

        @pl.when(blk < n_blocks - 1)
        def _():
            obuf[j] = through(3, sbuf[j], cs)
            send(j).start()

    for j in range(n):
        cs = slice(j * CW, (j + 1) * CW)
        for q in range(4):
            v = through(q - 1, sbuf[j], cs) if q else sbuf[j]
            out_ref[seq_slot(me, q), :, cs] = v
        store(j).start()

    @pl.when(blk < n_blocks - 1)
    def _():
        for j in range(n):
            send(j).wait_send()

    for j in range(n):
        store(j).wait()


def chain_call(e01, e2, e3, n_blocks):
    hbm = pl.BlockSpec(memory_space=pltpu.HBM)
    n = XW // CW
    return pl.pallas_call(
        functools.partial(chain_kernel, n_blocks),
        in_specs=[hbm] * 3,
        out_specs=hbm,
        out_shape=jax.ShapeDtypeStruct((4, T, XW), f32),
        scratch_shapes=[pltpu.VMEM((4, T + SUB, XW), f32), pltpu.VMEM((n, T, CW), f32), pltpu.VMEM((n, T, CW), f32),
                        pltpu.VMEM((4, T, XW), f32),                         pltpu.SemaphoreType.DMA((4,)), pltpu.SemaphoreType.DMA((n,)),
                        pltpu.SemaphoreType.DMA((n,)), pltpu.SemaphoreType.DMA((n,))],
        compiler_params=pltpu.CompilerParams(collective_id=1, has_side_effects=True, vmem_limit_bytes=63 * MIB),
        name="chain",
    )(e01, e2, e3)


NT = 512


def out_kernel(y_ref, yr_ref, w_ref, wr0_ref, wr1_ref, *refs):
    h = XW // 2
    acc = (jnp.dot(y_ref[...], w_ref[...], preferred_element_type=f32)
           + jnp.dot(yr_ref[:, 0:h], wr0_ref[...], preferred_element_type=f32)
           + jnp.dot(yr_ref[:, h:], wr1_ref[...], preferred_element_type=f32))
    if len(refs) > 1:
        x_ref, other_ref = refs[:2]
        acc = x_ref[...].astype(f32) + (acc + other_ref[...])
    refs[-1][...] = acc.astype(refs[-1].dtype)


def out_call(run, part, y, yr, rpart, w, wr, x=None, other=None, into=None):
    rows = TOK // NCH
    h = XW // 2
    at = lambda r: (lambda j: (r, j))
    cols = at(0)
    ins = [y, yr, w, *wr]
    specs = [pl.BlockSpec((rows, XW), lambda j: (run * (TOK // rows) + part, 0), pipeline_mode=ONE),
             pl.BlockSpec((rows, XW), lambda j: (rpart, 0), pipeline_mode=ONE),
             pl.BlockSpec((XW, NT), cols), pl.BlockSpec((h, NT), cols), pl.BlockSpec((h, NT), cols)]
    alias = {}
    if x is not None:
        ins += [x, other]
        specs += [pl.BlockSpec((rows, NT), at(part)), pl.BlockSpec((rows, NT), cols)]
    if into is not None:
        alias = {len(ins): 0}
        ins.append(into)
        specs.append(pl.BlockSpec(memory_space=pl.ANY))
    return pl.pallas_call(
        out_kernel,
        grid=(D // NT,), in_specs=specs,
        out_specs=pl.BlockSpec((rows, NT), cols if x is None else at(part)),
        out_shape=jax.ShapeDtypeStruct((rows, D), f32) if x is None else jax.ShapeDtypeStruct(x.shape, bf16),
        input_output_aliases=alias,
        compiler_params=pltpu.CompilerParams(dimension_semantics=("arbitrary",), vmem_limit_bytes=56 * MIB),
        cost_estimate=pl.CostEstimate(flops=rows * 33_000_000, bytes_accessed=rows * 100000, transcendentals=0),
        name="out_proj",
    )(*ins)


def send(v, perm):
    return lax.ppermute(v, 'tp', perm)


def after(v, *deps):
    return lax.optimization_barrier((v,) + deps)[0]


CORE_SWAP = [(i, i ^ 1) for i in range(4)]
CHIP_SWAP = [(i, i ^ 2) for i in range(4)]


def solution(mesh):
    n_blocks = mesh.shape['sp']
    token_spec = seg_spec = P(('dp', 'sp', 'tp'))
    weight_specs = tuple(P(*['tp' if i == dim else None for i in range(dim + 1)]) for dim in (2, 2, 1, 1, 2, 0, 1, 0, 0, 0, 0, 0))

    def body(x_loc, seg_loc, w_zx, w_bc, w_dt, conv_x, conv_bc, bias_x, bias_bc, a_log, dt_bias, d_skip, norm_w, w_out):
        rows, d = x_loc.shape
        me = lax.axis_index('tp')
        per, kper = rows // MT, rows // (NCH * MT)
        n_pl = mesh.shape['dp'] * n_blocks
        aux, tails, *parts = ahead_call(seg_loc, x_loc, w_out, n_blocks, n_pl)
        x_par = send(after(x_loc, aux), CORE_SWAP)
        x_dir = [send(v, CHIP_SWAP) for v in parts[:len(PARTS)]]
        w_half = [send(v, CHIP_SWAP) for v in parts[len(PARTS):]]

        def w_gather(h, dep):
            return lax.all_gather(after(w_half[h], dep), ('dp', 'sp'), axis=0, tiled=True)

        tails = tails.reshape(-1, d)
        w2, wb = w_zx.reshape(d, 2 * XW), w_bc.reshape(d, NB)
        pad = lambda v: jnp.pad(v.astype(f32), ((0, SUB - v.shape[0]), (0, 0)))
        cw = pad(jnp.concatenate([conv_x, bias_x[None]], axis=0))
        cwb = pad(jnp.concatenate([conv_bc.reshape(4, NB), bias_bc.reshape(1, NB)], axis=0))
        hp1 = jnp.pad(jnp.stack([dt_bias, a_log]), ((0, 6), (0, T - HEADS)))
        hp2 = pad(jnp.stack([jnp.repeat(d_skip, HEAD), norm_w.astype(f32)]))
        pre = jnp.stack([seq_slot(me, s) for s in range(4)]).astype(jnp.int32)
        weights = (w2, wb, w_dt.T)
        consts = (cw, cwb, hp1)

        def front(slots, part, parts, runs, carry, into, per):
            return front_call(pre, aux, [lambda b, s=s: b[s] * parts + part for s in slots], runs, weights, carry, consts,
                              into, part, parts, per=per)

        tail_row = lambda s: (lambda b: b[s] * HALO)
        *own, ends = front((0, 1), 0, 1, [(tails, tail_row(0), [x_loc]), (tails, tail_row(1), [x_par])], None, [], per)
        w_rem = [w_gather(0, ends)]
        x_dir[0] = after(x_dir[0], ends)
        x_fwd = [send(x_dir[0], CORE_SWAP)]
        *rem2, c2 = front((2,), 0, NCH, [(tails, tail_row(2), x_dir[:1])], None, [], kper)
        *rem3, c3 = front((3,), 0, NCH, [(tails, tail_row(3), [after(x_fwd[0], c2)])], None, [], kper)
        x_dir[1] = after(x_dir[1], c3)
        x_fwd.append(send(x_dir[1], CORE_SWAP))
        end = lambda k: PARTS[k] * MT - HALO
        *rem2, c2 = front((2,), 2, 4, [(x_dir[0], end(0), [x_dir[1]])], c2, rem2, 1)
        x_dir[2] = after(x_dir[2], c2)
        x_fwd.append(send(x_dir[2], CORE_SWAP))
        *rem2, c2 = front((2,), 3, 4, [(x_dir[1], end(1), [x_dir[2]])], c2, rem2, 1)
        *rem3, c3 = front((3,), 1, NCH, [(x_fwd[0], end(0), [after(x_fwd[1], c2), x_fwd[2]])], c3, rem3, kper)
        starts = chain_call(ends, c2, c3, n_blocks)
        w_rem.append(w_gather(1, starts))

        def mix(amaps, xs, arrs, start, **kw):
            return mixz_call(pre, aux, amaps, xs, arrs, w2, start, hp2, **kw)

        at = lambda s, k=0: (lambda b: b[s] * per + k)
        yn, c = mix([at(3)], x_fwd[:1], rem3, starts, nx=1, per=kper, ofs=0, cofs=3)
        y_in = [send(yn, CHIP_SWAP)]
        yn, c = mix([at(3, 2), at(3, 3)], x_fwd[1:], rem3, c, nx=1, per=kper, ofs=kper, cofs=0)
        y_in.append(send(yn, CHIP_SWAP))
        yn, c = mix([at(2), at(2, 2), at(2, 3)], x_dir, rem2, after(starts, c), nx=1, per=per, ofs=0, cofs=2)
        y_in.append(send(yn, CHIP_SWAP))
        y_own, _ = mix([at(0), at(1)], [x_loc, x_par], own, after(starts, c), nx=2, per=per, ofs=0, cofs=0)
        other = []
        for k in range(NCH):
            part = out_call(1, k, y_own, y_in[k], 0, w_out, w_rem)
            other.append(send(part, CORE_SWAP))
        y = None
        for k in range(NCH):
            y = out_call(0, k, y_own, y_in[2], k, w_out, w_rem, x_loc, other[k], y)
        return y

    return jax.shard_map(body, mesh=mesh, in_specs=(token_spec, seg_spec) + weight_specs, out_specs=token_spec, check_vma=False)
```

```python
import functools
import jax
import jax.numpy as jnp
from jax import lax
from jax.sharding import PartitionSpec as P
from jax.experimental import pallas as pl
from jax.experimental.pallas import tpu as pltpu

T = 128
XW = 2048
NB = 512
GW = 1024
D = 4096
TOK = 1024
HEADS, HEAD = 32, 64
XT = 512
MT = 256
HALO = 16
SUB = 8
MH = MT + HALO
LOG2E = 1.4426950408889634
NORM_EPS = 1e-5
MIB = 2**20
f32, bf16 = jnp.float32, jnp.bfloat16
MESH = pl.DeviceIdType.MESH
ONE = pl.Buffered(1)


def silu(v):
    h = 0.5 * v
    return h + h * jnp.tanh(h)


def lane_bcast(cols, h):
    return jnp.broadcast_to(cols[:, h:h + 1], (cols.shape[0], T))


def pair_bcast(cols, p):
    lanes = lax.broadcasted_iota(jnp.int32, (cols.shape[0], T), 1)
    return jnp.where(lanes < HEAD, lane_bcast(cols, 2 * p), lane_bcast(cols, 2 * p + 1))


def columns(flags):
    return jnp.concatenate([flags, jnp.zeros((T - SUB, T), f32)], axis=0).T


def row(ref, r):
    return ref[r:r + 1, :]


def mac(a, b, ca=1, cb=0, **kw):
    return lax.dot_general(a, b, (((ca,), (cb,)), ((), ())), preferred_element_type=f32, **kw)


def rows_from(start, size):
    return pl.ds(start if isinstance(start, int) else pl.multiple_of(start, 16), size)


def front_kernel(pre, *refs, nx, per, where, ns, more, skip):
    srcs, auxs = refs[:ns], refs[ns:ns + nx]
    wx_ref, wb_ref, wdt_ref, cw_ref, cwb_ref, hp_ref, *cins = refs[ns + nx:][:6 + more]
    (xa_ref, bca_ref, dc_ref, cout_ref, xbuf, pbuf, bbuf, xw, bt, cum_all, wgt, abuf, sem) = refs[ns + nx + 6 + more + skip:]
    n = pl.program_id(0)
    last_n = XW // XT
    nm = nx * per
    rows = lax.broadcasted_iota(jnp.int32, (T, T), 0)
    cols = lax.broadcasted_iota(jnp.int32, (T, T), 1)
    lo_half = cols < HEAD
    tiles = [slice(t * T, (t + 1) * T) for t in range(MT // T)]

    def copies(m):
        src, row, halo, h = where[m]
        h = h(pre) if callable(h) else h
        if halo == src:
            return [pltpu.make_async_copy(srcs[src].at[rows_from(row - HALO, MH)], xbuf.at[m], sem.at[m])]
        return [pltpu.make_async_copy(srcs[halo].at[rows_from(h, HALO)], xbuf.at[m, pl.ds(0, HALO)], sem.at[m]),
                pltpu.make_async_copy(srcs[src].at[pl.ds(row, MT)], xbuf.at[m, pl.ds(HALO, MT)], sem.at[m])]

    def left(i):
        return slice(nm * MT + SUB * (i + 1), nm * MT + SUB * (i + 2))

    def heads_first(v):
        return pltpu.roll(v, lax.rem(T - (XT // HEAD) * (n - 1), T), 1)

    def at(m, ts):
        return pl.ds(pl.multiple_of(m * MT + ts.start, T), T)

    def conv(read, lo, w, keep):
        cs = slice(lo, lo + T)
        acc = read(0, cs) * row(w, 3)[:, cs] + row(w, 4)[:, cs]
        for k in range(3):
            acc = acc + (read(3 - k, cs) * w[k:k + 1, cs]) * keep[k]
        return silu(acc).astype(bf16)

    def taps(m, ts):
        return [lane_bcast(abuf[m, ts, :], 2 - k) for k in range(3)]

    def x_dot(m):
        pbuf[lax.rem(n, 2), m] = jnp.dot(xbuf[m], wx_ref[...], preferred_element_type=f32).astype(bf16).astype(f32)

    def setup(m, i, s):
        for ts in tiles:
            r0 = HALO + ts.start
            keep = taps(m, ts)
            for c in range(NB // T):
                act = conv(lambda d, cs: bbuf[r0 - d:r0 - d + T, cs], c * T, cwb_ref, keep)
                bca_ref[at(m, ts), c * T:(c + 1) * T] = act
                if c < 2:
                    bt[i, c, :, at(s, ts)] = act.T
            raw = bbuf[r0:r0 + T, NB:NB + T] + row(hp_ref, 0)
            dtv = jnp.maximum(raw, 0.0) + jnp.log1p(jnp.exp(-jnp.abs(raw)))
            log_a = -jnp.exp(row(hp_ref, 1)) * dtv * LOG2E
            cum = mac((rows >= cols).astype(f32), log_a, precision=lax.Precision.HIGHEST)
            dc_ref[at(m, ts), :] = jnp.where(cols < HEADS, cum, pltpu.roll(dtv, HEADS, 1))
            before = jnp.where((s == 0) & (ts.start == 0), 0.0, row(cum_all, nm * MT))
            cum = cum + before
            cum_all[at(m, ts), :] = cum
            cum_all[nm * MT:nm * MT + SUB, :] = jnp.broadcast_to(cum[T - 1:T, :], (8, T))
            wgt[at(m, ts), :] = dtv

    def weigh(i):
        lo, end = i * per * MT, (i + 1) * per * MT
        doc = abuf[end // MT - 1, MT - 1:MT, 5:6]
        last = row(cum_all, end - 1)
        keep_in = abuf[lo // MT, 0:1, 0:1] * (abuf[lo // MT, 0:1, 5:6] == doc).astype(f32)
        carry = jnp.broadcast_to(jnp.exp2(last) * keep_in, (8, T))
        for r in range(lo, end, T):
            keep = jnp.broadcast_to((abuf[r // MT, r % MT:r % MT + T, 5:6] == doc).astype(f32), (T, T))
            wgt[r:r + T, :] = jnp.exp2(last - cum_all[r:r + T, :]) * wgt[r:r + T, :] * keep
        cum_all[left(i), :] = carry

    def x_conv(m):
        slot = lax.rem(n + 1, 2)
        for ts in tiles:
            r0 = HALO + ts.start
            keep = taps(m, ts)
            wg = heads_first(wgt[at(m, ts), :])
            for p in range(XT // T):
                cs = slice(p * T, (p + 1) * T)
                xa = conv(lambda d, cs: pbuf[slot, m, r0 - d:r0 - d + T, cs], p * T, cw_ref, keep)
                xa_ref[at(m, ts), cs] = xa
                xw[at(m, ts), cs] = (xa.astype(f32) * pair_bcast(wg, p)).astype(bf16)

    def end_state():
        g = (n - 1) // (GW // XT)
        for i in range(nx):
            upd = jnp.dot(bt[i, g], xw[i * per * MT:(i + 1) * per * MT, :], preferred_element_type=f32)
            cr = heads_first(cum_all[left(i), :])
            for p in range(XT // T):
                cs = slice(p * T, (p + 1) * T)
                carry = pair_bcast(cr, p)
                if cins:
                    cout_ref[i, :T, cs] = cins[0][i, :T, cs] * jnp.broadcast_to(carry[:1], (T, T)) + upd[:, cs]
                    cout_ref[i, T:, cs] = cins[0][i, T:, cs] * carry
                else:
                    cout_ref[i, :T, cs] = upd[:, cs]
                    cout_ref[i, T:, cs] = carry

    @pl.when(n == 0)
    def _():
        for m in range(nm):
            for c in copies(m):
                c.start()
        bbuf[:, NB:] = jnp.zeros((MH, T), f32)
        for m in range(nm):
            i, s = divmod(m, per)
            for ts in tiles:
                abuf[m, ts, :] = columns(auxs[i][(s * MT + ts.start) // T])

        @pl.loop(0, nm)
        def _(m):
            for k in range(nm):
                @pl.when(m == k)
                def _():
                    for c in copies(k):
                        c.wait()
            bbuf[:, :NB] = jnp.dot(xbuf[m], wb_ref[...], preferred_element_type=f32).astype(bf16).astype(f32)
            bbuf[:, NB:NB + HEADS] = mac(xbuf[m], wdt_ref[...], 1, 1).astype(bf16).astype(f32)
            x_dot(m)
            setup(m, m // per, lax.rem(m, per))

        for i in range(nx):
            weigh(i)

    @pl.when((n > 0) & (n < last_n))
    def _():
        @pl.loop(0, nm)
        def _(m):
            x_dot(m)
            x_conv(m)

    @pl.when(n == last_n)
    def _():
        @pl.loop(0, nm)
        def _(m):
            x_conv(m)

    @pl.when(n > 0)
    def _():
        end_state()


def front_call(pre, aux, amaps, runs, weights, cin, consts, into, part, parts, *, per):
    nx = len(runs)
    srcs, where = [], []
    for ahead, row, arrays in runs:
        srcs.append(ahead)
        halo = len(srcs) - 1
        for arr in arrays:
            srcs.append(arr)
            for r in range(0, min(arr.shape[0], per * MT), MT):
                where.append((len(srcs) - 1, r, halo, row))
                halo, row = len(srcs) - 1, r + MT - HALO
    ns = len(srcs)
    nm = nx * per
    n = nm * MT
    nt = XW // XT
    w2, wb, wdt = weights
    hbm = pl.BlockSpec(memory_space=pl.ANY)
    prev = lambda j: jnp.maximum(j - 1, 0)
    whole = lambda *shape, mode=ONE, r=0: pl.BlockSpec(shape, lambda j, b: (r, 0), pipeline_mode=mode)
    cols = lambda k, r=0: pl.BlockSpec((k, XT), lambda j, b: (r, prev(j)))
    state = pl.BlockSpec((nx, T + 8, XT), lambda j, b: (0, 0, prev(j)))
    in_specs = [hbm] * ns + [pl.BlockSpec((per * MT // T, SUB, T), lambda j, b, f=f: (f(b), 0, 0), pipeline_mode=ONE) for f in amaps] + [
        pl.BlockSpec((D, XT), lambda j, b: (0, nt + jnp.minimum(j, nt - 1))), whole(D, NB), whole(HEADS, D),
        cols(SUB), whole(SUB, NB), whole(SUB, T)] + ([] if cin is None else [state]) + [hbm] * len(into)
    n_in = len(in_specs) + 1
    gs = pltpu.PrefetchScalarGridSpec(
        num_scalar_prefetch=1, grid=(nt + 1,), in_specs=in_specs,
        out_specs=[cols(n, part), whole(n, NB, mode=None, r=part), whole(n, T, mode=None, r=part), state],
        scratch_shapes=[pltpu.VMEM((nm, MH, D), bf16), pltpu.VMEM((2, nm, MH, XT), f32), pltpu.VMEM((MH, NB + T), f32),
                        pltpu.VMEM((n, XT), bf16), pltpu.VMEM((nx, 2, T, per * MT), bf16),
                        pltpu.VMEM((n + 8 * (nx + 1), T), f32), pltpu.VMEM((n, T), f32), pltpu.VMEM((nm, MT, T), f32),
                        pltpu.SemaphoreType.DMA((nm,))],
    )
    return pl.pallas_call(
        functools.partial(front_kernel, nx=nx, per=per, where=where, ns=ns, more=int(cin is not None), skip=len(into)), grid_spec=gs,
        out_shape=[jax.ShapeDtypeStruct((parts * n, XW), bf16), jax.ShapeDtypeStruct((parts * n, NB), bf16),
                   jax.ShapeDtypeStruct((parts * n, T), f32), jax.ShapeDtypeStruct((nx, T + SUB, XW), f32)],
        input_output_aliases={n_in - len(into) + o: o for o in range(len(into))},
        compiler_params=pltpu.CompilerParams(dimension_semantics=("arbitrary",), vmem_limit_bytes=62 * MIB),
        cost_estimate=pl.CostEstimate(flops=n * 25_000_000, bytes_accessed=n * 10000, transcendentals=n * 4096),
        name="front",
    )(pre, *srcs, *[aux] * nx, w2, wb, wdt, *consts, *([] if cin is None else [cin]), *into)


def mixz_kernel(pre, *refs, ns, first, n_out):
    xs_, auxs = refs[:ns], refs[ns:2 * ns]
    (xa_ref, bg_ref, cg_ref, dc_ref, wz_ref, cin_ref, hp_ref, *yn_refs, cout_ref, xv, av, zbuf, ybuf, xw, state, ynbuf) = refs[2 * ns:]
    g, i, tile = pl.program_id(0), pl.program_id(1), pl.program_id(2)
    n_tiles = pl.num_programs(2)

    @pl.when(tile == 0)
    def _():
        state[...] = cin_ref[0]

    at = i * n_tiles + tile
    yn = yn_refs[0] if n_out == 1 else ynbuf
    for k in range(ns):
        @pl.when((at >= first[k]) & (at < first[k + 1]))
        def _():
            xv[...] = xs_[k][...]
            av[...] = auxs[k][...]

    rows = lax.broadcasted_iota(jnp.int32, (T, T), 0)
    cols = lax.broadcasted_iota(jnp.int32, (T, T), 1)
    lo_half = cols < 64
    zero = jnp.zeros((T, T), bf16)
    for t in range(MT // T):
        rs = slice(t * T, (t + 1) * T)
        aux = columns(av[t])
        mask = (rows >= cols) & (lane_bcast(aux, 5) == jnp.broadcast_to(av[t, 5:6, :], (T, T)))
        k_in = lane_bcast(aux, 3)
        k_end = lane_bcast(aux, 4)
        dc = pltpu.roll(dc_ref[rs, :], lax.rem(T - 16 * g, T), 1)
        dct = dc.T
        rel = dct[:HEADS // 2, :] - jnp.log2(dct[HEADS:HEADS + HEADS // 2, :])
        bg, cg = bg_ref[rs, :], cg_ref[rs, :]
        sm = jnp.where(mask, mac(cg, bg, 1, 1), 0.0)
        ybuf[...] = mac(cg, state[...].astype(bf16))
        sq = jnp.zeros((T, T), f32)
        if t == 0:
            zbuf[...] = jnp.dot(xv[...], wz_ref[...], preferred_element_type=f32).astype(bf16).astype(f32)
        for p in range(GW // T):
            cs = slice(p * T, (p + 1) * T)
            xa = xa_ref[rs, cs]
            xaf = xa.astype(f32)
            c0, c1 = lane_bcast(dc, 2 * p), lane_bcast(dc, 2 * p + 1)
            mixes = []
            for hh, cb in ((2 * p, c0), (2 * p + 1, c1)):
                diff = jnp.minimum(cb - jnp.broadcast_to(rel[hh:hh + 1, :], (T, T)), 126.0)
                mixes.append((sm * jnp.exp2(diff)).astype(bf16))
            lhs = jnp.concatenate(mixes, axis=1)
            rhs = jnp.concatenate([jnp.where(lo_half, xa, zero), jnp.where(lo_half, zero, xa)], axis=0)
            y = mac(lhs, rhs)
            cump = jnp.where(lo_half, c0, c1)
            dtp = pair_bcast(dc, HEADS // 2 + p)
            last = cump[T - 1:T, :]
            xw[:, cs] = (xaf * (jnp.exp2(last - cump) * dtp * k_end)).astype(bf16)
            y = y + ybuf[:, cs] * (jnp.exp2(cump) * k_in) + hp_ref[:1, cs] * xaf
            v = y * silu(zbuf[rs, cs])
            ybuf[:, cs] = v
            sq = sq + v * v
            state[:, cs] = state[:, cs] * (jnp.exp2(last) * k_in[T - 1:T, :])
        ms = jnp.sum(sq, axis=1, keepdims=True) * (1.0 / GW)
        r = jnp.broadcast_to(lax.rsqrt(ms + NORM_EPS), (T, T))
        for p in range(GW // T):
            cs = slice(p * T, (p + 1) * T)
            yn[rs, cs] = (ybuf[:, cs] * r * hp_ref[1:2, cs]).astype(bf16)
        state[...] = state[...] + mac(bg, xw[...], 0, 0)

    if n_out > 1:
        for k in range(n_out):
            @pl.when(tile // (n_tiles // n_out) == k)
            def _():
                yn_refs[k][...] = ynbuf[...]

    @pl.when(tile == n_tiles - 1)
    def _():
        cout_ref[0] = state[...]


def mixz_call(pre, aux, amaps, xs, arrs, w2, cin, hp, *, nx, per, ofs, cofs, n_out=1):
    ns = len(xs)
    first = [0]
    for v in xs:
        first.append(min(first[-1] + v.shape[0] // MT, nx * per))
    n = nx * per * MT
    xa, bca, dc = arrs
    piece = lambda k: (lambda i, t: jnp.clip(i * per + t - first[k], 0, first[k + 1] - first[k] - 1))
    rows = lambda w, c, o=ofs: pl.BlockSpec((MT, w), lambda g, i, t, b: (o + i * per + t, c(g)))
    state = lambda ofs: pl.BlockSpec((1, T, GW), lambda g, i, t, b: (ofs + i, 0, g))
    cols = lambda k: pl.BlockSpec((k, GW), lambda g, i, t, b: (0, g))
    in_specs = [pl.BlockSpec((MT, D), lambda g, i, t, b, k=k: (piece(k)(i, t), 0)) for k in range(ns)]
    in_specs += [pl.BlockSpec((MT // T, SUB, T), lambda g, i, t, b, k=k: (amaps[k](b) + piece(k)(i, t), 0, 0)) for k in range(ns)]
    same = lambda g: g
    in_specs += [rows(GW, same), rows(T, same), rows(T, lambda g: 2 + g), rows(T, lambda g: 0), cols(D), state(cofs), cols(8)]
    po = per // n_out
    outs = [rows(GW, same, 0)] if n_out == 1 else [
        pl.BlockSpec((MT, GW), lambda g, i, t, b, k=k: (jnp.clip(t - k * po, 0, po - 1), g)) for k in range(n_out)]
    gs = pltpu.PrefetchScalarGridSpec(
        num_scalar_prefetch=1, grid=(2, nx, per), in_specs=in_specs, out_specs=outs + [state(0)],
        scratch_shapes=[pltpu.VMEM((MT, D), bf16), pltpu.VMEM((MT // T, SUB, T), f32), pltpu.VMEM((MT, GW), f32), pltpu.VMEM((T, GW), f32),
                        pltpu.VMEM((T, GW), bf16), pltpu.VMEM((T, GW), f32), pltpu.VMEM((MT if n_out > 1 else HALO, GW), bf16)],
    )
    return pl.pallas_call(
        functools.partial(mixz_kernel, ns=ns, first=first, n_out=n_out), grid_spec=gs,
        out_shape=[jax.ShapeDtypeStruct((n // n_out, XW), bf16)] * n_out + [jax.ShapeDtypeStruct((nx, T, XW), f32)],
        compiler_params=pltpu.CompilerParams(dimension_semantics=("arbitrary",) * 3, vmem_limit_bytes=60 * MIB),
        cost_estimate=pl.CostEstimate(flops=n * 20_000_000, bytes_accessed=n * 14000, transcendentals=n * 10000),
        name="mixz",
    )(pre, *xs, *[aux] * ns, xa, bca, bca, dc, w2, cin, hp)


def seq_slot(me, s):
    c = (me % 2 + s % 2) % 2
    y = (me // 2 + s // 2) % 2
    return 2 * y + c


PARTS = (2, 1, 1)
NCH = 2


def count(flag):
    return jnp.where(flag, 1, 0)


def token_flags(segs_ref, q, flags_ref):
    seg = segs_ref[q + 1]
    shape = seg.shape
    tiles, lanes = (lax.broadcasted_iota(jnp.int32, shape, d) for d in range(2))
    before = jnp.where(tiles == 0, jnp.broadcast_to(segs_ref[q][shape[0] - 1:, :], shape), pltpu.roll(seg, 1, 0))
    back = [jnp.where(lanes < d, pltpu.roll(before, d, 1), pltpu.roll(seg, d, 1)) for d in (1, 2, 3)]
    back += [jnp.broadcast_to(back[0][:, :1], shape), jnp.broadcast_to(seg[:, T - 1:], shape)]
    flags = [jnp.where(seg == v, 1.0, 0.0) for v in back] + [(seg - jnp.broadcast_to(segs_ref[1][:1, :1], shape)).astype(f32)]
    for t in range(shape[0]):
        for f, v in enumerate(flags):
            flags_ref[q * shape[0] + t, f:f + 1, :] = v[t:t + 1, :]
        flags_ref[q * shape[0] + t, len(flags):, :] = jnp.zeros((SUB - len(flags), T), f32)


def ahead_kernel(n_blocks, n_pl, seg_ref, tail_ref, x_hbm, w_hbm, flags_ref, tails_ref, *refs):
    me, blk = lax.axis_index('tp'), lax.axis_index('sp')
    *outs, segs_ref, xbuf, wbuf, in_sem, out_sem, send_sem, recv_sem = refs
    xs, ws = outs[:len(PARTS)], outs[len(PARTS):]
    step = ws[0].shape[0]
    place = lax.axis_index('dp') * n_blocks + blk
    pieces, row = [], 0
    for dst in xs:
        size = dst.shape[0]
        pieces.append((x_hbm.at[pl.ds(row, size)], xbuf.at[pl.ds(row, size)], dst))
        row += size
    for k, dst in enumerate(ws):
        pieces.append((w_hbm.at[pl.ds(pl.multiple_of((k * n_pl + place) * step, HALO), step)], wbuf.at[k], dst))
    moves = [(pltpu.make_async_copy(src, buf, in_sem.at[k]), pltpu.make_async_copy(buf, dst, out_sem.at[k]))
             for k, (src, buf, dst) in enumerate(pieces)]
    for load, _ in moves:
        load.start()
    barrier = pltpu.get_barrier_semaphore()
    others = [{'tp': seq_slot(me, s)} for s in (1, 2, 3)]
    before = {'sp': jnp.maximum(blk - 1, 0), 'tp': 3}
    after = [{'sp': jnp.minimum(blk + 1, n_blocks - 1), 'tp': q} for q in range(4)]
    sends_on = (me == 3) & (blk < n_blocks - 1)
    for dev in others:
        pl.semaphore_signal(barrier, inc=1, device_id=dev, device_id_type=MESH)

    @pl.when(blk > 0)
    def _():
        pl.semaphore_signal(barrier, inc=1, device_id=before, device_id_type=MESH)

    @pl.when(sends_on)
    def _():
        for dev in after:
            pl.semaphore_signal(barrier, inc=1, device_id=dev, device_id_type=MESH)

    pl.semaphore_wait(barrier, 3 + count(blk > 0) + 4 * count(sends_on))

    def copies(dev, entry, k, rk):
        return [pltpu.make_async_remote_copy(src_ref=seg_ref, dst_ref=segs_ref.at[entry], send_sem=send_sem.at[k, 0],
                                             recv_sem=recv_sem.at[rk, 0], device_id=dev, device_id_type=MESH),
                pltpu.make_async_remote_copy(src_ref=tail_ref, dst_ref=tails_ref.at[entry], send_sem=send_sem.at[k, 1],
                                             recv_sem=recv_sem.at[rk, 1], device_id=dev, device_id_type=MESH)]

    inner = [copies(dev, me + 1, k, k) for k, dev in enumerate(others)]
    outer = [copies(dev, 0, 3 + q, 3) for q, dev in enumerate(after)]
    for cs in inner:
        for c in cs:
            c.start()

    @pl.when(sends_on)
    def _():
        for cs in outer:
            for c in cs:
                c.start()

    for load, store in moves:
        load.wait()
        store.start()
    segs_ref[me + 1] = seg_ref[...]
    tails_ref[me + 1] = tail_ref[...]

    @pl.when(blk == 0)
    def _():
        segs_ref[0] = jnp.zeros_like(seg_ref)
        tails_ref[0] = jnp.zeros_like(tail_ref)

    for cs in inner:
        for c in cs:
            c.wait_send()
            c.wait_recv()

    @pl.when(sends_on)
    def _():
        for cs in outer:
            for c in cs:
                c.wait_send()

    @pl.when(blk > 0)
    def _():
        for c in outer[0]:
            c.wait_recv()

    for q in range(4):
        token_flags(segs_ref, q, flags_ref)
    for _, store in moves:
        store.wait()


def ahead_call(seg, x, w, n_blocks, n_pl):
    rows = x.shape[0]
    step = w.shape[0] // (NCH * n_pl)
    n_out = len(PARTS) + NCH
    vmem, hbm = pl.BlockSpec(memory_space=pltpu.VMEM), pl.BlockSpec(memory_space=pl.ANY)
    sds = jax.ShapeDtypeStruct
    return pl.pallas_call(
        functools.partial(ahead_kernel, n_blocks, n_pl),
        grid=(1,),
        in_specs=[vmem, pl.BlockSpec((HALO, D), lambda i: (rows // HALO - 1, 0)), hbm, hbm],
        out_specs=[vmem] * 2 + [hbm] * n_out,
        out_shape=[sds((4 * rows // T, SUB, T), f32), sds((5, HALO, D), bf16)] + [sds((p * MT, D), bf16) for p in PARTS] + [sds((step, D), bf16)] * NCH,
        scratch_shapes=[pltpu.VMEM((5, rows // T, T), jnp.int32), pltpu.VMEM((rows, D), bf16), pltpu.VMEM((NCH, step, D), bf16), pltpu.SemaphoreType.DMA((n_out,)),
                        pltpu.SemaphoreType.DMA((n_out,)), pltpu.SemaphoreType.DMA((7, 2)), pltpu.SemaphoreType.DMA((4, 2))],
        compiler_params=pltpu.CompilerParams(collective_id=0, has_side_effects=True, vmem_limit_bytes=24 * MIB),
        name="ahead",
    )(seg.reshape(rows // T, T), x, x, w)


CW = 128


def chain_kernel(n_blocks, e01_ref, e2_ref, e3_ref, out_hbm, ebuf, sbuf, obuf, out_ref, lsem, osem, send_sem, recv_sem):
    me, blk = lax.axis_index('tp'), lax.axis_index('sp')
    srcs = [e01_ref.at[0], e01_ref.at[1], e2_ref.at[0], e3_ref.at[0]]
    loads = [pltpu.make_async_copy(src, ebuf.at[seq_slot(me, s)], lsem.at[s]) for s, src in enumerate(srcs)]
    for c in loads:
        c.start()
    barrier = pltpu.get_barrier_semaphore()
    before = {'sp': jnp.maximum(blk - 1, 0)}
    after = {'sp': jnp.minimum(blk + 1, n_blocks - 1)}

    @pl.when(blk > 0)
    def _():
        pl.semaphore_signal(barrier, inc=1, device_id=before, device_id_type=MESH)

    @pl.when(blk < n_blocks - 1)
    def _():
        pl.semaphore_signal(barrier, inc=1, device_id=after, device_id_type=MESH)

    pl.semaphore_wait(barrier, count(blk > 0) + count(blk < n_blocks - 1))

    for c in loads:
        c.wait()

    def through(q, s, cs):
        return ebuf[q, :T, cs] + ebuf[q, T:T + 1, cs] * s

    for q in (1, 2, 3):
        ebuf[q, :T, :] = through(q, ebuf[q - 1, :T, :], slice(None))
        ebuf[q, T:, :] = ebuf[q, T:, :] * ebuf[q - 1, T:, :]

    @pl.when(blk == 0)
    def _():
        sbuf[...] = jnp.zeros_like(sbuf)

    n = XW // CW

    def store(j):
        cs = pl.ds(j * CW, CW)
        return pltpu.make_async_copy(out_ref.at[:, :, cs], out_hbm.at[:, :, cs], osem.at[j])

    def send(j):
        return pltpu.make_async_remote_copy(src_ref=obuf.at[j], dst_ref=sbuf.at[j], send_sem=send_sem.at[j],
                                            recv_sem=recv_sem.at[j], device_id=after, device_id_type=MESH)

    for j in range(n):
        cs = slice(j * CW, (j + 1) * CW)

        @pl.when(blk > 0)
        def _():
            send(j).wait_recv()

        @pl.when(blk < n_blocks - 1)
        def _():
            obuf[j] = through(3, sbuf[j], cs)
            send(j).start()

    for j in range(n):
        cs = slice(j * CW, (j + 1) * CW)
        for q in range(4):
            v = through(q - 1, sbuf[j], cs) if q else sbuf[j]
            out_ref[seq_slot(me, q), :, cs] = v
        store(j).start()

    @pl.when(blk < n_blocks - 1)
    def _():
        for j in range(n):
            send(j).wait_send()

    for j in range(n):
        store(j).wait()


def chain_call(e01, e2, e3, n_blocks):
    hbm = pl.BlockSpec(memory_space=pltpu.HBM)
    n = XW // CW
    return pl.pallas_call(
        functools.partial(chain_kernel, n_blocks),
        in_specs=[hbm] * 3,
        out_specs=hbm,
        out_shape=jax.ShapeDtypeStruct((4, T, XW), f32),
        scratch_shapes=[pltpu.VMEM((4, T + SUB, XW), f32), pltpu.VMEM((n, T, CW), f32), pltpu.VMEM((n, T, CW), f32),
                        pltpu.VMEM((4, T, XW), f32),                         pltpu.SemaphoreType.DMA((4,)), pltpu.SemaphoreType.DMA((n,)),
                        pltpu.SemaphoreType.DMA((n,)), pltpu.SemaphoreType.DMA((n,))],
        compiler_params=pltpu.CompilerParams(collective_id=1, has_side_effects=True, vmem_limit_bytes=63 * MIB),
        name="chain",
    )(e01, e2, e3)


NT = 512


def out_kernel(y_ref, yr_ref, w_ref, wr0_ref, wr1_ref, *refs):
    h = XW // 2
    acc = (jnp.dot(y_ref[...], w_ref[...], preferred_element_type=f32)
           + jnp.dot(yr_ref[:, :h], wr0_ref[...], preferred_element_type=f32)
           + jnp.dot(yr_ref[:, h:], wr1_ref[...], preferred_element_type=f32))
    if len(refs) > 1:
        x_ref, other_ref = refs[:2]
        acc = x_ref[...].astype(f32) + (acc + other_ref[...])
    refs[-1][...] = acc.astype(refs[-1].dtype)


def out_call(run, part, y, yr, rpart, w, wr, x=None, other=None, into=None):
    rows = TOK // NCH
    h = XW // 2
    at = lambda r: (lambda j: (r, j))
    cols = at(0)
    ins = [y, yr, w, *wr]
    specs = [pl.BlockSpec((rows, XW), lambda j: (run * (TOK // rows) + part, 0), pipeline_mode=ONE),
             pl.BlockSpec((rows, XW), lambda j: (rpart, 0), pipeline_mode=ONE),
             pl.BlockSpec((XW, NT), cols), pl.BlockSpec((h, NT), cols), pl.BlockSpec((h, NT), cols)]
    alias = {}
    if x is not None:
        ins += [x, other]
        specs += [pl.BlockSpec((rows, NT), at(part)), pl.BlockSpec((rows, NT), cols)]
    if into is not None:
        alias = {len(ins): 0}
        ins.append(into)
        specs.append(pl.BlockSpec(memory_space=pl.ANY))
    return pl.pallas_call(
        out_kernel,
        grid=(D // NT,), in_specs=specs,
        out_specs=pl.BlockSpec((rows, NT), cols if x is None else at(part)),
        out_shape=jax.ShapeDtypeStruct((rows, D), f32) if x is None else jax.ShapeDtypeStruct(x.shape, bf16),
        input_output_aliases=alias,
        compiler_params=pltpu.CompilerParams(dimension_semantics=("arbitrary",), vmem_limit_bytes=56 * MIB),
        cost_estimate=pl.CostEstimate(flops=rows * 33_000_000, bytes_accessed=rows * 100000, transcendentals=0),
        name="out_proj",
    )(*ins)


def send(v, perm):
    return lax.ppermute(v, 'tp', perm)


def after(v, *deps):
    return lax.optimization_barrier((v,) + deps)[0]


CORE_SWAP = [(i, i ^ 1) for i in range(4)]
CHIP_SWAP = [(i, i ^ 2) for i in range(4)]


def solution(mesh):
    n_blocks = mesh.shape['sp']
    token_spec = seg_spec = P(('dp', 'sp', 'tp'))
    weight_specs = tuple(P(*['tp' if i == dim else None for i in range(dim + 1)]) for dim in (2, 2, 1, 1, 2, 0, 1, 0, 0, 0, 0, 0))

    def body(x_loc, seg_loc, w_zx, w_bc, w_dt, conv_x, conv_bc, bias_x, bias_bc, a_log, dt_bias, d_skip, norm_w, w_out):
        rows, d = x_loc.shape
        me = lax.axis_index('tp')
        per, kper = rows // MT, rows // (NCH * MT)
        n_pl = mesh.shape['dp'] * n_blocks
        aux, tails, *parts = ahead_call(seg_loc, x_loc, w_out, n_blocks, n_pl)
        x_par = send(after(x_loc, aux), CORE_SWAP)
        x_dir = [send(v, CHIP_SWAP) for v in parts[:len(PARTS)]]
        w_half = [send(v, CHIP_SWAP) for v in parts[len(PARTS):]]

        def w_gather(h, dep):
            return lax.all_gather(after(w_half[h], dep), ('dp', 'sp'), axis=0, tiled=True)

        tails = tails.reshape(-1, d)
        w2, wb = w_zx.reshape(d, 2 * XW), w_bc.reshape(d, NB)
        pad = lambda v: jnp.pad(v.astype(f32), ((0, SUB - v.shape[0]), (0, 0)))
        cw = pad(jnp.concatenate([conv_x, bias_x[None]], axis=0))
        cwb = pad(jnp.concatenate([conv_bc.reshape(4, NB), bias_bc.reshape(1, NB)], axis=0))
        hp1 = jnp.pad(jnp.stack([dt_bias, a_log]), ((0, 6), (0, T - HEADS)))
        hp2 = pad(jnp.stack([jnp.repeat(d_skip, HEAD), norm_w.astype(f32)]))
        pre = jnp.stack([seq_slot(me, s) for s in range(4)]).astype(jnp.int32)
        weights = (w2, wb, w_dt.T)
        consts = (cw, cwb, hp1)

        def front(slots, part, parts, runs, carry, into, per):
            return front_call(pre, aux, [lambda b, s=s: b[s] * parts + part for s in slots], runs, weights, carry, consts,
                              into, part, parts, per=per)

        tail_row = lambda s: (lambda b: b[s] * HALO)
        *own, ends = front((0, 1), 0, 1, [(tails, tail_row(0), [x_loc]), (tails, tail_row(1), [x_par])], None, [], per)
        w_rem = [w_gather(0, ends)]
        x_dir[0] = after(x_dir[0], ends)
        x_fwd = [send(x_dir[0], CORE_SWAP)]
        *rem2, c2 = front((2,), 0, NCH, [(tails, tail_row(2), x_dir[:1])], None, [], kper)
        *rem3, c3 = front((3,), 0, NCH, [(tails, tail_row(3), [after(x_fwd[0], c2)])], None, [], kper)
        x_dir[1] = after(x_dir[1], c3)
        x_fwd.append(send(x_dir[1], CORE_SWAP))
        end = lambda k: PARTS[k] * MT - HALO
        *rem2, c2 = front((2,), 2, 4, [(x_dir[0], end(0), [x_dir[1]])], c2, rem2, 1)
        x_dir[2] = after(x_dir[2], c2)
        x_fwd.append(send(x_dir[2], CORE_SWAP))
        *rem2, c2 = front((2,), 3, 4, [(x_dir[1], end(1), [x_dir[2]])], c2, rem2, 1)
        *rem3, c3 = front((3,), 1, NCH, [(x_fwd[0], end(0), [after(x_fwd[1], c2), x_fwd[2]])], c3, rem3, kper)
        starts = chain_call(ends, c2, c3, n_blocks)
        w_rem.append(w_gather(1, starts))

        def mix(amaps, xs, arrs, start, **kw):
            return mixz_call(pre, aux, amaps, xs, arrs, w2, start, hp2, **kw)

        at = lambda s, k=0: (lambda b: b[s] * per + k)
        yn, c = mix([at(3), at(3, 2), at(3, 3)], x_fwd, rem3, starts, nx=1, per=per, ofs=0, cofs=3)
        y_in = [send(yn, CHIP_SWAP)]
        *yn, c = mix([at(2), at(2, 2), at(2, 3)], x_dir, rem2, after(starts, c), nx=1, per=per, ofs=0, cofs=2, n_out=NCH)
        y_in += [send(v, CHIP_SWAP) for v in yn]
        y_own, _ = mix([at(0), at(1)], [x_loc, x_par], own, after(starts, c), nx=2, per=per, ofs=0, cofs=0)
        other = []
        for k in range(NCH):
            part = out_call(1, k, y_own, y_in[0], k, w_out, w_rem)
            other.append(send(part, CORE_SWAP))
        y = None
        for k in range(NCH):
            y = out_call(0, k, y_own, y_in[k + 1], 0, w_out, w_rem, x_loc, other[k], y)
        return y

    return jax.shard_map(body, mesh=mesh, in_specs=(token_spec, seg_spec) + weight_specs, out_specs=token_spec, check_vma=False)
```
